32 devices in a mesh: dp: 8 (over y, x, core), rep: 4 (over z).
Axes of the slice: x: 2, y: 2, z: 4, core: 2. Of those that a mesh axis runs over, the one named last changes fastest.
Arguments:
- student_in: bfloat16 [16384, 320], P(('dp', 'rep')), may hold values from -6 to 6
- target_in: bfloat16 [16384, 320], P(('dp', 'rep')), may hold values from -6 to 6
- timesteps: int32 [64], P(('dp', 'rep')), may hold values from 20 to 999
- student_win: float32 [1280, 320], P('dp'), may hold values from -0.3125 to 0.3125
- student_wout: float32 [640, 320], P('dp'), may hold values from -0.25 to 0.25
- student_wtime: float32 [640, 320], P('dp'), may hold values from -0.25 to 0.25
- student_gain: float32 [320], replicated, may hold values from 0.5 to 1.5
- student_bias: float32 [320], replicated, may hold values from -3 to 3
- target_win: float32 [1280, 320], P('dp'), may hold values from -0.3125 to 0.3125
- target_wout: float32 [640, 320], P('dp'), may hold values from -0.25 to 0.25
- target_wtime: float32 [640, 320], P('dp'), may hold values from -0.25 to 0.25
- target_gain: float32 [320], replicated, may hold values from 0.5 to 1.5
- target_bias: float32 [320], replicated, may hold values from -3 to 3
Outputs:
- grad_win: float32 [1280, 320], P('dp')
- grad_wout: float32 [640, 320], P('dp')
- grad_wtime: float32 [640, 320], P('dp')
- grad_gain: float32 [320], replicated
- grad_bias: float32 [320], replicated
- ema_win: float32 [1280, 320], P('dp')
- ema_wout: float32 [640, 320], P('dp')
- ema_wtime: float32 [640, 320], P('dp')
- ema_gain: float32 [320], replicated
- ema_bias: float32 [320], replicated
The draws below stay inside these ranges and needn't reach their ends.
Inputs may be any that keep to these rules, and one draw needn't show every extreme that they name: `timesteps`: student timestep of each sample; the target is evaluated at 20 steps earlier.
All inputs are finite; a program needn't handle non-finite values.
Results may differ from the reference program's by a relative error of at most 0.004.
The reference program's roundings to bfloat16 on the way (of `time_feat`, `normed_b`, `hidden`, `grad_yb` and `grad_mix`) count: a program that leaves them out, or rounds other values in their place, can miss the bound.
Values may be sent and summed in bfloat16 or wider, within the bound.
A program may use at most 64 MiB of HBM per device.

```python
import math
import jax
import jax.numpy as jnp
from jax import lax

D = 320
FF = 640
TEMB = 640
SKIP = 20
TOK_DEV = 512
SAMPLES = 64
TOKENS = 16384
N_DP = 8


def set_ends(values, key, least, top_value):
    longest = values.shape.index(max(values.shape))
    spots = []
    for shift in (0, 1):
        where = [jax.random.randint(jax.random.fold_in(key, axis), (), 0, length) for axis, length in enumerate(values.shape)]
        where[longest] = (where[longest] + shift) % values.shape[longest]
        spots.append(tuple(where))
    return values.at[spots[0]].set(least).at[spots[1]].set(top_value)


def levels(stream_key, dims, split, least, largest):
    def one(axis_at, shards_of):
        steps = jax.random.uniform(jax.random.fold_in(jax.random.fold_in(stream_key, 6), axis_at), (shards_of,), jnp.float32, least / len(split), largest / len(split))
        return jnp.repeat(jnp.exp(steps), dims[axis_at] // shards_of).reshape((-1,) + (1,) * (len(dims) - axis_at - 1))

    level = one(*split[0])
    for cut in split[1:]:
        level = level * one(*cut)
    return level


def normal_values(own_key, extent, spread, most, shards=(), kind=jnp.bfloat16):
    values = spread * jax.random.normal(own_key, extent, jnp.float32)
    if shards:
        values = values * levels(own_key, extent, shards, -0.22, 0.18)
    return jnp.clip(values, -most, most).astype(kind)


def setup_inputs(seed: int = 0) -> dict:
    keys = jax.random.split(jax.random.key(seed), 14)
    return {
        "student_in": normal_values(keys[0], (TOKENS, D), 1.0, 6.0, ((0, 32),)),
        "target_in": normal_values(keys[1], (TOKENS, D), 1.0, 6.0, ((0, 32),)),
        "timesteps": set_ends(jax.random.randint(keys[2], (SAMPLES,), SKIP, 1000), jax.random.fold_in(keys[2], 1), SKIP, 999).astype(jnp.int32),
        "student_win": normal_values(keys[3], (2 * FF, D), D ** -0.5, 0.3125, ((0, 8),), jnp.float32),
        "student_wout": normal_values(keys[4], (FF, D), FF ** -0.5, 0.25, ((0, 8),), jnp.float32),
        "student_wtime": normal_values(keys[5], (TEMB, D), TEMB ** -0.5, 0.25, ((0, 8),), jnp.float32),
        "student_gain": jnp.clip(1.0 + 0.1 * jax.random.normal(keys[6], (D,), jnp.float32), 0.5, 1.5),
        "student_bias": normal_values(keys[7], (D,), 0.5, 3.0, (), jnp.float32),
        "target_win": normal_values(keys[8], (2 * FF, D), D ** -0.5, 0.3125, ((0, 8),), jnp.float32),
        "target_wout": normal_values(keys[9], (FF, D), FF ** -0.5, 0.25, ((0, 8),), jnp.float32),
        "target_wtime": normal_values(keys[10], (TEMB, D), TEMB ** -0.5, 0.25, ((0, 8),), jnp.float32),
        "target_gain": jnp.clip(1.0 + 0.1 * jax.random.normal(keys[11], (D,), jnp.float32), 0.5, 1.5),
        "target_bias": normal_values(keys[12], (D,), 0.5, 3.0, (), jnp.float32),
    }


ema_decay = 0.95
learn_rate = 0.05

def sinusoid(step_ids, width):
    half_width = width // 2
    frequency = jnp.exp(-math.log(10000.0) * jnp.arange(half_width, dtype=jnp.float32) / half_width)
    angles = step_ids.astype(jnp.float32)[:, None] * frequency[None, :]
    return jnp.concatenate([jnp.cos(angles), jnp.sin(angles)], axis=1)

def gelu_tanh(value):
    inner = 0.7978845608 * (value + 0.044715 * value * value * value)
    return 0.5 * value * (1.0 + jnp.tanh(inner))

def gelu_slope(value):
    tangent = jnp.tanh(0.7978845608 * (value + 0.044715 * value * value * value))
    return 0.5 * (1.0 + tangent) + 0.5 * value * (1.0 - tangent * tangent) * 0.7978845608 * (1.0 + 0.134145 * value * value)

def contract_last(left, right):
    return lax.dot_general(left, right, (((1,), (1,)), ((), ())), preferred_element_type=jnp.float32)

def contract_first(left, right):
    return lax.dot_general(left, right, (((0,), (0,)), ((), ())), preferred_element_type=jnp.float32)

def forward(tok_rows, step_ids, w_in, w_out, w_time, gain, bias):
    time_feat = jax.nn.silu(sinusoid(step_ids, w_time.shape[0])).astype(jnp.bfloat16)
    embedding = jnp.dot(time_feat, w_time, preferred_element_type=jnp.float32)
    samples = step_ids.shape[0]
    width = tok_rows.shape[1]
    summed = tok_rows.astype(jnp.float32).reshape(samples, -1, width) + embedding[:, None, :]
    summed = summed.reshape(-1, width)
    center = summed - lax.optimization_barrier(jnp.mean(summed, axis=1, keepdims=True))
    inv_std = lax.rsqrt(lax.optimization_barrier(jnp.mean(center * center, axis=1, keepdims=True)) + 1e-05)
    normed = center * inv_std
    normed_b = (normed * gain + bias).astype(jnp.bfloat16)
    mixed = contract_last(normed_b, w_in)
    hidden_count = w_out.shape[0]
    gate_part = mixed[:, :hidden_count]
    up_part = mixed[:, hidden_count:]
    gelu_gate = gelu_tanh(gate_part)
    hidden = (gelu_gate * up_part).astype(jnp.bfloat16)
    output = summed + jnp.dot(hidden, w_out, preferred_element_type=jnp.float32)
    return (output, (time_feat, normed, inv_std, normed_b, gate_part, up_part, gelu_gate, hidden))

def backward(grad_y, saved, w_in, w_out, gain):
    time_feat, normed, inv_std, normed_b, gate_part, up_part, gelu_gate, hidden = saved
    grad_yb = grad_y.astype(jnp.bfloat16)
    grad_h = contract_last(grad_yb, w_out)
    grad_mix = jnp.concatenate([grad_h * up_part * gelu_slope(gate_part), grad_h * gelu_gate], axis=1).astype(jnp.bfloat16)
    grad_z = jnp.dot(grad_mix, w_in, preferred_element_type=jnp.float32)
    grad_gain = lax.optimization_barrier(jnp.sum(grad_z * normed, axis=0))
    grad_bias = lax.optimization_barrier(jnp.sum(grad_z, axis=0))
    grad_n = grad_z * gain
    grad_s = grad_y + inv_std * (grad_n - lax.optimization_barrier(jnp.mean(grad_n, axis=1, keepdims=True)) - normed * lax.optimization_barrier(jnp.mean(grad_n * normed, axis=1, keepdims=True)))
    samples = time_feat.shape[0]
    grad_emb = lax.optimization_barrier(jnp.sum(grad_s.reshape(samples, -1, grad_s.shape[1]), axis=1))
    grad_time = lax.dot_general(time_feat.astype(jnp.float32), grad_emb, (((0,), (0,)), ((), ())), precision=lax.Precision.HIGHEST, preferred_element_type=jnp.float32)
    return (grad_yb, grad_mix, grad_gain, grad_bias, grad_time)

def reference(student_in, target_in, timesteps, student_win, student_wout, student_wtime, student_gain, student_bias, target_win, target_wout, target_wtime, target_gain, target_bias):
    s_in = student_win.astype(jnp.bfloat16)
    s_out = student_wout.astype(jnp.bfloat16)
    s_time = student_wtime.astype(jnp.bfloat16)
    t_in = target_win.astype(jnp.bfloat16)
    t_out = target_wout.astype(jnp.bfloat16)
    t_time = target_wtime.astype(jnp.bfloat16)
    width = student_in.shape[1]
    student_blocks = student_in.reshape(N_DP, -1, width)
    target_blocks = target_in.reshape(N_DP, -1, width)
    step_blocks = timesteps.reshape(N_DP, -1)

    def one_block(carry, block):
        s_rows, t_rows, step_ids = block
        student_out, saved = forward(s_rows, step_ids, s_in, s_out, s_time, student_gain, student_bias)
        target_out, unused = forward(t_rows, step_ids - SKIP, t_in, t_out, t_time, target_gain, target_bias)
        grad_y = (student_out - target_out) / TOK_DEV
        grad_yb, grad_mix, grad_gain, grad_bias, grad_time = backward(grad_y, saved, s_in, s_out, student_gain)
        grad_in = contract_first(grad_mix, saved[3])
        grad_out = contract_first(saved[7], grad_yb)
        totals = (carry[0] + grad_in, carry[1] + grad_out, carry[2] + grad_time, carry[3] + grad_gain, carry[4] + grad_bias)
        return (totals, None)
    start = (jnp.zeros(student_win.shape, jnp.float32), jnp.zeros(student_wout.shape, jnp.float32), jnp.zeros(student_wtime.shape, jnp.float32), jnp.zeros(student_gain.shape, jnp.float32), jnp.zeros(student_bias.shape, jnp.float32))
    totals, unused = lax.scan(one_block, start, (student_blocks, target_blocks, step_blocks))
    grad_win, grad_wout, grad_wtime, grad_gain, grad_bias = totals

    def average(target_p, student_p, grad_p):
        return ema_decay * target_p + (1.0 - ema_decay) * (student_p - learn_rate * grad_p)
    return (grad_win, grad_wout, grad_wtime, grad_gain, grad_bias, average(target_win, student_win, grad_win), average(target_wout, student_wout, grad_wout), average(target_wtime, student_wtime, grad_wtime), average(target_gain, student_gain, grad_gain), average(target_bias, student_bias, grad_bias))
```

```python
import functools
import math

import jax
import jax.numpy as jnp
from jax import lax
from jax.experimental import pallas as pl
from jax.experimental.pallas import tpu as pltpu
from jax.sharding import PartitionSpec as P

MESH = pl.DeviceIdType.MESH
SUB = 8

SKIP = 20


ema_decay = 0.95
learn_rate = 0.05


def sinusoid(step_ids, width):
    half_width = width // 2
    frequency = jnp.exp(-math.log(10000.0) * jnp.arange(half_width, dtype=jnp.float32) / half_width)
    angles = step_ids.astype(jnp.float32)[:, None] * frequency[None, :]
    return jnp.concatenate([jnp.cos(angles), jnp.sin(angles)], axis=1)


def gelu_tanh(value):
    inner = 0.7978845608 * (value + 0.044715 * value * value * value)
    return 0.5 * value * (1.0 + jnp.tanh(inner))


def gelu_slope(value):
    tangent = jnp.tanh(0.7978845608 * (value + 0.044715 * value * value * value))
    return 0.5 * (1.0 + tangent) + 0.5 * value * (1.0 - tangent * tangent) * 0.7978845608 * (
        1.0 + 0.134145 * value * value
    )


def contract_last(left, right):
    return lax.dot_general(
        left, right, (((1,), (1,)), ((), ())), preferred_element_type=jnp.float32
    )


def contract_first(left, right):
    return lax.dot_general(
        left, right, (((0,), (0,)), ((), ())), preferred_element_type=jnp.float32
    )


def forward(tok_rows, step_ids, w_in, w_out, w_time, gain, bias):
    time_feat = jax.nn.silu(sinusoid(step_ids, w_time.shape[0])).astype(jnp.bfloat16)
    embedding = jnp.dot(time_feat, w_time, preferred_element_type=jnp.float32)
    samples = step_ids.shape[0]
    width = tok_rows.shape[1]
    summed = tok_rows.astype(jnp.float32).reshape(samples, -1, width) + embedding[:, None, :]
    summed = summed.reshape(-1, width)
    center = summed - jnp.mean(summed, axis=1, keepdims=True)
    inv_std = lax.rsqrt(jnp.mean(center * center, axis=1, keepdims=True) + 1e-05)
    normed = center * inv_std
    normed_b = (normed * gain + bias).astype(jnp.bfloat16)
    mixed = contract_last(normed_b, w_in)
    hidden_count = w_out.shape[0]
    gate_part = mixed[:, :hidden_count]
    up_part = mixed[:, hidden_count:]
    gelu_gate = gelu_tanh(gate_part)
    hidden = (gelu_gate * up_part).astype(jnp.bfloat16)
    output = summed + jnp.dot(hidden, w_out, preferred_element_type=jnp.float32)
    return (output, (time_feat, normed, inv_std, normed_b, gate_part, up_part, gelu_gate, hidden))


def backward(grad_y, saved, w_in, w_out, gain):
    time_feat, normed, inv_std, normed_b, gate_part, up_part, gelu_gate, hidden = saved
    grad_yb = grad_y.astype(jnp.bfloat16)
    grad_h = contract_last(grad_yb, w_out)
    grad_mix = jnp.concatenate(
        [grad_h * up_part * gelu_slope(gate_part), grad_h * gelu_gate], axis=1
    ).astype(jnp.bfloat16)
    grad_z = jnp.dot(grad_mix, w_in, preferred_element_type=jnp.float32)
    grad_gain = jnp.sum(grad_z * normed, axis=0)
    grad_bias = jnp.sum(grad_z, axis=0)
    grad_n = grad_z * gain
    grad_s = grad_y + inv_std * (
        grad_n
        - jnp.mean(grad_n, axis=1, keepdims=True)
        - normed * jnp.mean(grad_n * normed, axis=1, keepdims=True)
    )
    samples = time_feat.shape[0]
    grad_emb = jnp.sum(grad_s.reshape(samples, -1, grad_s.shape[1]), axis=1)
    grad_time = lax.dot_general(
        time_feat.astype(jnp.float32),
        grad_emb,
        (((0,), (0,)), ((), ())),
        precision=lax.Precision.HIGHEST,
        preferred_element_type=jnp.float32,
    )
    return (grad_yb, grad_mix, grad_gain, grad_bias, grad_time)


def fetch(piece_in, piece_out, piece_time):
    return (
        lax.all_gather(piece_in, "dp", axis=0, tiled=True),
        lax.all_gather(piece_out, "dp", axis=0, tiled=True),
        lax.all_gather(piece_time, "dp", axis=0, tiled=True),
    )


def per_device(
    student_in,
    target_in,
    timesteps,
    student_win,
    student_wout,
    student_wtime,
    student_gain,
    student_bias,
    target_win,
    target_wout,
    target_wtime,
    target_gain,
    target_bias,
):
    s_in, s_out, s_time = fetch(
        student_win.astype(jnp.bfloat16),
        student_wout.astype(jnp.bfloat16),
        student_wtime.astype(jnp.bfloat16),
    )
    student_out, saved = forward(
        student_in, timesteps, s_in, s_out, s_time, student_gain, student_bias
    )
    t_in, t_out, t_time = fetch(
        target_win.astype(jnp.bfloat16),
        target_wout.astype(jnp.bfloat16),
        target_wtime.astype(jnp.bfloat16),
    )
    target_out, unused = forward(
        target_in, timesteps - SKIP, t_in, t_out, t_time, target_gain, target_bias
    )
    grad_y = (student_out - target_out) / student_in.shape[0]
    back_in, back_out = (
        lax.all_gather(student_win.astype(jnp.bfloat16), "dp", axis=0, tiled=True),
        lax.all_gather(student_wout.astype(jnp.bfloat16), "dp", axis=0, tiled=True),
    )
    grad_yb, grad_mix, grad_gain, grad_bias, grad_time = backward(
        grad_y, saved, back_in, back_out, student_gain
    )
    normed_b = saved[3]
    hidden = saved[7]
    part = grad_mix
    shard_in = lax.psum_scatter(
        contract_first(part, normed_b), "dp", scatter_dimension=0, tiled=True
    )
    part = hidden
    shard_out = lax.psum_scatter(
        contract_first(part, grad_yb), "dp", scatter_dimension=0, tiled=True
    )
    shard_time = lax.psum_scatter(grad_time, "dp", scatter_dimension=0, tiled=True)
    shard_in, shard_out, shard_time = lax.psum((shard_in, shard_out, shard_time), "rep")
    total_gain, total_bias = lax.psum((grad_gain, grad_bias), ("dp", "rep"))

    def average(target_p, student_p, grad_p):
        return ema_decay * target_p + (1.0 - ema_decay) * (student_p - learn_rate * grad_p)

    return (
        shard_in,
        shard_out,
        shard_time,
        total_gain,
        total_bias,
        average(target_win, student_win, shard_in),
        average(target_wout, student_wout, shard_out),
        average(target_wtime, student_wtime, shard_time),
        average(target_gain, student_gain, total_gain),
        average(target_bias, student_bias, total_bias),
    )


GATE_C = 0.7978845608


def put_packed(ref, value):
    rows, lo = value.shape[0], value.shape[1] // 128 * 128
    for i in range(lo // 128):
        ref[i * rows : (i + 1) * rows, :] = value[:, i * 128 : (i + 1) * 128].astype(ref.dtype)
    at, half = lo // 128 * rows, rows // 2
    rest = jnp.concatenate([value[:half, lo:], value[half:, lo:]], axis=1)
    ref[at : at + half, :] = rest.astype(ref.dtype)


def unpacked(value, rows, width):
    lo = width // 128 * 128
    at, half, rest = lo // 128 * rows, rows // 2, width - lo
    parts = [value[i * rows : (i + 1) * rows] for i in range(lo // 128)]
    tail = value[at : at + half]
    parts.append(jnp.concatenate([tail[:, :rest], tail[:, rest:]], axis=0))
    return jnp.concatenate(parts, axis=1)


def fused_kernel(n_rep, n_sam, names, *refs):
    r = dict(zip(names, refs))
    f32, bf16 = jnp.float32, jnp.bfloat16
    me, rep = lax.axis_index("dp"), lax.axis_index("rep")
    core, col, row = lax.rem(me, 2), lax.rem(lax.div(me, 2), 2), lax.div(me, 4)
    sw, so, st, tw, to, tt = (r[k] for k in ("sw", "so", "st", "tw", "to", "tt"))
    sg, sb, tg, tb, x_s, x_t = (r[k] for k in ("sg", "sb", "tg", "tb", "x_s", "x_t"))
    rows_in, rows_out, rows_time = sw.shape[0], so.shape[0], st.shape[0]
    width, tokens = x_s.shape
    per = tokens // n_sam
    lo = width // 128 * 128
    rest = width - lo
    ws_all, os_all, wt_all, ot_all = (r[k] for k in ("ws_all", "os_all", "wt_all", "ot_all"))
    ff = os_all.shape[0]
    tf_own, tf_all, e_part, e_in = (r[k] for k in ("tf_own", "tf_all", "e_part", "e_in"))
    g_all, e_all = r["g_o"], r["e_o"]

    flip = lambda b, on: 1 - b if on else b

    def peer(t):
        return flip(row, t & 4) * 4 + flip(col, t & 2) * 2 + flip(core, t & 1)

    def dp_id(t):
        return {"dp": peer(t)}

    def rep_peer(j):
        return flip(lax.div(rep, 2), j & 2) * 2 + flip(lax.rem(rep, 2), j & 1)

    def rep_id(j):
        return {"rep": rep_peer(j)}

    barrier = pltpu.get_barrier_semaphore()
    for t in range(1, 8):
        pl.semaphore_signal(barrier, inc=1, device_id=dp_id(t), device_id_type=MESH)
    for j in range(1, n_rep):
        pl.semaphore_signal(barrier, inc=1, device_id=rep_id(j), device_id_type=MESH)

    loads = []
    for i, name in enumerate(LOADED):
        copy = pltpu.make_async_copy(r[name + "_h"], r[name], r["ld_sem"].at[i])
        copy.start()
        loads.append(copy)

    def loaded(*keys):
        for key in keys:
            loads[LOADED.index(key)].wait()

    def send(src, dst, s_sem, r_sem, where):
        pltpu.make_async_remote_copy(
            src_ref=src, dst_ref=dst, send_sem=s_sem, recv_sem=r_sem,
            device_id=where, device_id_type=MESH,
        ).start()

    def bytes_of(ref, sem):
        return pltpu.make_async_remote_copy(
            src_ref=ref, dst_ref=ref, send_sem=sem, recv_sem=sem,
            device_id=dp_id(1), device_id_type=MESH,
        )

    def arrive(ref, sem):
        bytes_of(ref, sem).wait_recv()

    sent = []

    def exchange(key, source, slots, peers, where):
        for j in peers:
            src, dst = source(j), slots(j)
            send(src, dst, r[key + "_send"], r[key + "_recv"], where(j))

    bufs = (r["p_sin"], r["p_out"], r["p_tin"], r["p_tout"])
    s_in, out, t_in, t_out = range(4)
    g_send, g_recv = r["g_send"], r["g_recv"]
    loaded("ts")
    line = lax.broadcasted_iota(jnp.int32, (SUB, rows_time), 0)
    lane = lax.broadcasted_iota(jnp.int32, (SUB, rows_time), 1)
    steps = jnp.zeros((SUB, rows_time), f32)
    for k in range(n_sam):
        value = r["ts"][k]
        steps = jnp.where(line == k, value.astype(f32), steps)
        steps = jnp.where(line == n_sam + k, (value - SKIP).astype(f32), steps)
    half_width = 4 * rows_time
    for d in range(8):
        place = (lane + (d % 4) * rows_time).astype(f32)
        angle = steps * jnp.exp(-math.log(10000.0) * place / half_width)
        wave = jax.nn.silu(jnp.cos(angle) if d < 4 else jnp.sin(angle))
        tf_own[d] = jnp.where(line < 2 * n_sam, wave.astype(bf16).astype(f32), 0.0)
    tf_all[pl.ds(me, 1)] = tf_own[pl.ds(me, 1)]
    loaded("sw")
    put_packed(bufs[s_in].at[me], sw[...])
    loaded("so", "to")
    for i in range(lo // 128):
        at, lanes = slice(i * rows_out, (i + 1) * rows_out), slice(i * 128, (i + 1) * 128)
        bufs[out][me, at, :] = so[:, lanes].astype(bf16)
        bufs[t_out][me, at, :] = to[:, lanes].astype(bf16)
    at = slice(lo // 128 * rows_out, (lo // 128 + 1) * rows_out)
    bufs[out][me, at, :] = jnp.concatenate([so[:, lo:], to[:, lo:]], axis=1).astype(bf16)
    loaded("tw")
    put_packed(bufs[t_in].at[me], tw[...])
    loaded("st", "tt")
    pl.semaphore_wait(barrier, 7 + n_rep - 1)

    def cut(seg):
        return bufs[seg].shape[1] // 32 * 16

    def push(seg, orel, t, r_at, start=0, count=None):
        count = bufs[seg].shape[1] if count is None else count
        part = bufs[seg].at[peer(orel), pl.ds(start, count)]
        send(part, part, g_send.at[seg], g_recv.at[seg * 4 + r_at], dp_id(t))

    def landed(seg, r_at, count=1):
        arrive(bufs[seg].at[pl.ds(0, count)], g_recv.at[seg * 4 + r_at])

    def open_gather(seg):
        push(seg, 0, 2, 0)
        push(seg, 0, 4, 1)
        push(seg, 0, 1, 3)
        sent.append((bufs[seg].at[pl.ds(0, 7)], g_send.at[seg]))

    def relay(seg):
        c = cut(seg)
        landed(seg, 0)
        push(seg, 2, 4, 2, 0, c)
        landed(seg, 1)
        push(seg, 4, 2, 2, c, bufs[seg].shape[1] - c)
        push(seg, 2, 1, 3)
        push(seg, 4, 1, 3)

    def relay_far(seg):
        landed(seg, 2)
        push(seg, 6, 1, 3)

    def close_gather(seg):
        landed(seg, 3, 4)

    def place_in(seg, dst):
        half = rows_in // 2
        for o in range(8):
            for i in range(lo // 128):
                dst[o * rows_in : (o + 1) * rows_in, i * 128 : (i + 1) * 128] = bufs[seg][
                    o, i * rows_in : (i + 1) * rows_in, :
                ]
            at = lo // 128 * rows_in
            tail = bufs[seg][o, at : at + half, :]
            dst[o * rows_in : o * rows_in + half, lo:] = tail[:, :rest]
            dst[o * rows_in + half : (o + 1) * rows_in, lo:] = tail[:, rest:]

    def place_out(seg, dst, first):
        for o in range(8):
            to_rows = slice(o * rows_out, (o + 1) * rows_out)
            for i in range(lo // 128):
                dst[to_rows, i * 128 : (i + 1) * 128] = bufs[seg][o, i * rows_out : (i + 1) * rows_out, :]
            at = lo // 128 * rows_out
            dst[to_rows, lo:] = bufs[out][o, at : at + rows_out, :][:, first : first + rest]

    near = (1, 2, 4, 3, 5, 6, 7)
    exchange("tf", lambda t: tf_own.at[peer(t)], lambda t: tf_all.at[me], near, dp_id)
    open_gather(s_in)
    st_b, tt_b = st[...].astype(bf16), tt[...].astype(bf16)
    arrive(tf_all.at[pl.ds(0, 7)], r["tf_recv"])
    feats = tf_all[...].reshape(8 * SUB, rows_time).astype(bf16)
    part_s = jnp.dot(feats, st_b, preferred_element_type=f32)
    part_t = jnp.dot(feats, tt_b, preferred_element_type=f32)
    which = lax.rem(lax.broadcasted_iota(jnp.int32, part_s.shape, 0), SUB)
    e_part[...] = jnp.where(which < n_sam, part_s, part_t).reshape(e_part.shape)
    e_in[pl.ds(me, 1)] = e_part[pl.ds(me, 1)]
    exchange("e", lambda t: e_part.at[peer(t)], lambda t: e_in.at[me], near, dp_id)
    relay(s_in)
    open_gather(out)
    open_gather(t_in)

    ft_all, em_all = r["ft_all"], r["em_all"]
    ft_all[pl.ds(rep, 1)] = jnp.concatenate([tf_all[d, :n_sam, :] for d in range(8)], axis=0).astype(bf16)[None]
    far = (3, 2, 1)
    exchange("ft", lambda j: ft_all.at[rep], lambda j: ft_all.at[rep], far, rep_id)
    start = 0
    for student, target in ((sw, tw), (so, to), (st, tt)):
        count = student.shape[0]
        e_all[start : start + count, :] = ema_decay * target[...] + (1.0 - ema_decay) * student[...]
        start += count
    loaded("x_s", "sg", "sb")

    arrive(e_in.at[pl.ds(0, 7)], r["e_recv"])
    emb = e_in[0]
    for k in range(1, 8):
        emb = emb + e_in[k]

    y_v, normed_v, inv_v, nb_v, nbt_v = (r[k] for k in ("y_v", "normed_v", "inv_v", "nb_v", "nbt_v"))
    hid_v, a_v, b_v, gyb_v, gm_v = (r[k] for k in ("hid_v", "a_v", "b_v", "gyb_v", "gm_v"))

    def normalise(x_ref, k, shift, gain, bias):
        summed = x_ref[:, pl.ds(k * per, per)].astype(f32).T + shift
        center = summed - jnp.mean(summed, axis=1, keepdims=True)
        inv = lax.rsqrt(jnp.mean(center * center, axis=1, keepdims=True) + 1e-05)
        normed = center * inv
        return summed, inv, normed, (normed * gain + bias).astype(bf16)

    for k in range(n_sam):
        at = pl.ds(k * per, per)
        summed, inv, normed, nb = normalise(x_s, k, emb[k : k + 1], sg[...][None], sb[...][None])
        y_v[at, :], normed_v[at, :], nb_v[at, :] = summed, normed, nb
        inv_v[at, :] = inv
    relay(out)
    open_gather(t_out)
    relay_far(s_in)
    loaded("x_t", "tg", "tb")
    for k in range(n_sam):
        at = pl.ds(k * per, per)
        summed, inv, normed, nb = normalise(
            x_t, k, emb[n_sam + k : n_sam + k + 1], tg[...][None], tb[...][None]
        )
        y_v[at, :], nbt_v[at, :] = y_v[at, :] - summed, nb
    close_gather(s_in)
    place_in(s_in, ws_all)

    for k in range(n_sam):
        at = pl.ds(k * per, per)
        gate = contract_last(nb_v[at, :], ws_all[:ff, :])
        up = contract_last(nb_v[at, :], ws_all[ff:, :])
        tangent = jnp.tanh(GATE_C * (gate + 0.044715 * gate * gate * gate))
        half = 0.5 * (1.0 + tangent)
        act = gate * half
        slope = half + 0.5 * gate * (1.0 - tangent * tangent) * GATE_C * (1.0 + 0.134145 * gate * gate)
        a_v[at, :], b_v[at, :] = up * slope, act
        hid_v[at, :] = (act * up).astype(bf16)
        if k == 0:
            relay(t_in)
            relay_far(out)
    relay(t_out)
    close_gather(out)
    place_out(out, os_all, 0)
    for k in range(n_sam):
        at = pl.ds(k * per, per)
        y_v[at, :] = y_v[at, :] + jnp.dot(hid_v[at, :], os_all[...], preferred_element_type=f32)
    relay_far(t_in)
    relay_far(t_out)
    close_gather(t_in)
    place_in(t_in, wt_all)

    for k in range(n_sam):
        at = pl.ds(k * per, per)
        gate = contract_last(nbt_v[at, :], wt_all[:ff, :])
        up = contract_last(nbt_v[at, :], wt_all[ff:, :])
        hid = (gelu_tanh(gate) * up).astype(bf16)
        if k == 0:
            close_gather(t_out)
            place_out(t_out, ot_all, rest)
        gy = (y_v[at, :] - jnp.dot(hid, ot_all[...], preferred_element_type=f32)) * (1.0 / tokens)
        y_v[at, :], gyb_v[at, :] = gy, gy.astype(bf16)

    r1_o, r1_i = r["r1_o"], r["r1_i"]
    blocks = {
        "o": (r["gs_o"], r1_o, rows_out, 0),
        "a": (r["gs_i"], r1_i, rows_in, 0),
        "b": (r["gs_i"], r1_i, rows_in, rows_out),
    }

    def to_core(src, dst, count, q, key):
        part = src.at[pl.ds(pl.multiple_of((2 * q + 1 - core) * count, 16), count)]
        send(part, dst.at[q], r[key + "_send"], r[key + "_recv"], dp_id(1))

    def pair(key, rel):
        g, r1, count, first = blocks[key]
        owner = peer(rel)
        own = g[pl.ds(pl.multiple_of(owner * count + first, 16), rows_out), :]
        return own + r1[lax.div(owner, 2), first : first + rows_out, :].astype(f32)

    def to_chip(key, k):
        s2, r2 = r["s2_" + key], r["r2_" + key]
        put_packed(s2.at[k], pair(key, 2 * k))
        send(s2.at[k], r2.at[k], r["r2s_" + key], r["r2r_" + key], dp_id(2 * k))

    total_out = contract_first(hid_v[...], gyb_v[...])
    r["gs_o"][...] = total_out
    r["gb_o"][...] = total_out.astype(bf16)
    for q in range(4):
        to_core(r["gb_o"], r1_o, rows_out, q, "c0")

    grad_gain = jnp.zeros((1, width), f32)
    grad_bias = grad_gain
    embs = []
    small, small_rep = r["small"], r["small_rep"]
    for k in range(n_sam):
        at = pl.ds(k * per, per)
        gh = contract_last(gyb_v[at, :], os_all[...])
        gma, gmb = (gh * a_v[at, :]).astype(bf16), (gh * b_v[at, :]).astype(bf16)
        gm_v[0, at, :], gm_v[1, at, :] = gma, gmb
        gz = jnp.dot(gma, ws_all[:ff, :], preferred_element_type=f32) + jnp.dot(
            gmb, ws_all[ff:, :], preferred_element_type=f32
        )
        normed = normed_v[at, :]
        grad_gain = grad_gain + jnp.sum(gz * normed, axis=0, keepdims=True)
        grad_bias = grad_bias + jnp.sum(gz, axis=0, keepdims=True)
        gn = gz * sg[...][None]
        gs = y_v[at, :] + inv_v[at, :] * (
            gn
            - jnp.mean(gn, axis=1, keepdims=True)
            - normed * jnp.mean(gn * normed, axis=1, keepdims=True)
        )
        embs.append(jnp.sum(gs, axis=0, keepdims=True))
        if k == 0:
            arrive(r1_o, r["c0_recv"])
            for q in (3, 1, 2):
                to_chip("o", q)
            put_packed(r["p_o"], pair("o", 0))
    fill = jnp.zeros((SUB - n_sam - 2, width), f32)
    small[pl.ds(me, 1)] = jnp.concatenate(embs + [grad_gain, grad_bias, fill], axis=0)[None]

    for turn in range(2):
        h = 1 - row if turn == 0 else row
        total = contract_first(gm_v[h], nb_v[...])
        at = pl.ds(pl.multiple_of(h * ff, 16), ff)
        r["gs_i"][at, :], r["gb_i"][at, :] = total, total.astype(bf16)
        for q in range(2):
            to_core(r["gb_i"], r1_i, rows_in, 2 * h + q, "c" + str(1 + turn))
        if turn == 0:
            exchange("sm", lambda t: small.at[me], lambda t: small.at[me], near, dp_id)
    arrive(r1_i.at[pl.ds(0, 2)], r["c1_recv"])
    for key in "ab":
        to_chip(key, 3)
        to_chip(key, 2)
    arrive(r1_i.at[pl.ds(0, 2)], r["c2_recv"])
    for key in "ab":
        to_chip(key, 1)
    for key in "ab":
        put_packed(r["p_" + key], pair(key, 0))

    def to_planes(key):
        p, pb, r2, r3 = r["p_" + key], r["pb_" + key], r["r2_" + key], r["r3_" + key]
        used, share = r2.shape[1], pb.shape[1]
        arrive(r2.at[pl.ds(1, 3)], r["r2r_" + key])
        p[:used, :] = p[:used, :] + r2[1].astype(f32) + r2[2].astype(f32) + r2[3].astype(f32)
        p[used:, :] = jnp.zeros((p.shape[0] - used, 128), f32)
        for q in range(n_rep):
            pb[q] = p[q * share : (q + 1) * share, :].astype(bf16)
        for j in far:
            send(pb.at[rep_peer(j)], r3.at[j], r["r3s_" + key], r["r3r_" + key], rep_id(j))

    def share_total(key):
        p, r3, fin = r["p_" + key], r["r3_" + key], r["fin_" + key]
        share = fin.shape[1]
        total = p[pl.ds(pl.multiple_of(rep * share, 8), share), :]
        arrive(r3.at[pl.ds(1, 3)], r["r3r_" + key])
        for j in range(1, n_rep):
            total = total + r3[j].astype(f32)
        fin[pl.ds(rep, 1)] = total.astype(bf16)[None]
        for j in far:
            send(fin.at[rep], fin.at[rep], r["r4s_" + key], r["r4r_" + key], rep_id(j))

    def finish(start, grad):
        at = slice(start, start + grad.shape[0])
        g_all[at, :] = grad
        e_all[at, :] = e_all[at, :] - (1.0 - ema_decay) * learn_rate * grad

    def collect(key, start):
        p, fin = r["p_" + key], r["fin_" + key]
        share = fin.shape[1]
        arrive(fin.at[pl.ds(0, 3)], r["r4r_" + key])
        for q in range(n_rep):
            p[q * share : (q + 1) * share, :] = fin[q].astype(f32)
        finish(start, unpacked(p[...], rows_out, width))

    to_planes("o")
    arrive(small.at[pl.ds(0, 7)], r["sm_recv"])
    em_all[pl.ds(rep, 1)] = jnp.concatenate([small[d, :n_sam, :] for d in range(8)], axis=0).astype(bf16)[None]
    sums = small[0]
    for k in range(1, 8):
        sums = sums + small[k]
    small_rep[pl.ds(rep, 1)] = sums[None]
    exchange("em", lambda j: em_all.at[rep], lambda j: em_all.at[rep], far, rep_id)
    exchange("rs", lambda j: small_rep.at[rep], lambda j: small_rep.at[rep], far, rep_id)
    share_total("o")
    to_planes("a")
    arrive(ft_all.at[pl.ds(0, 3)], r["ft_recv"])
    arrive(em_all.at[pl.ds(0, 3)], r["em_recv"])
    arrive(small_rep.at[pl.ds(0, 3)], r["rs_recv"])
    grad_time = contract_first(ft_all[0], em_all[0])
    sums = small_rep[0]
    for j in range(1, n_rep):
        grad_time = grad_time + contract_first(ft_all[j], em_all[j])
        sums = sums + small_rep[j]
    finish(rows_in + rows_out, grad_time)
    gg, gb = sums[n_sam, :], sums[n_sam + 1, :]
    r["gg_o"][...], r["gb_o_"][...] = gg, gb
    r["eg_o"][...] = average(tg[...], sg[...], gg)
    r["eb_o"][...] = average(tb[...], sb[...], gb)
    to_planes("b")
    collect("o", rows_in)
    share_total("a")
    share_total("b")
    collect("a", 0)
    collect("b", rows_out)
    for key, ref in (("tf", tf_all), ("e", e_in), ("sm", small)):
        sent.append((ref.at[pl.ds(0, 7)], r[key + "_send"]))
    for key, ref in (("ft", ft_all), ("em", em_all), ("rs", small_rep)):
        sent.append((ref.at[pl.ds(0, 3)], r[key + "_send"]))
    sent += [(r1_o, r["c0_send"]), (r1_i.at[pl.ds(0, 2)], r["c1_send"]), (r1_i.at[pl.ds(0, 2)], r["c2_send"])]
    for key in "oab":
        sent.append((r["r2_" + key].at[pl.ds(0, 3)], r["r2s_" + key]))
        sent.append((r["r3_" + key].at[pl.ds(0, 3)], r["r3s_" + key]))
        sent.append((r["fin_" + key].at[pl.ds(0, 3)], r["r4s_" + key]))
    for ref, sem in sent:
        bytes_of(ref, sem).wait_send()


LOADED = ("ts", "sw", "so", "to", "tw", "st", "tt", "x_s", "sg", "sb", "x_t", "tg", "tb")


def average(target_p, student_p, grad_p):
    return ema_decay * target_p + (1.0 - ema_decay) * (student_p - learn_rate * grad_p)


def output_kernel(grads, means, gg, gb, eg, eb, gw_o, go_o, gt_o, gg_o, gb_o, ew_o, eo_o, et_o, eg_o, eb_o, sem):
    copies = []
    for src, outs in ((grads, (gw_o, go_o, gt_o)), (means, (ew_o, eo_o, et_o))):
        start = 0
        for dst in outs:
            copies.append((src.at[pl.ds(start, dst.shape[0])], dst))
            start += dst.shape[0]
    copies += [(gg, gg_o), (gb, gb_o), (eg, eg_o), (eb, eb_o)]
    copies = [pltpu.make_async_copy(src, dst, sem.at[i]) for i, (src, dst) in enumerate(copies)]
    for copy in copies:
        copy.start()
    for copy in copies:
        copy.wait()


def fused_device(n_dp, n_rep, *args):
    (student_in, target_in, timesteps, sw, so, st, sg, sb, tw, to, tt, tg, tb) = args
    f32, bf16 = jnp.float32, jnp.bfloat16
    tokens, width = student_in.shape
    n_sam = timesteps.shape[0]
    rows_in, rows_out, rows_time = sw.shape[0], so.shape[0], st.shape[0]
    ff = rows_out * n_dp
    rows_all = rows_in + rows_out + rows_time
    vm = pltpu.VMEM
    dma = pltpu.SemaphoreType.DMA
    full = width // 128
    packed_in, packed_out = rows_in * full + rows_in // 2, rows_out * full + rows_out // 2
    share = -(-packed_out // (8 * n_rep)) * 8
    scratch = dict(
        ts=pltpu.SMEM((n_sam,), jnp.int32),
        sw=vm(sw.shape, f32), so=vm(so.shape, f32), st=vm(st.shape, f32),
        tw=vm(tw.shape, f32), to=vm(to.shape, f32), tt=vm(tt.shape, f32),
        sg=vm(sg.shape, f32), sb=vm(sb.shape, f32), tg=vm(tg.shape, f32), tb=vm(tb.shape, f32),
        x_s=vm((width, tokens), bf16), x_t=vm((width, tokens), bf16),
        p_sin=vm((n_dp, packed_in, 128), bf16), p_out=vm((n_dp, rows_out * (full + 1), 128), bf16),
        p_tin=vm((n_dp, packed_in, 128), bf16), p_tout=vm((n_dp, rows_out * full, 128), bf16),
        ws_all=vm((n_dp * rows_in, width), bf16), os_all=vm((ff, width), bf16),
        wt_all=vm((n_dp * rows_in, width), bf16), ot_all=vm((ff, width), bf16),
        tf_own=vm((n_dp, SUB, rows_time), f32), tf_all=vm((n_dp, SUB, rows_time), f32),
        e_part=vm((n_dp, SUB, width), f32), e_in=vm((n_dp, SUB, width), f32),
        small=vm((n_dp, SUB, width), f32), small_rep=vm((n_rep, SUB, width), f32),
        ft_all=vm((n_rep, n_dp * n_sam, rows_time), bf16), em_all=vm((n_rep, n_dp * n_sam, width), bf16),
        normed_v=vm((tokens, width), f32), inv_v=vm((tokens, 1), f32), nb_v=vm((tokens, width), bf16),
        hid_v=vm((tokens, ff), bf16), a_v=vm((tokens, ff), f32), b_v=vm((tokens, ff), f32),
        y_v=vm((tokens, width), f32), nbt_v=vm((tokens, width), bf16), gyb_v=vm((tokens, width), bf16),
        gm_v=vm((2, tokens, ff), bf16),
        gs_i=vm((n_dp * rows_in, width), f32), gs_o=vm((ff, width), f32),
        gb_i=vm((n_dp * rows_in, width), bf16), gb_o=vm((ff, width), bf16),
        r1_i=vm((4, rows_in, width), bf16), r1_o=vm((4, rows_out, width), bf16),
        ld_sem=dma((len(LOADED),)), g_send=dma((4,)), g_recv=dma((16,)),
    )
    for key in "oab":
        for name in ("s2_", "r2_"):
            scratch[name + key] = vm((4, packed_out, 128), bf16)
        scratch["p_" + key] = vm((n_rep * share, 128), f32)
        for name in ("pb_", "r3_", "fin_"):
            scratch[name + key] = vm((n_rep, share, 128), bf16)
        for name in ("r2", "r3", "r4"):
            scratch[name + "s_" + key], scratch[name + "r_" + key] = dma, dma
    for key in ("tf", "e", "sm", "ft", "em", "rs", "c0", "c1", "c2"):
        scratch[key + "_send"], scratch[key + "_recv"] = dma, dma
    shape = jax.ShapeDtypeStruct
    results = dict(
        g_o=shape((rows_all, width), f32), e_o=shape((rows_all, width), f32), gg_o=shape((width,), f32),
        gb_o_=shape((width,), f32), eg_o=shape((width,), f32), eb_o=shape((width,), f32),
    )
    operands = dict(
        ts=timesteps, sw=sw, so=so, to=to, tw=tw, st=st, tt=tt, x_s=student_in.T, sg=sg, sb=sb,
        x_t=target_in.T, tg=tg, tb=tb,
    )
    names = tuple(key + "_h" for key in operands) + tuple(results) + tuple(scratch)
    values = pl.pallas_call(
        functools.partial(fused_kernel, n_rep, n_sam, names),
        out_shape=tuple(results.values()),
        in_specs=[pl.BlockSpec(memory_space=pltpu.HBM)] * len(operands),
        out_specs=[pl.BlockSpec(memory_space=vm)] * len(results),
        scratch_shapes=list(scratch.values()),
        compiler_params=pltpu.CompilerParams(
            collective_id=0, has_side_effects=True, vmem_limit_bytes=40 * 1024 * 1024
        ),
        name="distill_step",
    )(*(pltpu.with_memory_space_constraint(value, pltpu.HBM) for value in operands.values()))
    big = [shape(w.shape, f32) for w in (sw, so, st)]
    flat = [shape((width,), f32)] * 2
    return tuple(
        pl.pallas_call(
            output_kernel,
            out_shape=(*big, *flat, *big, *flat),
            in_specs=[pl.BlockSpec(memory_space=vm)] * len(results),
            out_specs=[pl.BlockSpec(memory_space=pltpu.HBM)] * 10,
            scratch_shapes=[dma((10,))],
            compiler_params=pltpu.CompilerParams(vmem_limit_bytes=8 * 1024 * 1024),
            name="output_step",
        )(*values)
    )


def fits_fused(n_dp, n_rep, args):
    tokens, samples = args[0].shape[0], args[2].shape[0]
    n_dev = n_dp * n_rep
    rows = [args[i].shape[0] for i in (3, 4, 5)]
    return (
        n_dp == 8
        and n_rep == 4
        and samples % n_dev == 0
        and 2 * (samples // n_dev) + 0 <= SUB
        and samples // n_dev + 2 <= SUB
        and tokens % samples == 0
        and (tokens // samples) % 128 == 0
        and all(r % (16 * n_dp) == 0 for r in rows)
        and all(r % (32 * n_dp) == 0 for r in rows[:1])
        and rows[0] == 2 * rows[1]
        and rows[2] == rows[1]
        and args[0].shape[1] % 128 == 64
    )


def solution(mesh):
    in_specs = (
        P(("dp", "rep"), None),
        P(("dp", "rep"), None),
        P(("dp", "rep")),
        P("dp", None),
        P("dp", None),
        P("dp", None),
        P(),
        P(),
        P("dp", None),
        P("dp", None),
        P("dp", None),
        P(),
        P(),
    )
    out_specs = (
        P("dp", None),
        P("dp", None),
        P("dp", None),
        P(),
        P(),
        P("dp", None),
        P("dp", None),
        P("dp", None),
        P(),
        P(),
    )
    n_dp, n_rep = mesh.shape["dp"], mesh.shape["rep"]

    def step(*args):
        fused = fits_fused(n_dp, n_rep, args)
        body = functools.partial(fused_device, n_dp, n_rep) if fused else per_device
        return jax.shard_map(
            body, mesh=mesh, in_specs=in_specs, out_specs=out_specs, check_vma=False
        )(*args)

    return step
```

```python
import functools
import math

import jax
import jax.numpy as jnp
from jax import lax
from jax.experimental import pallas as pl
from jax.experimental.pallas import tpu as pltpu
from jax.sharding import PartitionSpec as P

MESH = pl.DeviceIdType.MESH
SUB = 8

SKIP = 20


ema_decay = 0.95
learn_rate = 0.05


def sinusoid(step_ids, width):
    half_width = width // 2
    frequency = jnp.exp(-math.log(10000.0) * jnp.arange(half_width, dtype=jnp.float32) / half_width)
    angles = step_ids.astype(jnp.float32)[:, None] * frequency[None, :]
    return jnp.concatenate([jnp.cos(angles), jnp.sin(angles)], axis=1)


def gelu_tanh(value):
    inner = 0.7978845608 * (value + 0.044715 * value * value * value)
    return 0.5 * value * (1.0 + jnp.tanh(inner))


def gelu_slope(value):
    tangent = jnp.tanh(0.7978845608 * (value + 0.044715 * value * value * value))
    return 0.5 * (1.0 + tangent) + 0.5 * value * (1.0 - tangent * tangent) * 0.7978845608 * (
        1.0 + 0.134145 * value * value
    )


def contract_last(left, right):
    return lax.dot_general(
        left, right, (((1,), (1,)), ((), ())), preferred_element_type=jnp.float32
    )


def contract_first(left, right):
    return lax.dot_general(
        left, right, (((0,), (0,)), ((), ())), preferred_element_type=jnp.float32
    )


def forward(tok_rows, step_ids, w_in, w_out, w_time, gain, bias):
    time_feat = jax.nn.silu(sinusoid(step_ids, w_time.shape[0])).astype(jnp.bfloat16)
    embedding = jnp.dot(time_feat, w_time, preferred_element_type=jnp.float32)
    samples = step_ids.shape[0]
    width = tok_rows.shape[1]
    summed = tok_rows.astype(jnp.float32).reshape(samples, -1, width) + embedding[:, None, :]
    summed = summed.reshape(-1, width)
    center = summed - jnp.mean(summed, axis=1, keepdims=True)
    inv_std = lax.rsqrt(jnp.mean(center * center, axis=1, keepdims=True) + 1e-05)
    normed = center * inv_std
    normed_b = (normed * gain + bias).astype(jnp.bfloat16)
    mixed = contract_last(normed_b, w_in)
    hidden_count = w_out.shape[0]
    gate_part = mixed[:, :hidden_count]
    up_part = mixed[:, hidden_count:]
    gelu_gate = gelu_tanh(gate_part)
    hidden = (gelu_gate * up_part).astype(jnp.bfloat16)
    output = summed + jnp.dot(hidden, w_out, preferred_element_type=jnp.float32)
    return (output, (time_feat, normed, inv_std, normed_b, gate_part, up_part, gelu_gate, hidden))


def backward(grad_y, saved, w_in, w_out, gain):
    time_feat, normed, inv_std, normed_b, gate_part, up_part, gelu_gate, hidden = saved
    grad_yb = grad_y.astype(jnp.bfloat16)
    grad_h = contract_last(grad_yb, w_out)
    grad_mix = jnp.concatenate(
        [grad_h * up_part * gelu_slope(gate_part), grad_h * gelu_gate], axis=1
    ).astype(jnp.bfloat16)
    grad_z = jnp.dot(grad_mix, w_in, preferred_element_type=jnp.float32)
    grad_gain = jnp.sum(grad_z * normed, axis=0)
    grad_bias = jnp.sum(grad_z, axis=0)
    grad_n = grad_z * gain
    grad_s = grad_y + inv_std * (
        grad_n
        - jnp.mean(grad_n, axis=1, keepdims=True)
        - normed * jnp.mean(grad_n * normed, axis=1, keepdims=True)
    )
    samples = time_feat.shape[0]
    grad_emb = jnp.sum(grad_s.reshape(samples, -1, grad_s.shape[1]), axis=1)
    grad_time = lax.dot_general(
        time_feat.astype(jnp.float32),
        grad_emb,
        (((0,), (0,)), ((), ())),
        precision=lax.Precision.HIGHEST,
        preferred_element_type=jnp.float32,
    )
    return (grad_yb, grad_mix, grad_gain, grad_bias, grad_time)


def fetch(piece_in, piece_out, piece_time):
    return (
        lax.all_gather(piece_in, "dp", axis=0, tiled=True),
        lax.all_gather(piece_out, "dp", axis=0, tiled=True),
        lax.all_gather(piece_time, "dp", axis=0, tiled=True),
    )


def per_device(
    student_in,
    target_in,
    timesteps,
    student_win,
    student_wout,
    student_wtime,
    student_gain,
    student_bias,
    target_win,
    target_wout,
    target_wtime,
    target_gain,
    target_bias,
):
    s_in, s_out, s_time = fetch(
        student_win.astype(jnp.bfloat16),
        student_wout.astype(jnp.bfloat16),
        student_wtime.astype(jnp.bfloat16),
    )
    student_out, saved = forward(
        student_in, timesteps, s_in, s_out, s_time, student_gain, student_bias
    )
    t_in, t_out, t_time = fetch(
        target_win.astype(jnp.bfloat16),
        target_wout.astype(jnp.bfloat16),
        target_wtime.astype(jnp.bfloat16),
    )
    target_out, unused = forward(
        target_in, timesteps - SKIP, t_in, t_out, t_time, target_gain, target_bias
    )
    grad_y = (student_out - target_out) / student_in.shape[0]
    back_in, back_out = (
        lax.all_gather(student_win.astype(jnp.bfloat16), "dp", axis=0, tiled=True),
        lax.all_gather(student_wout.astype(jnp.bfloat16), "dp", axis=0, tiled=True),
    )
    grad_yb, grad_mix, grad_gain, grad_bias, grad_time = backward(
        grad_y, saved, back_in, back_out, student_gain
    )
    normed_b = saved[3]
    hidden = saved[7]
    part = grad_mix
    shard_in = lax.psum_scatter(
        contract_first(part, normed_b), "dp", scatter_dimension=0, tiled=True
    )
    part = hidden
    shard_out = lax.psum_scatter(
        contract_first(part, grad_yb), "dp", scatter_dimension=0, tiled=True
    )
    shard_time = lax.psum_scatter(grad_time, "dp", scatter_dimension=0, tiled=True)
    shard_in, shard_out, shard_time = lax.psum((shard_in, shard_out, shard_time), "rep")
    total_gain, total_bias = lax.psum((grad_gain, grad_bias), ("dp", "rep"))

    def average(target_p, student_p, grad_p):
        return ema_decay * target_p + (1.0 - ema_decay) * (student_p - learn_rate * grad_p)

    return (
        shard_in,
        shard_out,
        shard_time,
        total_gain,
        total_bias,
        average(target_win, student_win, shard_in),
        average(target_wout, student_wout, shard_out),
        average(target_wtime, student_wtime, shard_time),
        average(target_gain, student_gain, total_gain),
        average(target_bias, student_bias, total_bias),
    )


GATE_C = 0.7978845608


def put_packed(ref, value):
    rows, lo = value.shape[0], value.shape[1] // 128 * 128
    for i in range(lo // 128):
        ref[i * rows : (i + 1) * rows, :] = value[:, i * 128 : (i + 1) * 128].astype(ref.dtype)
    at, half = lo // 128 * rows, rows // 2
    rest = jnp.concatenate([value[:half, lo:], value[half:, lo:]], axis=1)
    ref[at : at + half, :] = rest.astype(ref.dtype)


def unpacked(value, rows, width):
    lo = width // 128 * 128
    at, half, rest = lo // 128 * rows, rows // 2, width - lo
    parts = [value[i * rows : (i + 1) * rows] for i in range(lo // 128)]
    tail = value[at : at + half]
    parts.append(jnp.concatenate([tail[:, :rest], tail[:, rest:]], axis=0))
    return jnp.concatenate(parts, axis=1)


def fused_kernel(n_rep, n_sam, names, *refs):
    r = dict(zip(names, refs))
    f32, bf16 = jnp.float32, jnp.bfloat16
    me, rep = lax.axis_index("dp"), lax.axis_index("rep")
    core, col, row = lax.rem(me, 2), lax.rem(lax.div(me, 2), 2), lax.div(me, 4)
    sw, so, st, tw, to, tt = (r[k] for k in ("sw", "so", "st", "tw", "to", "tt"))
    sg, sb, tg, tb, x_s, x_t = (r[k] for k in ("sg", "sb", "tg", "tb", "x_s", "x_t"))
    rows_in, rows_out, rows_time = sw.shape[0], so.shape[0], st.shape[0]
    packed_out = r["s2_a"].shape[1]
    width, tokens = x_s.shape
    per = tokens // n_sam
    lo = width // 128 * 128
    rest = width - lo
    ws_all, os_all, wt_all, ot_all = (r[k] for k in ("ws_all", "os_all", "wt_all", "ot_all"))
    ff = os_all.shape[0]
    tf_own, tf_all, e_part, e_in = (r[k] for k in ("tf_own", "tf_all", "e_part", "e_in"))
    g_all, e_all = r["g_o"], r["e_o"]

    flip = lambda b, on: 1 - b if on else b

    def peer(t):
        return flip(row, t & 4) * 4 + flip(col, t & 2) * 2 + flip(core, t & 1)

    def dp_id(t):
        return {"dp": peer(t)}

    def rep_peer(j):
        return flip(lax.div(rep, 2), j & 2) * 2 + flip(lax.rem(rep, 2), j & 1)

    def rep_id(j):
        return {"rep": rep_peer(j)}

    barrier = pltpu.get_barrier_semaphore()
    for t in range(1, 8):
        pl.semaphore_signal(barrier, inc=1, device_id=dp_id(t), device_id_type=MESH)
    for j in range(1, n_rep):
        pl.semaphore_signal(barrier, inc=1, device_id=rep_id(j), device_id_type=MESH)

    loads = []
    for i, name in enumerate(LOADED):
        copy = pltpu.make_async_copy(r[name + "_h"], r[name], r["ld_sem"].at[i])
        copy.start()
        loads.append(copy)

    def loaded(*keys):
        for key in keys:
            loads[LOADED.index(key)].wait()

    def send(src, dst, s_sem, r_sem, where):
        pltpu.make_async_remote_copy(
            src_ref=src, dst_ref=dst, send_sem=s_sem, recv_sem=r_sem,
            device_id=where, device_id_type=MESH,
        ).start()

    def bytes_of(ref, sem):
        return pltpu.make_async_remote_copy(
            src_ref=ref, dst_ref=ref, send_sem=sem, recv_sem=sem,
            device_id=dp_id(1), device_id_type=MESH,
        )

    def arrive(ref, sem):
        bytes_of(ref, sem).wait_recv()

    sent = []

    def exchange(key, source, slots, peers, where):
        for j in peers:
            src, dst = source(j), slots(j)
            send(src, dst, r[key + "_send"], r[key + "_recv"], where(j))

    bufs = (r["p_sin"], r["p_out"], r["p_tin"], r["p_tout"])
    s_in, out, t_in, t_out = range(4)
    g_send, g_recv = r["g_send"], r["g_recv"]
    loaded("ts")
    line = lax.broadcasted_iota(jnp.int32, (SUB, rows_time), 0)
    lane = lax.broadcasted_iota(jnp.int32, (SUB, rows_time), 1)
    steps = jnp.zeros((SUB, rows_time), f32)
    for k in range(n_sam):
        value = r["ts"][k]
        steps = jnp.where(line == k, value.astype(f32), steps)
        steps = jnp.where(line == n_sam + k, (value - SKIP).astype(f32), steps)
    half_width = 4 * rows_time
    for d in range(8):
        place = (lane + (d % 4) * rows_time).astype(f32)
        angle = steps * jnp.exp(-math.log(10000.0) * place / half_width)
        wave = jax.nn.silu(jnp.cos(angle) if d < 4 else jnp.sin(angle))
        tf_own[d] = jnp.where(line < 2 * n_sam, wave.astype(bf16).astype(f32), 0.0)
    tf_all[pl.ds(me, 1)] = tf_own[pl.ds(me, 1)]
    loaded("sw")
    put_packed(bufs[s_in].at[me], sw[...])
    loaded("so", "to")
    for i in range(lo // 128):
        at, lanes = slice(i * rows_out, (i + 1) * rows_out), slice(i * 128, (i + 1) * 128)
        bufs[out][me, at, :] = so[:, lanes].astype(bf16)
        bufs[t_out][me, at, :] = to[:, lanes].astype(bf16)
    at = slice(lo // 128 * rows_out, (lo // 128 + 1) * rows_out)
    bufs[out][me, at, :] = jnp.concatenate([so[:, lo:], to[:, lo:]], axis=1).astype(bf16)
    loaded("tw")
    put_packed(bufs[t_in].at[me], tw[...])
    loaded("st", "tt")
    pl.semaphore_wait(barrier, 7 + n_rep - 1)

    def cut(seg):
        return bufs[seg].shape[1] // 32 * 16

    def push(seg, orel, t, r_at, start=0, count=None):
        count = bufs[seg].shape[1] if count is None else count
        part = bufs[seg].at[peer(orel), pl.ds(start, count)]
        send(part, part, g_send.at[seg], g_recv.at[seg * 4 + r_at], dp_id(t))

    def landed(seg, r_at, count=1):
        arrive(bufs[seg].at[pl.ds(0, count)], g_recv.at[seg * 4 + r_at])

    def open_gather(seg):
        push(seg, 0, 2, 0)
        push(seg, 0, 4, 1)
        push(seg, 0, 1, 3)
        sent.append((bufs[seg].at[pl.ds(0, 7)], g_send.at[seg]))

    def relay(seg):
        c = cut(seg)
        landed(seg, 0)
        push(seg, 2, 4, 2, 0, c)
        landed(seg, 1)
        push(seg, 4, 2, 2, c, bufs[seg].shape[1] - c)
        push(seg, 2, 1, 3)
        push(seg, 4, 1, 3)

    def relay_far(seg):
        landed(seg, 2)
        push(seg, 6, 1, 3)

    def close_gather(seg):
        landed(seg, 3, 4)

    def place_in(seg, dst):
        half = rows_in // 2
        for o in range(8):
            for i in range(lo // 128):
                dst[o * rows_in : (o + 1) * rows_in, i * 128 : (i + 1) * 128] = bufs[seg][
                    o, i * rows_in : (i + 1) * rows_in, :
                ]
            at = lo // 128 * rows_in
            tail = bufs[seg][o, at : at + half, :]
            dst[o * rows_in : o * rows_in + half, lo:] = tail[:, :rest]
            dst[o * rows_in + half : (o + 1) * rows_in, lo:] = tail[:, rest:]

    def place_out(seg, dst, first):
        for o in range(8):
            to_rows = slice(o * rows_out, (o + 1) * rows_out)
            for i in range(lo // 128):
                dst[to_rows, i * 128 : (i + 1) * 128] = bufs[seg][o, i * rows_out : (i + 1) * rows_out, :]
            at = lo // 128 * rows_out
            dst[to_rows, lo:] = bufs[out][o, at : at + rows_out, :][:, first : first + rest]

    near = (1, 2, 4, 3, 5, 6, 7)
    exchange("tf", lambda t: tf_own.at[peer(t)], lambda t: tf_all.at[me], near, dp_id)
    open_gather(s_in)
    open_gather(t_in)
    st_b, tt_b = st[...].astype(bf16), tt[...].astype(bf16)
    arrive(tf_all.at[pl.ds(0, 7)], r["tf_recv"])
    feats = tf_all[...].reshape(8 * SUB, rows_time).astype(bf16)
    part_s = jnp.dot(feats, st_b, preferred_element_type=f32)
    part_t = jnp.dot(feats, tt_b, preferred_element_type=f32)
    which = lax.rem(lax.broadcasted_iota(jnp.int32, part_s.shape, 0), SUB)
    e_part[...] = jnp.where(which < n_sam, part_s, part_t).reshape(e_part.shape)
    e_in[pl.ds(me, 1)] = e_part[pl.ds(me, 1)]
    exchange("e", lambda t: e_part.at[peer(t)], lambda t: e_in.at[me], near, dp_id)
    relay(s_in)
    open_gather(out)

    ft_all, em_all = r["ft_all"], r["em_all"]
    ft_all[pl.ds(rep, 1)] = jnp.concatenate([tf_all[d, :n_sam, :] for d in range(8)], axis=0).astype(bf16)[None]
    far = (3, 2, 1)
    exchange("ft", lambda j: ft_all.at[rep], lambda j: ft_all.at[rep], far, rep_id)
    start = 0
    for student, target in ((sw, tw), (so, to), (st, tt)):
        count = student.shape[0]
        e_all[start : start + count, :] = ema_decay * target[...] + (1.0 - ema_decay) * student[...]
        start += count
    relay(t_in)
    open_gather(t_out)
    loaded("x_s", "sg", "sb")
    relay_far(s_in)

    arrive(e_in.at[pl.ds(0, 7)], r["e_recv"])
    emb = e_in[0]
    for k in range(1, 8):
        emb = emb + e_in[k]

    y_v, normed_v, inv_v, nb_v, nbt_v = (r[k] for k in ("y_v", "normed_v", "inv_v", "nb_v", "nbt_v"))
    hid_v, hidt_v, a_v, b_v, gyb_v, gm_v = (r[k] for k in ("hid_v", "hidt_v", "a_v", "b_v", "gyb_v", "gm_v"))

    def normalise(x_ref, k, shift, gain, bias):
        summed = x_ref[:, pl.ds(k * per, per)].astype(f32).T + shift
        center = summed - jnp.mean(summed, axis=1, keepdims=True)
        inv = lax.rsqrt(jnp.mean(center * center, axis=1, keepdims=True) + 1e-05)
        normed = center * inv
        return summed, inv, normed, (normed * gain + bias).astype(bf16)

    for k in range(n_sam):
        at = pl.ds(k * per, per)
        summed, inv, normed, nb = normalise(x_s, k, emb[k : k + 1], sg[...][None], sb[...][None])
        y_v[at, :], normed_v[at, :], nb_v[at, :] = summed, normed, nb
        inv_v[at, :] = inv
    loaded("x_t", "tg", "tb")
    for k in range(n_sam):
        at = pl.ds(k * per, per)
        summed, inv, normed, nb = normalise(
            x_t, k, emb[n_sam + k : n_sam + k + 1], tg[...][None], tb[...][None]
        )
        y_v[at, :], nbt_v[at, :] = y_v[at, :] - summed, nb
    relay(out)
    close_gather(s_in)
    place_in(s_in, ws_all)

    for k in range(n_sam):
        at = pl.ds(k * per, per)
        gate = contract_last(nb_v[at, :], ws_all[:ff, :])
        up = contract_last(nb_v[at, :], ws_all[ff:, :])
        tangent = jnp.tanh(GATE_C * (gate + 0.044715 * gate * gate * gate))
        half = 0.5 * (1.0 + tangent)
        act = gate * half
        slope = half + 0.5 * gate * (1.0 - tangent * tangent) * GATE_C * (1.0 + 0.134145 * gate * gate)
        a_v[at, :], b_v[at, :] = up * slope, act
        hid_v[at, :] = (act * up).astype(bf16)
        if k == 0:
            relay_far(t_in)
    relay(t_out)
    relay_far(out)
    close_gather(t_in)
    place_in(t_in, wt_all)
    for k in range(n_sam):
        at = pl.ds(k * per, per)
        gate = contract_last(nbt_v[at, :], wt_all[:ff, :])
        up = contract_last(nbt_v[at, :], wt_all[ff:, :])
        hidt_v[at, :] = (gelu_tanh(gate) * up).astype(bf16)
    close_gather(out)
    place_out(out, os_all, 0)
    relay_far(t_out)
    for k in range(n_sam):
        at = pl.ds(k * per, per)
        y_v[at, :] = y_v[at, :] + jnp.dot(hid_v[at, :], os_all[...], preferred_element_type=f32)
    close_gather(t_out)
    place_out(t_out, ot_all, rest)
    for k in range(n_sam):
        at = pl.ds(k * per, per)
        gy = (y_v[at, :] - jnp.dot(hidt_v[at, :], ot_all[...], preferred_element_type=f32)) * (1.0 / tokens)
        y_v[at, :], gyb_v[at, :] = gy, gy.astype(bf16)

    r1_o, r1_i = r["r1_o"], r["r1_i"]
    blocks = {
        "o": (r["gs_o"], r1_o, rows_out, 0),
        "a": (r["gs_i"], r1_i, rows_in, 0),
        "b": (r["gs_i"], r1_i, rows_in, rows_out),
    }

    def to_core(src, dst, count, q, key):
        part = src.at[pl.ds(pl.multiple_of((2 * q + 1 - core) * count, 16), count)]
        send(part, dst.at[q], r[key + "_send"], r[key + "_recv"], dp_id(1))

    def pair(key, rel):
        g, r1, count, first = blocks[key]
        owner = peer(rel)
        own = g[pl.ds(pl.multiple_of(owner * count + first, 16), rows_out), :]
        return own + r1[lax.div(owner, 2), first : first + rows_out, :].astype(f32)

    def to_chip(key, k):
        s2, r2 = r["s2_" + key], r["r2_" + key]
        put_packed(s2.at[k], pair(key, 2 * k))
        send(s2.at[k], r2.at[k], r["r2s_" + key], r["r2r_" + key], dp_id(2 * k))

    total_out = contract_first(hid_v[...], gyb_v[...])
    r["gs_o"][...] = total_out
    r["gb_o"][...] = total_out.astype(bf16)
    for q in range(4):
        to_core(r["gb_o"], r1_o, rows_out, q, "c0")

    for k in range(n_sam):
        at = pl.ds(k * per, per)
        gh = contract_last(gyb_v[at, :], os_all[...])
        gm_v[0, at, :], gm_v[1, at, :] = (gh * a_v[at, :]).astype(bf16), (gh * b_v[at, :]).astype(bf16)

    def weight_grad(turn):
        h = 1 - row if turn == 0 else row
        total = contract_first(gm_v[h], nb_v[...])
        at = pl.ds(pl.multiple_of(h * ff, 16), ff)
        r["gs_i"][at, :], r["gb_i"][at, :] = total, total.astype(bf16)
        for q in range(2):
            to_core(r["gb_i"], r1_i, rows_in, 2 * h + q, "c" + str(1 + turn))

    grad_gain = jnp.zeros((1, width), f32)
    grad_bias = grad_gain
    embs = []
    small, small_rep = r["small"], r["small_rep"]

    def input_grad(k):
        at = pl.ds(k * per, per)
        gz = jnp.dot(gm_v[0, at, :], ws_all[:ff, :], preferred_element_type=f32) + jnp.dot(
            gm_v[1, at, :], ws_all[ff:, :], preferred_element_type=f32
        )
        normed = normed_v[at, :]
        gn = gz * sg[...][None]
        gs = y_v[at, :] + inv_v[at, :] * (
            gn
            - jnp.mean(gn, axis=1, keepdims=True)
            - normed * jnp.mean(gn * normed, axis=1, keepdims=True)
        )
        embs.append(jnp.sum(gs, axis=0, keepdims=True))
        return jnp.sum(gz * normed, axis=0, keepdims=True), jnp.sum(gz, axis=0, keepdims=True)

    weight_grad(0)
    arrive(r1_o, r["c0_recv"])
    z_v, zb_v, rz_v = r["z_v"], r["zb_v"], r["rz_v"]
    share = rz_v.shape[2]
    for q in range(4):
        own = r["gs_o"][pl.ds(pl.multiple_of((2 * q + core) * rows_out, 16), rows_out), :]
        put_packed(z_v.at[q], own + r1_o[q].astype(f32))
        z_v[q, packed_out:, :] = jnp.zeros((z_v.shape[1] - packed_out, 128), f32)
        for j in range(n_rep):
            zb_v[j, q] = z_v[q, j * share : (j + 1) * share, :].astype(bf16)
    exchange("rz", lambda j: zb_v.at[rep_peer(j)], lambda j: rz_v.at[j], far, rep_id)
    weight_grad(1)
    for k in range(n_sam):
        more_gain, more_bias = input_grad(k)
        grad_gain, grad_bias = grad_gain + more_gain, grad_bias + more_bias
        if k == 0:
            arrive(r1_i.at[pl.ds(0, 2)], r["c1_recv"])
            to_chip("a", 3)
            to_chip("a", 2)
    arrive(r1_i.at[pl.ds(0, 2)], r["c2_recv"])
    to_chip("a", 1)
    high = [v.astype(bf16).astype(f32) for v in (grad_gain, grad_bias)]
    low = [v - h for v, h in zip((grad_gain, grad_bias), high)]
    n_small = n_sam + 4
    r["pack_v"][...] = jnp.zeros(r["pack_v"].shape, f32)
    put_packed(r["pack_v"], jnp.concatenate(embs + high + low, axis=0))
    small[pl.ds(me, 1)] = r["pack_v"][...].astype(bf16)[None]
    exchange("sm", lambda t: small.at[me], lambda t: small.at[me], near, dp_id)
    for k in (3, 2, 1):
        to_chip("b", k)
    for key in "ab":
        put_packed(r["p_" + key], pair(key, 0))

    def to_planes(key):
        p, pb, r2, r3 = r["p_" + key], r["pb_" + key], r["r2_" + key], r["r3_" + key]
        used, share = r2.shape[1], pb.shape[1]
        arrive(r2.at[pl.ds(1, 3)], r["r2r_" + key])
        p[:used, :] = p[:used, :] + r2[1].astype(f32) + r2[2].astype(f32) + r2[3].astype(f32)
        p[used:, :] = jnp.zeros((p.shape[0] - used, 128), f32)
        for q in range(n_rep):
            pb[q] = p[q * share : (q + 1) * share, :].astype(bf16)
        for j in far:
            send(pb.at[rep_peer(j)], r3.at[j], r["r3s_" + key], r["r3r_" + key], rep_id(j))

    def plane_total():
        arrive(rz_v.at[pl.ds(1, 3)], r["rz_recv"])
        tz_v, tzb_v = r["tz_v"], r["tzb_v"]
        for q in range(4):
            total = z_v[q, pl.ds(pl.multiple_of(rep * share, 8), share), :]
            for j in range(1, n_rep):
                total = total + rz_v[j, q].astype(f32)
            tz_v[q], tzb_v[q] = total, total.astype(bf16)
        exchange(
            "r2z", lambda k: tzb_v.at[lax.div(peer(2 * k), 2)], lambda k: r["r2z_v"].at[k], (3, 1, 2),
            lambda k: dp_id(2 * k),
        )

    def chip_total():
        arrive(r["r2z_v"].at[pl.ds(1, 3)], r["r2z_recv"])
        total = r["tz_v"][lax.div(me, 2)]
        for k in (1, 2, 3):
            total = total + r["r2z_v"][k].astype(f32)
        spread("o", total)

    def spread(key, total):
        fin = r["fin_" + key]
        fin[pl.ds(rep, 1)] = total.astype(bf16)[None]
        for j in far:
            send(fin.at[rep], fin.at[rep], r["r4s_" + key], r["r4r_" + key], rep_id(j))

    def share_total(key):
        p, r3, fin = r["p_" + key], r["r3_" + key], r["fin_" + key]
        share = fin.shape[1]
        total = p[pl.ds(pl.multiple_of(rep * share, 8), share), :]
        arrive(r3.at[pl.ds(1, 3)], r["r3r_" + key])
        for j in range(1, n_rep):
            total = total + r3[j].astype(f32)
        spread(key, total)

    def finish(start, grad):
        at = slice(start, start + grad.shape[0])
        g_all[at, :] = grad
        e_all[at, :] = e_all[at, :] - (1.0 - ema_decay) * learn_rate * grad

    def collect(key, start):
        p, fin = r["p_" + key], r["fin_" + key]
        share = fin.shape[1]
        arrive(fin.at[pl.ds(0, 3)], r["r4r_" + key])
        for q in range(n_rep):
            p[q * share : (q + 1) * share, :] = fin[q].astype(f32)
        finish(start, unpacked(p[...], rows_out, width))

    to_planes("a")
    arrive(small.at[pl.ds(0, 7)], r["sm_recv"])
    part = [small[d].astype(f32) for d in range(8)]
    em_all[pl.ds(rep, 1)] = jnp.concatenate(
        [unpacked(p, n_small, width)[:n_sam] for p in part], axis=0
    ).astype(bf16)[None]
    sums = part[0]
    for k in range(1, 8):
        sums = sums + part[k]
    sums = unpacked(sums, n_small, width)
    sums = sums[n_sam : n_sam + 2] + sums[n_sam + 2 : n_sam + 4]
    high = sums.astype(bf16).astype(f32)
    put_packed(r["pack_v"], jnp.concatenate([high, sums - high], axis=0))
    small_rep[pl.ds(rep, 1)] = r["pack_v"][...].astype(bf16)[None]
    exchange("em", lambda j: em_all.at[rep], lambda j: em_all.at[rep], far, rep_id)
    exchange("rs", lambda j: small_rep.at[rep], lambda j: small_rep.at[rep], far, rep_id)
    plane_total()
    to_planes("b")
    share_total("a")
    chip_total()
    arrive(ft_all.at[pl.ds(0, 3)], r["ft_recv"])
    arrive(em_all.at[pl.ds(0, 3)], r["em_recv"])
    arrive(small_rep.at[pl.ds(0, 3)], r["rs_recv"])
    grad_time = contract_first(ft_all[0], em_all[0])
    sums = jnp.zeros((2, width), f32)
    for j in range(n_rep):
        part = unpacked(small_rep[j].astype(f32), 4, width)
        sums = sums + part[:2] + part[2:]
    for j in range(1, n_rep):
        grad_time = grad_time + contract_first(ft_all[j], em_all[j])
    finish(rows_in + rows_out, grad_time)
    gg, gb = sums[0, :], sums[1, :]
    r["gg_o"][...], r["gb_o_"][...] = gg, gb
    r["eg_o"][...] = average(tg[...], sg[...], gg)
    r["eb_o"][...] = average(tb[...], sb[...], gb)
    share_total("b")
    collect("o", rows_in)
    collect("a", 0)
    collect("b", rows_out)
    for key, ref in (("tf", tf_all), ("e", e_in), ("sm", small)):
        sent.append((ref.at[pl.ds(0, 7)], r[key + "_send"]))
    for key, ref in (("ft", ft_all), ("em", em_all), ("rs", small_rep)):
        sent.append((ref.at[pl.ds(0, 3)], r[key + "_send"]))
    sent += [(r1_o, r["c0_send"]), (r1_i.at[pl.ds(0, 2)], r["c1_send"]), (r1_i.at[pl.ds(0, 2)], r["c2_send"])]
    for key in "ab":
        sent.append((r["r2_" + key].at[pl.ds(0, 3)], r["r2s_" + key]))
        sent.append((r["r3_" + key].at[pl.ds(0, 3)], r["r3s_" + key]))
    sent += [(rz_v.at[pl.ds(0, 3)], r["rz_send"]), (r["r2z_v"].at[pl.ds(0, 3)], r["r2z_send"])]
    for key in "oab":
        sent.append((r["fin_" + key].at[pl.ds(0, 3)], r["r4s_" + key]))
    for ref, sem in sent:
        bytes_of(ref, sem).wait_send()


LOADED = ("ts", "sw", "so", "to", "tw", "st", "tt", "x_s", "sg", "sb", "x_t", "tg", "tb")


def average(target_p, student_p, grad_p):
    return ema_decay * target_p + (1.0 - ema_decay) * (student_p - learn_rate * grad_p)


def output_kernel(grads, means, gg, gb, eg, eb, gw_o, go_o, gt_o, gg_o, gb_o, ew_o, eo_o, et_o, eg_o, eb_o, sem):
    copies = []
    for src, outs in ((grads, (gw_o, go_o, gt_o)), (means, (ew_o, eo_o, et_o))):
        start = 0
        for dst in outs:
            copies.append((src.at[pl.ds(start, dst.shape[0])], dst))
            start += dst.shape[0]
    copies += [(gg, gg_o), (gb, gb_o), (eg, eg_o), (eb, eb_o)]
    copies = [pltpu.make_async_copy(src, dst, sem.at[i]) for i, (src, dst) in enumerate(copies)]
    for copy in copies:
        copy.start()
    for copy in copies:
        copy.wait()


def fused_device(n_dp, n_rep, *args):
    (student_in, target_in, timesteps, sw, so, st, sg, sb, tw, to, tt, tg, tb) = args
    f32, bf16 = jnp.float32, jnp.bfloat16
    tokens, width = student_in.shape
    n_sam = timesteps.shape[0]
    rows_in, rows_out, rows_time = sw.shape[0], so.shape[0], st.shape[0]
    ff = rows_out * n_dp
    rows_all = rows_in + rows_out + rows_time
    vm = pltpu.VMEM
    dma = pltpu.SemaphoreType.DMA
    full = width // 128
    rows_small = -(-((n_sam + 4) * full + (n_sam + 4) // 2) // 16) * 16
    packed_in, packed_out = rows_in * full + rows_in // 2, rows_out * full + rows_out // 2
    share = -(-packed_out // (8 * n_rep)) * 8
    scratch = dict(
        ts=pltpu.SMEM((n_sam,), jnp.int32),
        sw=vm(sw.shape, f32), so=vm(so.shape, f32), st=vm(st.shape, f32),
        tw=vm(tw.shape, f32), to=vm(to.shape, f32), tt=vm(tt.shape, f32),
        sg=vm(sg.shape, f32), sb=vm(sb.shape, f32), tg=vm(tg.shape, f32), tb=vm(tb.shape, f32),
        x_s=vm((width, tokens), bf16), x_t=vm((width, tokens), bf16),
        p_sin=vm((n_dp, packed_in, 128), bf16), p_out=vm((n_dp, rows_out * (full + 1), 128), bf16),
        p_tin=vm((n_dp, packed_in, 128), bf16), p_tout=vm((n_dp, rows_out * full, 128), bf16),
        ws_all=vm((n_dp * rows_in, width), bf16), os_all=vm((ff, width), bf16),
        wt_all=vm((n_dp * rows_in, width), bf16), ot_all=vm((ff, width), bf16),
        tf_own=vm((n_dp, SUB, rows_time), f32), tf_all=vm((n_dp, SUB, rows_time), f32),
        e_part=vm((n_dp, SUB, width), f32), e_in=vm((n_dp, SUB, width), f32),
        small=vm((n_dp, rows_small, 128), bf16), pack_v=vm((rows_small, 128), f32), small_rep=vm((n_rep, rows_small, 128), bf16),
        ft_all=vm((n_rep, n_dp * n_sam, rows_time), bf16), em_all=vm((n_rep, n_dp * n_sam, width), bf16),
        normed_v=vm((tokens, width), f32), inv_v=vm((tokens, 1), f32), nb_v=vm((tokens, width), bf16),
        hid_v=vm((tokens, ff), bf16), hidt_v=vm((tokens, ff), bf16), a_v=vm((tokens, ff), f32), b_v=vm((tokens, ff), f32),
        y_v=vm((tokens, width), f32), nbt_v=vm((tokens, width), bf16), gyb_v=vm((tokens, width), bf16),
        gm_v=vm((2, tokens, ff), bf16),
        gs_i=vm((n_dp * rows_in, width), f32), gs_o=vm((ff, width), f32),
        gb_i=vm((n_dp * rows_in, width), bf16), gb_o=vm((ff, width), bf16),
        r1_i=vm((4, rows_in, width), bf16), r1_o=vm((4, rows_out, width), bf16),
        ld_sem=dma((len(LOADED),)), g_send=dma((4,)), g_recv=dma((16,)),
    )
    for key in "oab":
        scratch["p_" + key] = vm((n_rep * share, 128), f32)
        scratch["fin_" + key] = vm((n_rep, share, 128), bf16)
        scratch["r4s_" + key], scratch["r4r_" + key] = dma, dma
    for key in "ab":
        for name in ("s2_", "r2_"):
            scratch[name + key] = vm((4, packed_out, 128), bf16)
        for name in ("pb_", "r3_"):
            scratch[name + key] = vm((n_rep, share, 128), bf16)
        for name in ("r2", "r3"):
            scratch[name + "s_" + key], scratch[name + "r_" + key] = dma, dma
    scratch["z_v"] = vm((4, n_rep * share, 128), f32)
    for name in ("zb_v", "rz_v"):
        scratch[name] = vm((n_rep, 4, share, 128), bf16)
    scratch["tz_v"] = vm((4, share, 128), f32)
    for name in ("tzb_v", "r2z_v"):
        scratch[name] = vm((4, share, 128), bf16)
    for key in ("tf", "e", "sm", "ft", "em", "rs", "c0", "c1", "c2", "rz", "r2z"):
        scratch[key + "_send"], scratch[key + "_recv"] = dma, dma
    shape = jax.ShapeDtypeStruct
    results = dict(
        g_o=shape((rows_all, width), f32), e_o=shape((rows_all, width), f32), gg_o=shape((width,), f32),
        gb_o_=shape((width,), f32), eg_o=shape((width,), f32), eb_o=shape((width,), f32),
    )
    operands = dict(
        ts=timesteps, sw=sw, so=so, to=to, tw=tw, st=st, tt=tt, x_s=student_in.T, sg=sg, sb=sb,
        x_t=target_in.T, tg=tg, tb=tb,
    )
    names = tuple(key + "_h" for key in operands) + tuple(results) + tuple(scratch)
    values = pl.pallas_call(
        functools.partial(fused_kernel, n_rep, n_sam, names),
        out_shape=tuple(results.values()),
        in_specs=[pl.BlockSpec(memory_space=pltpu.HBM)] * len(operands),
        out_specs=[pl.BlockSpec(memory_space=vm)] * len(results),
        scratch_shapes=list(scratch.values()),
        compiler_params=pltpu.CompilerParams(
            collective_id=0, has_side_effects=True, vmem_limit_bytes=40 * 1024 * 1024
        ),
        name="distill_step",
    )(*(pltpu.with_memory_space_constraint(value, pltpu.HBM) for value in operands.values()))
    big = [shape(w.shape, f32) for w in (sw, so, st)]
    flat = [shape((width,), f32)] * 2
    return tuple(
        pl.pallas_call(
            output_kernel,
            out_shape=(*big, *flat, *big, *flat),
            in_specs=[pl.BlockSpec(memory_space=vm)] * len(results),
            out_specs=[pl.BlockSpec(memory_space=pltpu.HBM)] * 10,
            scratch_shapes=[dma((10,))],
            compiler_params=pltpu.CompilerParams(vmem_limit_bytes=8 * 1024 * 1024),
            name="output_step",
        )(*values)
    )


def fits_fused(n_dp, n_rep, args):
    tokens, samples = args[0].shape[0], args[2].shape[0]
    n_dev = n_dp * n_rep
    rows = [args[i].shape[0] for i in (3, 4, 5)]
    return (
        n_dp == 8
        and n_rep == 4
        and samples % n_dev == 0
        and 2 * (samples // n_dev) + 0 <= SUB
        and (samples // n_dev) % 2 == 0
        and tokens % samples == 0
        and (tokens // samples) % 128 == 0
        and all(r % (16 * n_dp) == 0 for r in rows)
        and all(r % (32 * n_dp) == 0 for r in rows[:1])
        and rows[0] == 2 * rows[1]
        and rows[2] == rows[1]
        and args[0].shape[1] % 128 == 64
    )


def solution(mesh):
    in_specs = (
        P(("dp", "rep"), None),
        P(("dp", "rep"), None),
        P(("dp", "rep")),
        P("dp", None),
        P("dp", None),
        P("dp", None),
        P(),
        P(),
        P("dp", None),
        P("dp", None),
        P("dp", None),
        P(),
        P(),
    )
    out_specs = (
        P("dp", None),
        P("dp", None),
        P("dp", None),
        P(),
        P(),
        P("dp", None),
        P("dp", None),
        P("dp", None),
        P(),
        P(),
    )
    n_dp, n_rep = mesh.shape["dp"], mesh.shape["rep"]

    def step(*args):
        fused = fits_fused(n_dp, n_rep, args)
        body = functools.partial(fused_device, n_dp, n_rep) if fused else per_device
        return jax.shard_map(
            body, mesh=mesh, in_specs=in_specs, out_specs=out_specs, check_vma=False
        )(*args)

    return step
```

```python
import functools
import math

import jax
import jax.numpy as jnp
from jax import lax
from jax.experimental import pallas as pl
from jax.experimental.pallas import tpu as pltpu
from jax.sharding import PartitionSpec as P

MESH = pl.DeviceIdType.MESH
SUB = 8

SKIP = 20


ema_decay = 0.95
learn_rate = 0.05


def sinusoid(step_ids, width):
    half_width = width // 2
    frequency = jnp.exp(-math.log(10000.0) * jnp.arange(half_width, dtype=jnp.float32) / half_width)
    angles = step_ids.astype(jnp.float32)[:, None] * frequency[None, :]
    return jnp.concatenate([jnp.cos(angles), jnp.sin(angles)], axis=1)


def gelu_tanh(value):
    inner = 0.7978845608 * (value + 0.044715 * value * value * value)
    return 0.5 * value * (1.0 + jnp.tanh(inner))


def gelu_slope(value):
    tangent = jnp.tanh(0.7978845608 * (value + 0.044715 * value * value * value))
    return 0.5 * (1.0 + tangent) + 0.5 * value * (1.0 - tangent * tangent) * 0.7978845608 * (
        1.0 + 0.134145 * value * value
    )


def contract_last(left, right):
    return lax.dot_general(
        left, right, (((1,), (1,)), ((), ())), preferred_element_type=jnp.float32
    )


def contract_first(left, right):
    return lax.dot_general(
        left, right, (((0,), (0,)), ((), ())), preferred_element_type=jnp.float32
    )


def forward(tok_rows, step_ids, w_in, w_out, w_time, gain, bias):
    time_feat = jax.nn.silu(sinusoid(step_ids, w_time.shape[0])).astype(jnp.bfloat16)
    embedding = jnp.dot(time_feat, w_time, preferred_element_type=jnp.float32)
    samples = step_ids.shape[0]
    width = tok_rows.shape[1]
    summed = tok_rows.astype(jnp.float32).reshape(samples, -1, width) + embedding[:, None, :]
    summed = summed.reshape(-1, width)
    center = summed - jnp.mean(summed, axis=1, keepdims=True)
    inv_std = lax.rsqrt(jnp.mean(center * center, axis=1, keepdims=True) + 1e-05)
    normed = center * inv_std
    normed_b = (normed * gain + bias).astype(jnp.bfloat16)
    mixed = contract_last(normed_b, w_in)
    hidden_count = w_out.shape[0]
    gate_part = mixed[:, :hidden_count]
    up_part = mixed[:, hidden_count:]
    gelu_gate = gelu_tanh(gate_part)
    hidden = (gelu_gate * up_part).astype(jnp.bfloat16)
    output = summed + jnp.dot(hidden, w_out, preferred_element_type=jnp.float32)
    return (output, (time_feat, normed, inv_std, normed_b, gate_part, up_part, gelu_gate, hidden))


def backward(grad_y, saved, w_in, w_out, gain):
    time_feat, normed, inv_std, normed_b, gate_part, up_part, gelu_gate, hidden = saved
    grad_yb = grad_y.astype(jnp.bfloat16)
    grad_h = contract_last(grad_yb, w_out)
    grad_mix = jnp.concatenate(
        [grad_h * up_part * gelu_slope(gate_part), grad_h * gelu_gate], axis=1
    ).astype(jnp.bfloat16)
    grad_z = jnp.dot(grad_mix, w_in, preferred_element_type=jnp.float32)
    grad_gain = jnp.sum(grad_z * normed, axis=0)
    grad_bias = jnp.sum(grad_z, axis=0)
    grad_n = grad_z * gain
    grad_s = grad_y + inv_std * (
        grad_n
        - jnp.mean(grad_n, axis=1, keepdims=True)
        - normed * jnp.mean(grad_n * normed, axis=1, keepdims=True)
    )
    samples = time_feat.shape[0]
    grad_emb = jnp.sum(grad_s.reshape(samples, -1, grad_s.shape[1]), axis=1)
    grad_time = lax.dot_general(
        time_feat.astype(jnp.float32),
        grad_emb,
        (((0,), (0,)), ((), ())),
        precision=lax.Precision.HIGHEST,
        preferred_element_type=jnp.float32,
    )
    return (grad_yb, grad_mix, grad_gain, grad_bias, grad_time)


def fetch(piece_in, piece_out, piece_time):
    return (
        lax.all_gather(piece_in, "dp", axis=0, tiled=True),
        lax.all_gather(piece_out, "dp", axis=0, tiled=True),
        lax.all_gather(piece_time, "dp", axis=0, tiled=True),
    )


def per_device(
    student_in,
    target_in,
    timesteps,
    student_win,
    student_wout,
    student_wtime,
    student_gain,
    student_bias,
    target_win,
    target_wout,
    target_wtime,
    target_gain,
    target_bias,
):
    s_in, s_out, s_time = fetch(
        student_win.astype(jnp.bfloat16),
        student_wout.astype(jnp.bfloat16),
        student_wtime.astype(jnp.bfloat16),
    )
    student_out, saved = forward(
        student_in, timesteps, s_in, s_out, s_time, student_gain, student_bias
    )
    t_in, t_out, t_time = fetch(
        target_win.astype(jnp.bfloat16),
        target_wout.astype(jnp.bfloat16),
        target_wtime.astype(jnp.bfloat16),
    )
    target_out, unused = forward(
        target_in, timesteps - SKIP, t_in, t_out, t_time, target_gain, target_bias
    )
    grad_y = (student_out - target_out) / student_in.shape[0]
    back_in, back_out = (
        lax.all_gather(student_win.astype(jnp.bfloat16), "dp", axis=0, tiled=True),
        lax.all_gather(student_wout.astype(jnp.bfloat16), "dp", axis=0, tiled=True),
    )
    grad_yb, grad_mix, grad_gain, grad_bias, grad_time = backward(
        grad_y, saved, back_in, back_out, student_gain
    )
    normed_b = saved[3]
    hidden = saved[7]
    part = grad_mix
    shard_in = lax.psum_scatter(
        contract_first(part, normed_b), "dp", scatter_dimension=0, tiled=True
    )
    part = hidden
    shard_out = lax.psum_scatter(
        contract_first(part, grad_yb), "dp", scatter_dimension=0, tiled=True
    )
    shard_time = lax.psum_scatter(grad_time, "dp", scatter_dimension=0, tiled=True)
    shard_in, shard_out, shard_time = lax.psum((shard_in, shard_out, shard_time), "rep")
    total_gain, total_bias = lax.psum((grad_gain, grad_bias), ("dp", "rep"))

    def average(target_p, student_p, grad_p):
        return ema_decay * target_p + (1.0 - ema_decay) * (student_p - learn_rate * grad_p)

    return (
        shard_in,
        shard_out,
        shard_time,
        total_gain,
        total_bias,
        average(target_win, student_win, shard_in),
        average(target_wout, student_wout, shard_out),
        average(target_wtime, student_wtime, shard_time),
        average(target_gain, student_gain, total_gain),
        average(target_bias, student_bias, total_bias),
    )


GATE_C = 0.7978845608


def put_packed(ref, value):
    rows, lo = value.shape[0], value.shape[1] // 128 * 128
    for i in range(lo // 128):
        ref[i * rows : (i + 1) * rows, :] = value[:, i * 128 : (i + 1) * 128].astype(ref.dtype)
    at, half = lo // 128 * rows, rows // 2
    rest = jnp.concatenate([value[:half, lo:], value[half:, lo:]], axis=1)
    ref[at : at + half, :] = rest.astype(ref.dtype)


def unpacked(value, rows, width):
    lo = width // 128 * 128
    at, half, rest = lo // 128 * rows, rows // 2, width - lo
    parts = [value[i * rows : (i + 1) * rows] for i in range(lo // 128)]
    tail = value[at : at + half]
    parts.append(jnp.concatenate([tail[:, :rest], tail[:, rest:]], axis=0))
    return jnp.concatenate(parts, axis=1)


def in_pieces(rows):
    big = rows * 2 // 5 // 16 * 16
    return {"a": (0, big), "b": (big, big), "c": (2 * big, rows - 2 * big)}


def fused_kernel(n_rep, n_sam, names, *refs):
    r = dict(zip(names, refs))
    f32, bf16 = jnp.float32, jnp.bfloat16
    me, rep = lax.axis_index("dp"), lax.axis_index("rep")
    core, col, row = lax.rem(me, 2), lax.rem(lax.div(me, 2), 2), lax.div(me, 4)
    sw, so, st, tw, to, tt = (r[k] for k in ("sw", "so", "st", "tw", "to", "tt"))
    sg, sb, tg, tb, x_s, x_t = (r[k] for k in ("sg", "sb", "tg", "tb", "x_s", "x_t"))
    rows_in, rows_out, rows_time = sw.shape[0], so.shape[0], st.shape[0]
    pieces = in_pieces(rows_in)
    width, tokens = x_s.shape
    per = tokens // n_sam
    lo = width // 128 * 128
    rest = width - lo
    ws_all, os_all, wt_all, ot_all = (r[k] for k in ("ws_all", "os_all", "wt_all", "ot_all"))
    ff = os_all.shape[0]
    tf_own, tf_all, e_part, e_in = (r[k] for k in ("tf_own", "tf_all", "e_part", "e_in"))
    g_all, e_all = r["g_o"], r["e_o"]

    flip = lambda b, on: 1 - b if on else b

    def peer(t):
        return flip(row, t & 4) * 4 + flip(col, t & 2) * 2 + flip(core, t & 1)

    def dp_id(t):
        return {"dp": peer(t)}

    def rep_peer(j):
        return flip(lax.div(rep, 2), j & 2) * 2 + flip(lax.rem(rep, 2), j & 1)

    def rep_id(j):
        return {"rep": rep_peer(j)}

    barrier = pltpu.get_barrier_semaphore()
    for t in range(1, 8):
        pl.semaphore_signal(barrier, inc=1, device_id=dp_id(t), device_id_type=MESH)
    for j in range(1, n_rep):
        pl.semaphore_signal(barrier, inc=1, device_id=rep_id(j), device_id_type=MESH)

    loads = []
    for i, name in enumerate(LOADED):
        copy = pltpu.make_async_copy(r[name + "_h"], r[name], r["ld_sem"].at[i])
        copy.start()
        loads.append(copy)

    def loaded(*keys):
        for key in keys:
            loads[LOADED.index(key)].wait()

    def send(src, dst, s_sem, r_sem, where):
        pltpu.make_async_remote_copy(
            src_ref=src, dst_ref=dst, send_sem=s_sem, recv_sem=r_sem,
            device_id=where, device_id_type=MESH,
        ).start()

    def bytes_of(ref, sem):
        return pltpu.make_async_remote_copy(
            src_ref=ref, dst_ref=ref, send_sem=sem, recv_sem=sem,
            device_id=dp_id(1), device_id_type=MESH,
        )

    def arrive(ref, sem):
        bytes_of(ref, sem).wait_recv()

    sent = []

    def exchange(key, source, slots, peers, where):
        for j in peers:
            src, dst = source(j), slots(j)
            send(src, dst, r[key + "_send"], r[key + "_recv"], where(j))

    bufs = (r["p_sin"], r["p_out"], r["p_tin"], r["p_tout"])
    s_in, out, t_in, t_out = range(4)
    g_send, g_recv = r["g_send"], r["g_recv"]
    loaded("ts")
    line = lax.broadcasted_iota(jnp.int32, (SUB, rows_time), 0)
    lane = lax.broadcasted_iota(jnp.int32, (SUB, rows_time), 1)
    steps = jnp.zeros((SUB, rows_time), f32)
    for k in range(n_sam):
        value = r["ts"][k]
        steps = jnp.where(line == k, value.astype(f32), steps)
        steps = jnp.where(line == n_sam + k, (value - SKIP).astype(f32), steps)
    half_width = 4 * rows_time
    for d in range(8):
        place = (lane + (d % 4) * rows_time).astype(f32)
        angle = steps * jnp.exp(-math.log(10000.0) * place / half_width)
        wave = jax.nn.silu(jnp.cos(angle) if d < 4 else jnp.sin(angle))
        tf_own[d] = jnp.where(line < 2 * n_sam, wave.astype(bf16).astype(f32), 0.0)
    tf_all[pl.ds(me, 1)] = tf_own[pl.ds(me, 1)]
    loaded("sw")
    put_packed(bufs[s_in].at[me], sw[...])
    loaded("so", "to")
    for i in range(lo // 128):
        at, lanes = slice(i * rows_out, (i + 1) * rows_out), slice(i * 128, (i + 1) * 128)
        bufs[out][me, at, :] = so[:, lanes].astype(bf16)
        bufs[t_out][me, at, :] = to[:, lanes].astype(bf16)
    at = slice(lo // 128 * rows_out, (lo // 128 + 1) * rows_out)
    bufs[out][me, at, :] = jnp.concatenate([so[:, lo:], to[:, lo:]], axis=1).astype(bf16)
    loaded("tw")
    put_packed(bufs[t_in].at[me], tw[...])
    loaded("st", "tt")
    pl.semaphore_wait(barrier, 7 + n_rep - 1)

    def cut(seg):
        return bufs[seg].shape[1] // 32 * 16

    def push(seg, orel, t, r_at, start=0, count=None):
        count = bufs[seg].shape[1] if count is None else count
        part = bufs[seg].at[peer(orel), pl.ds(start, count)]
        send(part, part, g_send.at[seg], g_recv.at[seg * 6 + r_at], dp_id(t))

    def landed(seg, r_at, count=1):
        arrive(bufs[seg].at[pl.ds(0, count)], g_recv.at[seg * 6 + r_at])

    def landed_rows(seg, r_at, count):
        arrive(bufs[seg].at[0, pl.ds(0, count)], g_recv.at[seg * 6 + r_at])

    def open_gather(seg):
        c = cut(seg)
        d = bufs[seg].shape[1] - c
        push(seg, 0, 2, 0, 0, c)
        push(seg, 0, 4, 1, c, d)
        push(seg, 0, 2, 4, c, d)
        push(seg, 0, 4, 5, 0, c)
        push(seg, 0, 1, 3)
        sent.append((bufs[seg].at[pl.ds(0, 7)], g_send.at[seg]))

    def relay(seg):
        c = cut(seg)
        d = bufs[seg].shape[1] - c
        landed_rows(seg, 0, c)
        push(seg, 2, 4, 2, 0, c)
        landed_rows(seg, 1, d)
        push(seg, 4, 2, 2, c, d)

    def relay_near(seg):
        c = cut(seg)
        landed_rows(seg, 4, bufs[seg].shape[1] - c)
        push(seg, 2, 1, 3)
        landed_rows(seg, 5, c)
        push(seg, 4, 1, 3)

    def relay_far(seg):
        landed(seg, 2)
        push(seg, 6, 1, 3)

    def close_gather(seg):
        landed(seg, 3, 4)

    def place_in(seg, dst):
        half = rows_in // 2
        for o in range(8):
            for i in range(lo // 128):
                dst[o * rows_in : (o + 1) * rows_in, i * 128 : (i + 1) * 128] = bufs[seg][
                    o, i * rows_in : (i + 1) * rows_in, :
                ]
            at = lo // 128 * rows_in
            tail = bufs[seg][o, at : at + half, :]
            dst[o * rows_in : o * rows_in + half, lo:] = tail[:, :rest]
            dst[o * rows_in + half : (o + 1) * rows_in, lo:] = tail[:, rest:]

    def place_out(seg, dst, first):
        for o in range(8):
            to_rows = slice(o * rows_out, (o + 1) * rows_out)
            for i in range(lo // 128):
                dst[to_rows, i * 128 : (i + 1) * 128] = bufs[seg][o, i * rows_out : (i + 1) * rows_out, :]
            at = lo // 128 * rows_out
            dst[to_rows, lo:] = bufs[out][o, at : at + rows_out, :][:, first : first + rest]

    near = (1, 2, 4, 3, 5, 6, 7)
    exchange("tf", lambda t: tf_own.at[peer(t)], lambda t: tf_all.at[me], near, dp_id)
    open_gather(s_in)
    open_gather(t_in)
    st_b, tt_b = st[...].astype(bf16), tt[...].astype(bf16)
    arrive(tf_all.at[pl.ds(0, 7)], r["tf_recv"])
    feats = tf_all[...].reshape(8 * SUB, rows_time).astype(bf16)
    part_s = jnp.dot(feats, st_b, preferred_element_type=f32)
    part_t = jnp.dot(feats, tt_b, preferred_element_type=f32)
    which = lax.rem(lax.broadcasted_iota(jnp.int32, part_s.shape, 0), SUB)
    part = jnp.where(which < n_sam, part_s, part_t)
    for d in range(8):
        put_packed(e_part.at[d], part[d * SUB : d * SUB + 2 * n_sam])
    e_in[pl.ds(me, 1)] = e_part[pl.ds(me, 1)]
    exchange("e", lambda t: e_part.at[peer(t)], lambda t: e_in.at[me], near, dp_id)
    relay(s_in)
    open_gather(out)
    open_gather(t_out)

    ft_all, em_all = r["ft_all"], r["em_all"]
    ft_all[pl.ds(rep, 1)] = jnp.concatenate([tf_all[d, :n_sam, :] for d in range(8)], axis=0).astype(bf16)[None]
    far = (3, 2, 1)
    exchange("ft", lambda j: ft_all.at[rep], lambda j: ft_all.at[rep], far, rep_id)
    start = 0
    for student, target in ((sw, tw), (so, to), (st, tt)):
        count = student.shape[0]
        e_all[start : start + count, :] = ema_decay * target[...] + (1.0 - ema_decay) * student[...]
        start += count
    relay(t_in)
    relay_near(s_in)
    loaded("x_s", "sg", "sb")

    arrive(e_in.at[pl.ds(0, 7)], r["e_recv"])
    emb = e_in[0]
    for k in range(1, 8):
        emb = emb + e_in[k]
    emb = unpacked(emb, 2 * n_sam, width)

    y_v, normed_v, inv_v, nb_v, nbt_v = (r[k] for k in ("y_v", "normed_v", "inv_v", "nb_v", "nbt_v"))
    hid_v, hidt_v, a_v, b_v, gyb_v, gm_v = (r[k] for k in ("hid_v", "hidt_v", "a_v", "b_v", "gyb_v", "gm_v"))

    def normalise(x_ref, k, shift, gain, bias):
        summed = x_ref[:, pl.ds(k * per, per)].astype(f32).T + shift
        center = summed - jnp.mean(summed, axis=1, keepdims=True)
        inv = lax.rsqrt(jnp.mean(center * center, axis=1, keepdims=True) + 1e-05)
        normed = center * inv
        return summed, inv, normed, (normed * gain + bias).astype(bf16)

    for k in range(n_sam):
        at = pl.ds(k * per, per)
        summed, inv, normed, nb = normalise(x_s, k, emb[k : k + 1], sg[...][None], sb[...][None])
        y_v[at, :], normed_v[at, :], nb_v[at, :] = summed, normed, nb
        inv_v[at, :] = inv
    relay_far(s_in)
    relay(out)
    relay_near(t_in)
    loaded("x_t", "tg", "tb")
    for k in range(n_sam):
        at = pl.ds(k * per, per)
        summed, inv, normed, nb = normalise(
            x_t, k, emb[n_sam + k : n_sam + k + 1], tg[...][None], tb[...][None]
        )
        y_v[at, :], nbt_v[at, :] = y_v[at, :] - summed, nb
    relay_near(out)
    close_gather(s_in)
    place_in(s_in, ws_all)
    relay(t_out)

    for k in range(n_sam):
        at = pl.ds(k * per, per)
        gate = contract_last(nb_v[at, :], ws_all[:ff, :])
        up = contract_last(nb_v[at, :], ws_all[ff:, :])
        tangent = jnp.tanh(GATE_C * (gate + 0.044715 * gate * gate * gate))
        half = 0.5 * (1.0 + tangent)
        act = gate * half
        slope = half + 0.5 * gate * (1.0 - tangent * tangent) * GATE_C * (1.0 + 0.134145 * gate * gate)
        a_v[at, :], b_v[at, :] = up * slope, act
        hid_v[at, :] = (act * up).astype(bf16)
        if k == 0:
            relay_far(t_in)
            relay_near(t_out)
    relay_far(out)
    close_gather(t_in)
    place_in(t_in, wt_all)
    for k in range(n_sam):
        at = pl.ds(k * per, per)
        gate = contract_last(nbt_v[at, :], wt_all[:ff, :])
        up = contract_last(nbt_v[at, :], wt_all[ff:, :])
        hidt_v[at, :] = (gelu_tanh(gate) * up).astype(bf16)
        if k == 0:
            relay_far(t_out)
    close_gather(out)
    place_out(out, os_all, 0)
    for k in range(n_sam):
        at = pl.ds(k * per, per)
        y_v[at, :] = y_v[at, :] + jnp.dot(hid_v[at, :], os_all[...], preferred_element_type=f32)
    close_gather(t_out)
    place_out(t_out, ot_all, rest)
    for k in range(n_sam):
        at = pl.ds(k * per, per)
        gy = (y_v[at, :] - jnp.dot(hidt_v[at, :], ot_all[...], preferred_element_type=f32)) * (1.0 / tokens)
        y_v[at, :], gyb_v[at, :] = gy, gy.astype(bf16)

    r1_o, r1_i = r["r1_o"], r["r1_i"]

    def to_core(src, dst, count, q, key):
        part = src.at[pl.ds(pl.multiple_of((2 * q + 1 - core) * count, 16), count)]
        send(part, dst.at[q], r[key + "_send"], r[key + "_recv"], dp_id(1))

    def pair(key, rel):
        first, count = pieces[key]
        owner = peer(rel)
        own = r["gs_i"][pl.ds(pl.multiple_of(owner * rows_in + first, 16), count), :]
        return own + r1_i[lax.div(owner, 2), first : first + count, :].astype(f32)

    def to_chip(key, k):
        s2, r2 = r["s2_" + key], r["r2_" + key]
        put_packed(s2.at[k], pair(key, 2 * k))
        send(s2.at[k], r2.at[k], r["r2s_" + key], r["r2r_" + key], dp_id(2 * k))

    total_out = contract_first(hid_v[...], gyb_v[...])
    r["gs_o"][...] = total_out
    r["gb_o"][...] = total_out.astype(bf16)
    for q in range(4):
        to_core(r["gb_o"], r1_o, rows_out, q, "c0")
    for k in range(n_sam):
        at = pl.ds(k * per, per)
        gh = contract_last(gyb_v[at, :], os_all[...])
        gm_v[0, at, :], gm_v[1, at, :] = (gh * a_v[at, :]).astype(bf16), (gh * b_v[at, :]).astype(bf16)

    def weight_grad(turn):
        h = 1 - row if turn == 0 else row
        total = contract_first(gm_v[h], nb_v[...])
        at = pl.ds(pl.multiple_of(h * ff, 16), ff)
        r["gs_i"][at, :], r["gb_i"][at, :] = total, total.astype(bf16)
        for q in range(2):
            to_core(r["gb_i"], r1_i, rows_in, 2 * h + q, "c" + str(1 + turn))

    grad_gain = jnp.zeros((1, width), f32)
    grad_bias = grad_gain
    embs = []
    small, small_rep = r["small"], r["small_rep"]

    def input_grad(k):
        at = pl.ds(k * per, per)
        gz = jnp.dot(gm_v[0, at, :], ws_all[:ff, :], preferred_element_type=f32) + jnp.dot(
            gm_v[1, at, :], ws_all[ff:, :], preferred_element_type=f32
        )
        normed = normed_v[at, :]
        gn = gz * sg[...][None]
        gs = y_v[at, :] + inv_v[at, :] * (
            gn
            - jnp.mean(gn, axis=1, keepdims=True)
            - normed * jnp.mean(gn * normed, axis=1, keepdims=True)
        )
        embs.append(jnp.sum(gs, axis=0, keepdims=True))
        return jnp.sum(gz * normed, axis=0, keepdims=True), jnp.sum(gz, axis=0, keepdims=True)

    weight_grad(0)
    arrive(r1_o, r["c0_recv"])
    pk_v, z_v, zb_v, rz_v = r["pk_v"], r["z_v"], r["zb_v"], r["rz_v"]
    share = pk_v.shape[0] // n_rep
    for q in range(4):
        own = r["gs_o"][pl.ds(pl.multiple_of((2 * q + core) * rows_out, 16), rows_out), :]
        put_packed(pk_v, own + r1_o[q].astype(f32))
        for j in range(n_rep):
            z_v[j, q * share : (q + 1) * share, :] = pk_v[j * share : (j + 1) * share, :]
    for j in range(n_rep):
        zb_v[j] = z_v[j].astype(bf16)
    exchange("rz", lambda j: zb_v.at[rep_peer(j)], lambda j: rz_v.at[j], far, rep_id)
    weight_grad(1)
    arrive(r1_i.at[pl.ds(0, 2)], r["c1_recv"])
    to_chip("a", 3)
    to_chip("a", 2)
    for k in range(n_sam):
        more_gain, more_bias = input_grad(k)
        grad_gain, grad_bias = grad_gain + more_gain, grad_bias + more_bias
        if k == 0:
            arrive(r1_i.at[pl.ds(0, 2)], r["c2_recv"])
            to_chip("a", 1)
            for q in (3, 2, 1):
                to_chip("b", q)
    high = [v.astype(bf16).astype(f32) for v in (grad_gain, grad_bias)]
    low = [v - h for v, h in zip((grad_gain, grad_bias), high)]
    n_small = n_sam + 4
    r["pack_v"][...] = jnp.zeros(r["pack_v"].shape, f32)
    put_packed(r["pack_v"], jnp.concatenate(embs + high + low, axis=0))
    small[pl.ds(me, 1)] = r["pack_v"][...].astype(bf16)[None]
    exchange("sm", lambda t: small.at[me], lambda t: small.at[me], near, dp_id)
    for k in (3, 2, 1):
        to_chip("c", k)
    for key in "abc":
        put_packed(r["p_" + key], pair(key, 0))

    def chips_total(key):
        p, r2 = r["p_" + key], r["r2_" + key]
        arrive(r2.at[pl.ds(1, 3)], r["r2r_" + key])
        p[...] = p[...] + r2[1].astype(f32) + r2[2].astype(f32) + r2[3].astype(f32)
        return p

    def to_planes(key):
        p, pb, r3 = chips_total(key), r["pb_" + key], r["r3_" + key]
        part = pb.shape[1]
        for q in range(n_rep):
            pb[q] = p[q * part : (q + 1) * part, :].astype(bf16)
        for j in far:
            send(pb.at[rep_peer(j)], r3.at[j], r["r3s_" + key], r["r3r_" + key], rep_id(j))

    def to_planes_whole(key):
        r3 = r["r3_" + key]
        r3[pl.ds(rep, 1)] = chips_total(key)[...].astype(bf16)[None]
        for j in far:
            send(r3.at[rep], r3.at[rep], r["r3s_" + key], r["r3r_" + key], rep_id(j))

    def plane_total():
        arrive(rz_v.at[pl.ds(1, 3)], r["rz_recv"])
        tz_v, tzb_v = r["tz_v"], r["tzb_v"]
        total = z_v[rep]
        for j in range(1, n_rep):
            total = total + rz_v[j].astype(f32)
        pk_v[...] = total
        for q in range(4):
            part = pk_v[q * share : (q + 1) * share, :]
            tz_v[q], tzb_v[q] = part, part.astype(bf16)
        exchange(
            "r2z", lambda k: tzb_v.at[lax.div(peer(2 * k), 2)], lambda k: r["r2z_v"].at[k], (3, 1, 2),
            lambda k: dp_id(2 * k),
        )

    def chip_total():
        arrive(r["r2z_v"].at[pl.ds(1, 3)], r["r2z_recv"])
        total = r["tz_v"][lax.div(me, 2)]
        for k in (1, 2, 3):
            total = total + r["r2z_v"][k].astype(f32)
        spread("o", total)

    def spread(key, total):
        fin = r["fin_" + key]
        fin[pl.ds(rep, 1)] = total.astype(bf16)[None]
        for j in far:
            send(fin.at[rep], fin.at[rep], r["r4s_" + key], r["r4r_" + key], rep_id(j))

    def share_total(key):
        p, r3 = r["p_" + key], r["r3_" + key]
        part = r3.shape[1]
        total = p[pl.ds(pl.multiple_of(rep * part, 8), part), :]
        arrive(r3.at[pl.ds(1, 3)], r["r3r_" + key])
        for j in range(1, n_rep):
            total = total + r3[j].astype(f32)
        spread(key, total)

    def finish(start, grad):
        at = slice(start, start + grad.shape[0])
        g_all[at, :] = grad
        e_all[at, :] = e_all[at, :] - (1.0 - ema_decay) * learn_rate * grad

    def collect(key, start, count):
        p, fin = (pk_v if key == "o" else r["p_" + key]), r["fin_" + key]
        part = fin.shape[1]
        arrive(fin.at[pl.ds(0, 3)], r["r4r_" + key])
        for q in range(n_rep):
            p[q * part : (q + 1) * part, :] = fin[q].astype(f32)
        finish(start, unpacked(p[...], count, width))

    def collect_whole(key):
        r3 = r["r3_" + key]
        arrive(r3.at[pl.ds(0, 3)], r["r3r_" + key])
        total = r3[0].astype(f32)
        for j in range(1, n_rep):
            total = total + r3[j].astype(f32)
        first, count = pieces[key]
        finish(first, unpacked(total, count, width))

    to_planes("a")
    to_planes("b")
    arrive(small.at[pl.ds(0, 7)], r["sm_recv"])
    part = [small[d].astype(f32) for d in range(8)]
    put_packed(em_all.at[rep], jnp.concatenate([unpacked(p, n_small, width)[:n_sam] for p in part], axis=0))
    sums = part[0]
    for k in range(1, 8):
        sums = sums + part[k]
    sums = unpacked(sums, n_small, width)
    sums = sums[n_sam : n_sam + 2] + sums[n_sam + 2 : n_sam + 4]
    high = sums.astype(bf16).astype(f32)
    put_packed(r["pack_v"], jnp.concatenate([high, sums - high], axis=0))
    small_rep[pl.ds(rep, 1)] = r["pack_v"][...].astype(bf16)[None]
    exchange("em", lambda j: em_all.at[rep], lambda j: em_all.at[rep], far, rep_id)
    exchange("rs", lambda j: small_rep.at[rep], lambda j: small_rep.at[rep], far, rep_id)
    plane_total()
    to_planes_whole("c")
    share_total("a")
    chip_total()
    share_total("b")
    collect_whole("c")
    arrive(ft_all.at[pl.ds(0, 3)], r["ft_recv"])
    arrive(em_all.at[pl.ds(0, 3)], r["em_recv"])
    arrive(small_rep.at[pl.ds(0, 3)], r["rs_recv"])
    grad_time = jnp.zeros((rows_time, width), f32)
    for j in range(n_rep):
        samples = unpacked(em_all[j].astype(f32), 8 * n_sam, width).astype(bf16)
        grad_time = grad_time + contract_first(ft_all[j], samples)
    sums = jnp.zeros((2, width), f32)
    for j in range(n_rep):
        part = unpacked(small_rep[j].astype(f32), 4, width)
        sums = sums + part[:2] + part[2:]
    finish(rows_in + rows_out, grad_time)
    gg, gb = sums[0, :], sums[1, :]
    r["gg_o"][...], r["gb_o_"][...] = gg, gb
    r["eg_o"][...] = average(tg[...], sg[...], gg)
    r["eb_o"][...] = average(tb[...], sb[...], gb)
    collect("a", *pieces["a"])
    collect("o", rows_in, rows_out)
    collect("b", *pieces["b"])
    for key, ref in (("tf", tf_all), ("e", e_in), ("sm", small)):
        sent.append((ref.at[pl.ds(0, 7)], r[key + "_send"]))
    for key, ref in (("ft", ft_all), ("em", em_all), ("rs", small_rep)):
        sent.append((ref.at[pl.ds(0, 3)], r[key + "_send"]))
    sent += [(r1_o, r["c0_send"]), (r1_i.at[pl.ds(0, 2)], r["c1_send"]), (r1_i.at[pl.ds(0, 2)], r["c2_send"])]
    for key in "abc":
        sent.append((r["r2_" + key].at[pl.ds(0, 3)], r["r2s_" + key]))
        sent.append((r["r3_" + key].at[pl.ds(0, 3)], r["r3s_" + key]))
    sent += [(rz_v.at[pl.ds(0, 3)], r["rz_send"]), (r["r2z_v"].at[pl.ds(0, 3)], r["r2z_send"])]
    for key in "oab":
        sent.append((r["fin_" + key].at[pl.ds(0, 3)], r["r4s_" + key]))
    for ref, sem in sent:
        bytes_of(ref, sem).wait_send()


LOADED = ("ts", "sw", "so", "to", "tw", "st", "tt", "x_s", "sg", "sb", "x_t", "tg", "tb")


def average(target_p, student_p, grad_p):
    return ema_decay * target_p + (1.0 - ema_decay) * (student_p - learn_rate * grad_p)


def output_kernel(grads, means, gg, gb, eg, eb, gw_o, go_o, gt_o, gg_o, gb_o, ew_o, eo_o, et_o, eg_o, eb_o, sem):
    copies = []
    for src, outs in ((grads, (gw_o, go_o, gt_o)), (means, (ew_o, eo_o, et_o))):
        start = 0
        for dst in outs:
            copies.append((src.at[pl.ds(start, dst.shape[0])], dst))
            start += dst.shape[0]
    copies += [(gg, gg_o), (gb, gb_o), (eg, eg_o), (eb, eb_o)]
    copies = [pltpu.make_async_copy(src, dst, sem.at[i]) for i, (src, dst) in enumerate(copies)]
    for copy in copies:
        copy.start()
    for copy in copies:
        copy.wait()


def fused_device(n_dp, n_rep, *args):
    (student_in, target_in, timesteps, sw, so, st, sg, sb, tw, to, tt, tg, tb) = args
    f32, bf16 = jnp.float32, jnp.bfloat16
    tokens, width = student_in.shape
    n_sam = timesteps.shape[0]
    rows_in, rows_out, rows_time = sw.shape[0], so.shape[0], st.shape[0]
    ff = rows_out * n_dp
    rows_all = rows_in + rows_out + rows_time
    vm = pltpu.VMEM
    dma = pltpu.SemaphoreType.DMA
    full = width // 128
    rows_emb = -(-(2 * n_sam * full + n_sam) // SUB) * SUB
    rows_small = -(-((n_sam + 4) * full + (n_sam + 4) // 2) // 16) * 16
    packed_in, packed_out = rows_in * full + rows_in // 2, rows_out * full + rows_out // 2
    scratch = dict(
        ts=pltpu.SMEM((n_sam,), jnp.int32),
        sw=vm(sw.shape, f32), so=vm(so.shape, f32), st=vm(st.shape, f32),
        tw=vm(tw.shape, f32), to=vm(to.shape, f32), tt=vm(tt.shape, f32),
        sg=vm(sg.shape, f32), sb=vm(sb.shape, f32), tg=vm(tg.shape, f32), tb=vm(tb.shape, f32),
        x_s=vm((width, tokens), bf16), x_t=vm((width, tokens), bf16),
        p_sin=vm((n_dp, packed_in, 128), bf16), p_out=vm((n_dp, rows_out * (full + 1), 128), bf16),
        p_tin=vm((n_dp, packed_in, 128), bf16), p_tout=vm((n_dp, rows_out * full, 128), bf16),
        ws_all=vm((n_dp * rows_in, width), bf16), os_all=vm((ff, width), bf16),
        wt_all=vm((n_dp * rows_in, width), bf16), ot_all=vm((ff, width), bf16),
        tf_own=vm((n_dp, SUB, rows_time), f32), tf_all=vm((n_dp, SUB, rows_time), f32),
        e_part=vm((n_dp, rows_emb, 128), f32), e_in=vm((n_dp, rows_emb, 128), f32),
        small=vm((n_dp, rows_small, 128), bf16), pack_v=vm((rows_small, 128), f32), small_rep=vm((n_rep, rows_small, 128), bf16),
        ft_all=vm((n_rep, n_dp * n_sam, rows_time), bf16), em_all=vm((n_rep, n_dp * n_sam * full + n_dp * n_sam // 2, 128), bf16),
        normed_v=vm((tokens, width), f32), inv_v=vm((tokens, 1), f32), nb_v=vm((tokens, width), bf16),
        hid_v=vm((tokens, ff), bf16), hidt_v=vm((tokens, ff), bf16), a_v=vm((tokens, ff), f32), b_v=vm((tokens, ff), f32),
        y_v=vm((tokens, width), f32), nbt_v=vm((tokens, width), bf16), gyb_v=vm((tokens, width), bf16),
        gm_v=vm((2, tokens, ff), bf16),
        gs_i=vm((n_dp * rows_in, width), f32), gs_o=vm((ff, width), f32),
        gb_i=vm((n_dp * rows_in, width), bf16), gb_o=vm((ff, width), bf16),
        r1_i=vm((4, rows_in, width), bf16), r1_o=vm((4, rows_out, width), bf16),
        ld_sem=dma((len(LOADED),)), g_send=dma((4,)), g_recv=dma((24,)),
    )
    for key, (_, count) in in_pieces(rows_in).items():
        packed = count * full + count // 2
        scratch["p_" + key] = vm((packed, 128), f32)
        for name in ("s2_", "r2_"):
            scratch[name + key] = vm((4, packed, 128), bf16)
        scratch["r3_" + key] = vm((n_rep, packed if key == "c" else packed // n_rep, 128), bf16)
        if key != "c":
            scratch["pb_" + key] = vm((n_rep, packed // n_rep, 128), bf16)
        for name in ("r2", "r3"):
            scratch[name + "s_" + key], scratch[name + "r_" + key] = dma, dma
    for key, packed in (("a", scratch["p_a"].shape[0]), ("b", scratch["p_b"].shape[0]), ("o", packed_out)):
        scratch["fin_" + key] = vm((n_rep, packed // n_rep, 128), bf16)
        scratch["r4s_" + key], scratch["r4r_" + key] = dma, dma
    scratch["pk_v"] = vm((packed_out, 128), f32)
    scratch["z_v"] = vm((n_rep, packed_out, 128), f32)
    for name in ("zb_v", "rz_v"):
        scratch[name] = vm((n_rep, packed_out, 128), bf16)
    scratch["tz_v"] = vm((4, packed_out // n_rep, 128), f32)
    for name in ("tzb_v", "r2z_v"):
        scratch[name] = vm((4, packed_out // n_rep, 128), bf16)
    for key in ("tf", "e", "sm", "ft", "em", "rs", "c0", "c1", "c2", "rz", "r2z"):
        scratch[key + "_send"], scratch[key + "_recv"] = dma, dma
    shape = jax.ShapeDtypeStruct
    results = dict(
        g_o=shape((rows_all, width), f32), e_o=shape((rows_all, width), f32), gg_o=shape((width,), f32),
        gb_o_=shape((width,), f32), eg_o=shape((width,), f32), eb_o=shape((width,), f32),
    )
    operands = dict(
        ts=timesteps, sw=sw, so=so, to=to, tw=tw, st=st, tt=tt, x_s=student_in.T, sg=sg, sb=sb,
        x_t=target_in.T, tg=tg, tb=tb,
    )
    names = tuple(key + "_h" for key in operands) + tuple(results) + tuple(scratch)
    values = pl.pallas_call(
        functools.partial(fused_kernel, n_rep, n_sam, names),
        out_shape=tuple(results.values()),
        in_specs=[pl.BlockSpec(memory_space=pltpu.HBM)] * len(operands),
        out_specs=[pl.BlockSpec(memory_space=vm)] * len(results),
        scratch_shapes=list(scratch.values()),
        compiler_params=pltpu.CompilerParams(
            collective_id=0, has_side_effects=True, vmem_limit_bytes=40 * 1024 * 1024
        ),
        name="distill_step",
    )(*(pltpu.with_memory_space_constraint(value, pltpu.HBM) for value in operands.values()))
    big = [shape(w.shape, f32) for w in (sw, so, st)]
    flat = [shape((width,), f32)] * 2
    return tuple(
        pl.pallas_call(
            output_kernel,
            out_shape=(*big, *flat, *big, *flat),
            in_specs=[pl.BlockSpec(memory_space=vm)] * len(results),
            out_specs=[pl.BlockSpec(memory_space=pltpu.HBM)] * 10,
            scratch_shapes=[dma((10,))],
            compiler_params=pltpu.CompilerParams(vmem_limit_bytes=8 * 1024 * 1024),
            name="output_step",
        )(*values)
    )


def fits_fused(n_dp, n_rep, args):
    tokens, samples = args[0].shape[0], args[2].shape[0]
    n_dev = n_dp * n_rep
    rows = [args[i].shape[0] for i in (3, 4, 5)]
    return (
        n_dp == 8
        and n_rep == 4
        and samples % n_dev == 0
        and 2 * (samples // n_dev) + 0 <= SUB
        and (samples // n_dev) % 2 == 0
        and tokens % samples == 0
        and (tokens // samples) % 128 == 0
        and all(r % (16 * n_dp) == 0 for r in rows)
        and all(r % (32 * n_dp) == 0 for r in rows[:1])
        and in_pieces(rows[0] // n_dp)["a"][1] % 64 == 0
        and in_pieces(rows[0] // n_dp)["a"][1] > 0
        and rows[0] == 2 * rows[1]
        and rows[2] == rows[1]
        and args[0].shape[1] % 128 == 64
    )


def solution(mesh):
    in_specs = (
        P(("dp", "rep"), None),
        P(("dp", "rep"), None),
        P(("dp", "rep")),
        P("dp", None),
        P("dp", None),
        P("dp", None),
        P(),
        P(),
        P("dp", None),
        P("dp", None),
        P("dp", None),
        P(),
        P(),
    )
    out_specs = (
        P("dp", None),
        P("dp", None),
        P("dp", None),
        P(),
        P(),
        P("dp", None),
        P("dp", None),
        P("dp", None),
        P(),
        P(),
    )
    n_dp, n_rep = mesh.shape["dp"], mesh.shape["rep"]

    def step(*args):
        fused = fits_fused(n_dp, n_rep, args)
        body = functools.partial(fused_device, n_dp, n_rep) if fused else per_device
        return jax.shard_map(
            body, mesh=mesh, in_specs=in_specs, out_specs=out_specs, check_vma=False
        )(*args)

    return step
```

```python
import functools
import math

import jax
import jax.numpy as jnp
from jax import lax
from jax.experimental import pallas as pl
from jax.experimental.pallas import tpu as pltpu
from jax.sharding import PartitionSpec as P

MESH = pl.DeviceIdType.MESH
SUB = 8

SKIP = 20


ema_decay = 0.95
learn_rate = 0.05


def sinusoid(step_ids, width):
    half_width = width // 2
    frequency = jnp.exp(-math.log(10000.0) * jnp.arange(half_width, dtype=jnp.float32) / half_width)
    angles = step_ids.astype(jnp.float32)[:, None] * frequency[None, :]
    return jnp.concatenate([jnp.cos(angles), jnp.sin(angles)], axis=1)


def gelu_tanh(value):
    inner = 0.7978845608 * (value + 0.044715 * value * value * value)
    return 0.5 * value * (1.0 + jnp.tanh(inner))


def gelu_slope(value):
    tangent = jnp.tanh(0.7978845608 * (value + 0.044715 * value * value * value))
    return 0.5 * (1.0 + tangent) + 0.5 * value * (1.0 - tangent * tangent) * 0.7978845608 * (
        1.0 + 0.134145 * value * value
    )


def contract_last(left, right):
    return lax.dot_general(
        left, right, (((1,), (1,)), ((), ())), preferred_element_type=jnp.float32
    )


def contract_first(left, right):
    return lax.dot_general(
        left, right, (((0,), (0,)), ((), ())), preferred_element_type=jnp.float32
    )


def forward(tok_rows, step_ids, w_in, w_out, w_time, gain, bias):
    time_feat = jax.nn.silu(sinusoid(step_ids, w_time.shape[0])).astype(jnp.bfloat16)
    embedding = jnp.dot(time_feat, w_time, preferred_element_type=jnp.float32)
    samples = step_ids.shape[0]
    width = tok_rows.shape[1]
    summed = tok_rows.astype(jnp.float32).reshape(samples, -1, width) + embedding[:, None, :]
    summed = summed.reshape(-1, width)
    center = summed - jnp.mean(summed, axis=1, keepdims=True)
    inv_std = lax.rsqrt(jnp.mean(center * center, axis=1, keepdims=True) + 1e-05)
    normed = center * inv_std
    normed_b = (normed * gain + bias).astype(jnp.bfloat16)
    mixed = contract_last(normed_b, w_in)
    hidden_count = w_out.shape[0]
    gate_part = mixed[:, :hidden_count]
    up_part = mixed[:, hidden_count:]
    gelu_gate = gelu_tanh(gate_part)
    hidden = (gelu_gate * up_part).astype(jnp.bfloat16)
    output = summed + jnp.dot(hidden, w_out, preferred_element_type=jnp.float32)
    return (output, (time_feat, normed, inv_std, normed_b, gate_part, up_part, gelu_gate, hidden))


def backward(grad_y, saved, w_in, w_out, gain):
    time_feat, normed, inv_std, normed_b, gate_part, up_part, gelu_gate, hidden = saved
    grad_yb = grad_y.astype(jnp.bfloat16)
    grad_h = contract_last(grad_yb, w_out)
    grad_mix = jnp.concatenate(
        [grad_h * up_part * gelu_slope(gate_part), grad_h * gelu_gate], axis=1
    ).astype(jnp.bfloat16)
    grad_z = jnp.dot(grad_mix, w_in, preferred_element_type=jnp.float32)
    grad_gain = jnp.sum(grad_z * normed, axis=0)
    grad_bias = jnp.sum(grad_z, axis=0)
    grad_n = grad_z * gain
    grad_s = grad_y + inv_std * (
        grad_n
        - jnp.mean(grad_n, axis=1, keepdims=True)
        - normed * jnp.mean(grad_n * normed, axis=1, keepdims=True)
    )
    samples = time_feat.shape[0]
    grad_emb = jnp.sum(grad_s.reshape(samples, -1, grad_s.shape[1]), axis=1)
    grad_time = lax.dot_general(
        time_feat.astype(jnp.float32),
        grad_emb,
        (((0,), (0,)), ((), ())),
        precision=lax.Precision.HIGHEST,
        preferred_element_type=jnp.float32,
    )
    return (grad_yb, grad_mix, grad_gain, grad_bias, grad_time)


def fetch(piece_in, piece_out, piece_time):
    return (
        lax.all_gather(piece_in, "dp", axis=0, tiled=True),
        lax.all_gather(piece_out, "dp", axis=0, tiled=True),
        lax.all_gather(piece_time, "dp", axis=0, tiled=True),
    )


def per_device(
    student_in,
    target_in,
    timesteps,
    student_win,
    student_wout,
    student_wtime,
    student_gain,
    student_bias,
    target_win,
    target_wout,
    target_wtime,
    target_gain,
    target_bias,
):
    s_in, s_out, s_time = fetch(
        student_win.astype(jnp.bfloat16),
        student_wout.astype(jnp.bfloat16),
        student_wtime.astype(jnp.bfloat16),
    )
    student_out, saved = forward(
        student_in, timesteps, s_in, s_out, s_time, student_gain, student_bias
    )
    t_in, t_out, t_time = fetch(
        target_win.astype(jnp.bfloat16),
        target_wout.astype(jnp.bfloat16),
        target_wtime.astype(jnp.bfloat16),
    )
    target_out, unused = forward(
        target_in, timesteps - SKIP, t_in, t_out, t_time, target_gain, target_bias
    )
    grad_y = (student_out - target_out) / student_in.shape[0]
    back_in, back_out = (
        lax.all_gather(student_win.astype(jnp.bfloat16), "dp", axis=0, tiled=True),
        lax.all_gather(student_wout.astype(jnp.bfloat16), "dp", axis=0, tiled=True),
    )
    grad_yb, grad_mix, grad_gain, grad_bias, grad_time = backward(
        grad_y, saved, back_in, back_out, student_gain
    )
    normed_b = saved[3]
    hidden = saved[7]
    part = grad_mix
    shard_in = lax.psum_scatter(
        contract_first(part, normed_b), "dp", scatter_dimension=0, tiled=True
    )
    part = hidden
    shard_out = lax.psum_scatter(
        contract_first(part, grad_yb), "dp", scatter_dimension=0, tiled=True
    )
    shard_time = lax.psum_scatter(grad_time, "dp", scatter_dimension=0, tiled=True)
    shard_in, shard_out, shard_time = lax.psum((shard_in, shard_out, shard_time), "rep")
    total_gain, total_bias = lax.psum((grad_gain, grad_bias), ("dp", "rep"))

    def average(target_p, student_p, grad_p):
        return ema_decay * target_p + (1.0 - ema_decay) * (student_p - learn_rate * grad_p)

    return (
        shard_in,
        shard_out,
        shard_time,
        total_gain,
        total_bias,
        average(target_win, student_win, shard_in),
        average(target_wout, student_wout, shard_out),
        average(target_wtime, student_wtime, shard_time),
        average(target_gain, student_gain, total_gain),
        average(target_bias, student_bias, total_bias),
    )


GATE_C = 0.7978845608


def put_packed(ref, value):
    rows, lo = value.shape[0], value.shape[1] // 128 * 128
    for i in range(lo // 128):
        ref[i * rows : (i + 1) * rows, :] = value[:, i * 128 : (i + 1) * 128].astype(ref.dtype)
    at, half = lo // 128 * rows, rows // 2
    rest = jnp.concatenate([value[:half, lo:], value[half:, lo:]], axis=1)
    ref[at : at + half, :] = rest.astype(ref.dtype)


def unpacked(value, rows, width):
    lo = width // 128 * 128
    at, half, rest = lo // 128 * rows, rows // 2, width - lo
    parts = [value[i * rows : (i + 1) * rows] for i in range(lo // 128)]
    tail = value[at : at + half]
    parts.append(jnp.concatenate([tail[:, :rest], tail[:, rest:]], axis=0))
    return jnp.concatenate(parts, axis=1)


def in_pieces(rows):
    big = rows * 2 // 5 // 16 * 16
    return {"a": (0, big), "b": (big, big), "c": (2 * big, rows - 2 * big)}


def fused_kernel(n_rep, n_sam, names, *refs):
    r = dict(zip(names, refs))
    f32, bf16 = jnp.float32, jnp.bfloat16
    me, rep = lax.axis_index("dp"), lax.axis_index("rep")
    core, col, row = lax.rem(me, 2), lax.rem(lax.div(me, 2), 2), lax.div(me, 4)
    sw, so, st, tw, to, tt = (r[k] for k in ("sw", "so", "st", "tw", "to", "tt"))
    sg, sb, tg, tb, x_s, x_t = (r[k] for k in ("sg", "sb", "tg", "tb", "x_s", "x_t"))
    rows_in, rows_out, rows_time = sw.shape[0], so.shape[0], st.shape[0]
    pieces = in_pieces(rows_in)
    width, tokens = x_s.shape
    per = tokens // n_sam
    lo = width // 128 * 128
    rest = width - lo
    ws_all, os_all, wt_all, ot_all = (r[k] for k in ("ws_all", "os_all", "wt_all", "ot_all"))
    ff = os_all.shape[0]
    tf_own, tf_all, e_part, e_in = (r[k] for k in ("tf_own", "tf_all", "e_part", "e_in"))
    g_all, e_all = r["g_o"], r["e_o"]

    flip = lambda b, on: 1 - b if on else b

    def peer(t):
        return flip(row, t & 4) * 4 + flip(col, t & 2) * 2 + flip(core, t & 1)

    def dp_id(t):
        return {"dp": peer(t)}

    def rep_peer(j):
        return flip(lax.div(rep, 2), j & 2) * 2 + flip(lax.rem(rep, 2), j & 1)

    def rep_id(j):
        return {"rep": rep_peer(j)}

    barrier = pltpu.get_barrier_semaphore()
    for t in range(1, 8):
        pl.semaphore_signal(barrier, inc=1, device_id=dp_id(t), device_id_type=MESH)
    for valid, step in ((rep > 0, -1), (rep < n_rep - 1, 1)):

        @pl.when(valid)
        def _(step=step):
            pl.semaphore_signal(barrier, inc=1, device_id={"rep": rep + step}, device_id_type=MESH)


    loads = []
    for i, name in enumerate(LOADED):
        copy = pltpu.make_async_copy(r[name + "_h"], r[name], r["ld_sem"].at[i])
        copy.start()
        loads.append(copy)

    def loaded(*keys):
        for key in keys:
            loads[LOADED.index(key)].wait()

    def send(src, dst, s_sem, r_sem, where):
        pltpu.make_async_remote_copy(
            src_ref=src, dst_ref=dst, send_sem=s_sem, recv_sem=r_sem,
            device_id=where, device_id_type=MESH,
        ).start()

    def bytes_of(ref, sem):
        return pltpu.make_async_remote_copy(
            src_ref=ref, dst_ref=ref, send_sem=sem, recv_sem=sem,
            device_id=dp_id(1), device_id_type=MESH,
        )

    def arrive(ref, sem):
        bytes_of(ref, sem).wait_recv()

    sent = []

    def exchange(key, source, slots, peers, where):
        for j in peers:
            src, dst = source(j), slots(j)
            send(src, dst, r[key + "_send"], r[key + "_recv"], where(j))

    bufs = (r["p_sin"], r["p_out"], r["p_tin"], r["p_tout"])
    s_in, out, t_in, t_out = range(4)
    g_send, g_recv = r["g_send"], r["g_recv"]
    loaded("ts")
    line = lax.broadcasted_iota(jnp.int32, (SUB, rows_time), 0)
    lane = lax.broadcasted_iota(jnp.int32, (SUB, rows_time), 1)
    steps = jnp.zeros((SUB, rows_time), f32)
    for k in range(n_sam):
        value = r["ts"][k]
        steps = jnp.where(line == k, value.astype(f32), steps)
        steps = jnp.where(line == n_sam + k, (value - SKIP).astype(f32), steps)
    half_width = 4 * rows_time
    for d in range(8):
        place = (lane + (d % 4) * rows_time).astype(f32)
        angle = steps * jnp.exp(-math.log(10000.0) * place / half_width)
        wave = jax.nn.silu(jnp.cos(angle) if d < 4 else jnp.sin(angle))
        tf_own[d] = jnp.where(line < 2 * n_sam, wave.astype(bf16).astype(f32), 0.0)
    tf_all[pl.ds(me, 1)] = tf_own[pl.ds(me, 1)]
    loaded("sw")
    put_packed(bufs[s_in].at[me], sw[...])
    pl.semaphore_wait(barrier, 7 + jnp.minimum(rep, 1) + jnp.minimum(n_rep - 1 - rep, 1))

    def cut(seg):
        return bufs[seg].shape[1] // 32 * 16

    def push(seg, orel, t, r_at, start=0, count=None):
        count = bufs[seg].shape[1] if count is None else count
        part = bufs[seg].at[peer(orel), pl.ds(start, count)]
        send(part, part, g_send.at[seg], g_recv.at[seg * 5 + r_at], dp_id(t))

    def landed(seg, r_at, count=1):
        arrive(bufs[seg].at[pl.ds(0, count)], g_recv.at[seg * 5 + r_at])

    def landed_rows(seg, r_at, count):
        arrive(bufs[seg].at[0, pl.ds(0, count)], g_recv.at[seg * 5 + r_at])

    def open_gather(seg):
        c = cut(seg)
        d = bufs[seg].shape[1] - c
        push(seg, 0, 2, 0, 0, c)
        push(seg, 0, 4, 1, c, d)
        push(seg, 0, 2, 4, c, d)
        push(seg, 0, 4, 4, 0, c)
        push(seg, 0, 1, 3)
        sent.append((bufs[seg].at[pl.ds(0, 7)], g_send.at[seg]))

    def relay(seg):
        c = cut(seg)
        d = bufs[seg].shape[1] - c
        landed_rows(seg, 0, c)
        push(seg, 2, 4, 2, 0, c)
        landed_rows(seg, 1, d)
        push(seg, 4, 2, 2, c, d)

    def relay_near(seg):
        landed(seg, 4)
        push(seg, 2, 1, 3)
        push(seg, 4, 1, 3)

    def relay_far(seg):
        landed(seg, 2)
        push(seg, 6, 1, 3)

    def close_gather(seg):
        landed(seg, 3, 4)

    here, there = (0, 2, 4, 6), (1, 3, 5, 7)

    def place_in(seg, dst, rels):
        half = rows_in // 2
        at = lo // 128 * rows_in
        for o in map(peer, rels):
            first = pl.multiple_of(o * rows_in, 16)
            second = pl.multiple_of(o * rows_in + half, 16)
            for i in range(lo // 128):
                dst[pl.ds(first, rows_in), i * 128 : (i + 1) * 128] = bufs[seg][o, i * rows_in : (i + 1) * rows_in, :]
            tail = bufs[seg][o, at : at + half, :]
            dst[pl.ds(first, half), lo:] = tail[:, :rest]
            dst[pl.ds(second, half), lo:] = tail[:, rest:]

    def place_out(seg, dst, lanes, rels):
        at = lo // 128 * rows_out
        for o in map(peer, rels):
            first = pl.multiple_of(o * rows_out, 16)
            for i in range(lo // 128):
                dst[pl.ds(first, rows_out), i * 128 : (i + 1) * 128] = bufs[seg][o, i * rows_out : (i + 1) * rows_out, :]
            dst[pl.ds(first, rows_out), lo:] = bufs[out][o, at : at + rows_out, :][:, lanes : lanes + rest]

    near = (1, 2, 4, 3, 5, 6, 7)
    exchange("tf", lambda t: tf_own.at[peer(t)], lambda t: tf_all.at[me], near, dp_id)
    open_gather(s_in)
    loaded("tw")
    put_packed(bufs[t_in].at[me], tw[...])
    open_gather(t_in)
    loaded("so", "to")
    for i in range(lo // 128):
        at, lanes = slice(i * rows_out, (i + 1) * rows_out), slice(i * 128, (i + 1) * 128)
        bufs[out][me, at, :] = so[:, lanes].astype(bf16)
        bufs[t_out][me, at, :] = to[:, lanes].astype(bf16)
    at = slice(lo // 128 * rows_out, (lo // 128 + 1) * rows_out)
    bufs[out][me, at, :] = jnp.concatenate([so[:, lo:], to[:, lo:]], axis=1).astype(bf16)
    loaded("st", "tt")
    st_b, tt_b = st[...].astype(bf16), tt[...].astype(bf16)
    arrive(tf_all.at[pl.ds(0, 7)], r["tf_recv"])
    feats = tf_all[...].reshape(8 * SUB, rows_time).astype(bf16)
    part_s = jnp.dot(feats, st_b, preferred_element_type=f32)
    part_t = jnp.dot(feats, tt_b, preferred_element_type=f32)
    which = lax.rem(lax.broadcasted_iota(jnp.int32, part_s.shape, 0), SUB)
    part = jnp.where(which < n_sam, part_s, part_t)
    for d in range(8):
        put_packed(e_part.at[d], part[d * SUB : d * SUB + 2 * n_sam])
    e_in[pl.ds(me, 1)] = e_part[pl.ds(me, 1)]
    exchange("e", lambda t: e_part.at[peer(t)], lambda t: e_in.at[me], near, dp_id)
    relay(s_in)
    open_gather(out)
    open_gather(t_out)

    ft_all, em_all = r["ft_all"], r["em_all"]
    ft_all[pl.ds(rep, 1)] = jnp.concatenate([tf_all[d, :n_sam, :] for d in range(8)], axis=0).astype(bf16)[None]
    far = (3, 2, 1)

    def pass_features(hops):
        for back, valid, onward in ((-1, rep >= hops, rep < n_rep - 1), (1, rep + hops < n_rep, rep > 0)):

            @pl.when(valid)
            def _(back=back, onward=onward):
                b = rep + back * hops
                at = ft_all.at[b]
                if hops:
                    arrive(at, r["ft_recv"].at[b])

                @pl.when(onward)
                def _():
                    send(at, at, r["ft_send"].at[(1 + back) // 2], r["ft_recv"].at[b], {"rep": rep - back})

    def features_sent():
        for k in range(n_rep):

            @pl.when(rep == k)
            def _(k=k):
                if k < n_rep - 1:
                    bytes_of(ft_all.at[pl.ds(0, k + 1)], r["ft_send"].at[0]).wait_send()
                if k > 0:
                    bytes_of(ft_all.at[pl.ds(0, n_rep - k)], r["ft_send"].at[1]).wait_send()

    pass_features(0)
    start = 0
    for student, target in ((sw, tw), (so, to), (st, tt)):
        count = student.shape[0]
        e_all[start : start + count, :] = ema_decay * target[...] + (1.0 - ema_decay) * student[...]
        start += count
    y_v, normed_v, inv_v, nb_v, nbt_v = (r[k] for k in ("y_v", "normed_v", "inv_v", "nb_v", "nbt_v"))
    xt_v = r["xt_v"]
    loaded("x_s", "sg", "sb")
    for k in range(n_sam):
        y_v[pl.ds(k * per, per), :] = x_s[:, pl.ds(k * per, per)].astype(f32).T
    relay(t_in)
    relay_near(s_in)
    loaded("x_t", "tg", "tb")
    for k in range(n_sam):
        xt_v[pl.ds(k * per, per), :] = x_t[:, pl.ds(k * per, per)].astype(f32).T

    arrive(e_in.at[pl.ds(0, 7)], r["e_recv"])
    emb = e_in[0]
    for k in range(1, 8):
        emb = emb + e_in[k]
    emb = unpacked(emb, 2 * n_sam, width)

    hid_v, hidt_v, a_v, b_v, gyb_v, gm_v = (r[k] for k in ("hid_v", "hidt_v", "a_v", "b_v", "gyb_v", "gm_v"))

    def normalise(x_rows, k, shift, gain, bias):
        summed = x_rows[pl.ds(k * per, per), :] + shift
        center = summed - jnp.mean(summed, axis=1, keepdims=True)
        inv = lax.rsqrt(jnp.mean(center * center, axis=1, keepdims=True) + 1e-05)
        normed = center * inv
        return summed, inv, normed, (normed * gain + bias).astype(bf16)

    for k in range(n_sam):
        at = pl.ds(k * per, per)
        summed, inv, normed, nb = normalise(y_v, k, emb[k : k + 1], sg[...][None], sb[...][None])
        y_v[at, :], normed_v[at, :], nb_v[at, :] = summed, normed, nb
        inv_v[at, :] = inv
    relay_far(s_in)
    relay(out)
    relay_near(t_in)
    for k in range(n_sam):
        at = pl.ds(k * per, per)
        summed, inv, normed, nb = normalise(
            xt_v, k, emb[n_sam + k : n_sam + k + 1], tg[...][None], tb[...][None]
        )
        y_v[at, :], nbt_v[at, :] = y_v[at, :] - summed, nb
    pass_features(1)
    relay_near(out)
    place_in(s_in, ws_all, here)
    close_gather(s_in)
    place_in(s_in, ws_all, there)
    relay(t_out)

    for k in range(n_sam):
        at = pl.ds(k * per, per)
        gate = contract_last(nb_v[at, :], ws_all[:ff, :])
        up = contract_last(nb_v[at, :], ws_all[ff:, :])
        square = gate * gate
        half = 0.5 + 0.5 * jnp.tanh(gate * (GATE_C + GATE_C * 0.044715 * square))
        act = gate * half
        slope = half + act * (1.0 - half) * (2.0 * GATE_C + 2.0 * GATE_C * 0.134145 * square)
        a_v[at, :], b_v[at, :] = up * slope, act
        hid_v[at, :] = (act * up).astype(bf16)
        if k == 0:
            relay_far(t_in)
            relay_near(t_out)
    relay_far(out)
    pass_features(2)
    place_in(t_in, wt_all, here)
    close_gather(t_in)
    place_in(t_in, wt_all, there)
    for k in range(n_sam):
        at = pl.ds(k * per, per)
        gate = contract_last(nbt_v[at, :], wt_all[:ff, :])
        up = contract_last(nbt_v[at, :], wt_all[ff:, :])
        half = 0.5 + 0.5 * jnp.tanh(gate * (GATE_C + GATE_C * 0.044715 * (gate * gate)))
        hidt_v[at, :] = (gate * half * up).astype(bf16)
        if k == 0:
            relay_far(t_out)
    place_out(out, os_all, 0, here)
    close_gather(out)
    place_out(out, os_all, 0, there)
    for k in range(n_sam):
        at = pl.ds(k * per, per)
        y_v[at, :] = y_v[at, :] + jnp.dot(hid_v[at, :], os_all[...], preferred_element_type=f32)
    place_out(t_out, ot_all, rest, here)
    close_gather(t_out)
    place_out(t_out, ot_all, rest, there)
    for k in range(n_sam):
        at = pl.ds(k * per, per)
        gy = (y_v[at, :] - jnp.dot(hidt_v[at, :], ot_all[...], preferred_element_type=f32)) * (1.0 / tokens)
        y_v[at, :], gyb_v[at, :] = gy, gy.astype(bf16)

    pass_features(3)
    r1_o, r1_i = r["r1_o"], r["r1_i"]

    def to_core(src, dst, count, q, key):
        part = src.at[pl.ds(pl.multiple_of((2 * q + 1 - core) * count, 16), count)]
        send(part, dst.at[q], r[key + "_send"], r[key + "_recv"], dp_id(1))

    def pair(key, rel):
        first, count = pieces[key]
        owner = peer(rel)
        own = r["gs_i"][pl.ds(pl.multiple_of(owner * rows_in + first, 16), count), :]
        return own + r1_i[lax.div(owner, 2), first : first + count, :].astype(f32)

    def to_chip(key, k):
        s2, r2 = r["s2_" + key], r["r2_" + key]
        put_packed(s2.at[k], pair(key, 2 * k))
        send(s2.at[k], r2.at[k], r["r2s_" + key], r["r2r_" + key], dp_id(2 * k))

    total_out = contract_first(hid_v[...], gyb_v[...])
    r["gs_o"][...] = total_out
    r["gb_o"][...] = total_out.astype(bf16)
    for q in range(4):
        to_core(r["gb_o"], r1_o, rows_out, q, "c0")
    for k in range(n_sam):
        at = pl.ds(k * per, per)
        gh = contract_last(gyb_v[at, :], os_all[...])
        gm_v[0, at, :], gm_v[1, at, :] = (gh * a_v[at, :]).astype(bf16), (gh * b_v[at, :]).astype(bf16)

    def weight_grad(turn):
        h = 1 - row if turn == 0 else row
        total = contract_first(gm_v[h], nb_v[...])
        at = pl.ds(pl.multiple_of(h * ff, 16), ff)
        r["gs_i"][at, :], r["gb_i"][at, :] = total, total.astype(bf16)
        for q in range(2):
            to_core(r["gb_i"], r1_i, rows_in, 2 * h + q, "c" + str(1 + turn))

    grad_gain = jnp.zeros((1, width), f32)
    grad_bias = grad_gain
    embs = []
    small = r["small"]

    def input_grad(k):
        at = pl.ds(k * per, per)
        gz = jnp.dot(gm_v[0, at, :], ws_all[:ff, :], preferred_element_type=f32) + jnp.dot(
            gm_v[1, at, :], ws_all[ff:, :], preferred_element_type=f32
        )
        normed = normed_v[at, :]
        gn = gz * sg[...][None]
        gs = y_v[at, :] + inv_v[at, :] * (
            gn
            - jnp.mean(gn, axis=1, keepdims=True)
            - normed * jnp.mean(gn * normed, axis=1, keepdims=True)
        )
        embs.append(jnp.sum(gs, axis=0, keepdims=True))
        return jnp.sum(gz * normed, axis=0, keepdims=True), jnp.sum(gz, axis=0, keepdims=True)

    weight_grad(0)
    arrive(r1_o, r["c0_recv"])
    pk_v, z_v, zb_v, rz_v = r["pk_v"], r["z_v"], r["zb_v"], r["rz_v"]
    share = pk_v.shape[0] // n_rep
    for q in range(4):
        own = r["gs_o"][pl.ds(pl.multiple_of((2 * q + core) * rows_out, 16), rows_out), :]
        put_packed(pk_v, own + r1_o[q].astype(f32))
        for j in range(n_rep):
            z_v[j, q * share : (q + 1) * share, :] = pk_v[j * share : (j + 1) * share, :]
    for j in range(n_rep):
        zb_v[j] = z_v[j].astype(bf16)
    exchange("rz", lambda j: zb_v.at[rep_peer(j)], lambda j: rz_v.at[j], far, rep_id)
    weight_grad(1)
    arrive(r1_i.at[pl.ds(0, 2)], r["c1_recv"])
    to_chip("a", 3)
    to_chip("a", 2)
    for k in range(n_sam):
        more_gain, more_bias = input_grad(k)
        grad_gain, grad_bias = grad_gain + more_gain, grad_bias + more_bias
        if k == 0:
            arrive(r1_i.at[pl.ds(0, 2)], r["c2_recv"])
            to_chip("a", 1)
            for q in (3, 2, 1):
                to_chip("b", q)
    high = [v.astype(bf16).astype(f32) for v in (grad_gain, grad_bias)]
    low = [v - h for v, h in zip((grad_gain, grad_bias), high)]
    n_small = n_sam + 4
    r["pack_v"][...] = jnp.zeros(r["pack_v"].shape, f32)
    put_packed(r["pack_v"], jnp.concatenate(embs + high + low, axis=0))
    small[pl.ds(me, 1)] = r["pack_v"][...].astype(bf16)[None]
    exchange("sm", lambda t: small.at[me], lambda t: small.at[me], near, dp_id)
    for k in (3, 2, 1):
        to_chip("c", k)
    for key in "abc":
        put_packed(r["p_" + key], pair(key, 0))

    def chips_total(key):
        p, r2 = r["p_" + key], r["r2_" + key]
        arrive(r2.at[pl.ds(1, 3)], r["r2r_" + key])
        p[...] = p[...] + r2[1].astype(f32) + r2[2].astype(f32) + r2[3].astype(f32)
        return p

    def to_planes(key):
        p, pb, r3 = chips_total(key), r["pb_" + key], r["r3_" + key]
        part = pb.shape[1]
        for q in range(n_rep):
            pb[q] = p[q * part : (q + 1) * part, :].astype(bf16)
        for j in far:
            send(pb.at[rep_peer(j)], r3.at[j], r["r3s_" + key], r["r3r_" + key], rep_id(j))

    def to_next_plane(key):
        r3 = r["r3_" + key]
        slot = lax.rem(rep, 2)
        r3[pl.ds(slot, 1)] = chips_total(key)[...].astype(bf16)[None]
        send(r3.at[slot], r3.at[slot], r["r3s_" + key], r["r3r_" + key], rep_id(1))

    def to_far_plane(key):
        r3, r4 = r["r3_" + key], r["r4_" + key]
        slot = lax.div(rep, 2)
        arrive(r3.at[0], r["r3r_" + key])
        r4[pl.ds(slot, 1)] = (r3[0].astype(f32) + r3[1].astype(f32)).astype(bf16)[None]
        send(r4.at[slot], r4.at[slot], r["r4s_" + key], r["r4r_" + key], rep_id(2))

    def plane_total():
        arrive(rz_v.at[pl.ds(1, 3)], r["rz_recv"])
        tz_v, tzb_v = r["tz_v"], r["tzb_v"]
        total = z_v[rep]
        for j in range(1, n_rep):
            total = total + rz_v[j].astype(f32)
        pk_v[...] = total
        for q in range(4):
            part = pk_v[q * share : (q + 1) * share, :]
            tz_v[q], tzb_v[q] = part, part.astype(bf16)
        exchange(
            "r2z", lambda k: tzb_v.at[lax.div(peer(2 * k), 2)], lambda k: r["r2z_v"].at[k], (3, 1, 2),
            lambda k: dp_id(2 * k),
        )

    def chip_total():
        arrive(r["r2z_v"].at[pl.ds(1, 3)], r["r2z_recv"])
        total = r["tz_v"][lax.div(me, 2)]
        for k in (1, 2, 3):
            total = total + r["r2z_v"][k].astype(f32)
        spread("o", total)

    def spread(key, total):
        fin = r["fin_" + key]
        fin[pl.ds(rep, 1)] = total.astype(bf16)[None]
        for j in far:
            send(fin.at[rep], fin.at[rep], r["r4s_" + key], r["r4r_" + key], rep_id(j))

    def share_total(key):
        p, r3 = r["p_" + key], r["r3_" + key]
        part = r3.shape[1]
        total = p[pl.ds(pl.multiple_of(rep * part, 8), part), :]
        arrive(r3.at[pl.ds(1, 3)], r["r3r_" + key])
        for j in range(1, n_rep):
            total = total + r3[j].astype(f32)
        spread(key, total)

    def finish(start, grad):
        at = slice(start, start + grad.shape[0])
        g_all[at, :] = grad
        e_all[at, :] = e_all[at, :] - (1.0 - ema_decay) * learn_rate * grad

    def collect(key, start, count):
        p, fin = (pk_v if key == "o" else r["p_" + key]), r["fin_" + key]
        part = fin.shape[1]
        arrive(fin.at[pl.ds(0, 3)], r["r4r_" + key])
        for q in range(n_rep):
            p[q * part : (q + 1) * part, :] = fin[q].astype(f32)
        finish(start, unpacked(p[...], count, width))

    def collect_whole(key):
        r4 = r["r4_" + key]
        arrive(r4.at[0], r["r4r_" + key])
        first, count = pieces[key]
        finish(first, unpacked(r4[0].astype(f32) + r4[1].astype(f32), count, width))

    to_planes("a")
    to_planes("b")
    plane_total()
    arrive(small.at[pl.ds(0, 7)], r["sm_recv"])
    part = [small[d].astype(f32) for d in range(8)]
    sums = part[0]
    for k in range(1, 8):
        sums = sums + part[k]
    sums = unpacked(sums, n_small, width)
    sums = sums[n_sam : n_sam + 2] + sums[n_sam + 2 : n_sam + 4]
    high = sums.astype(bf16).astype(f32)
    put_packed(r["pack_v"], jnp.concatenate([high, sums - high], axis=0))
    n_em = em_all.shape[1] - small.shape[1]
    put_packed(em_all.at[rep], jnp.concatenate([unpacked(p, n_small, width)[:n_sam] for p in part], axis=0))
    em_all[pl.ds(rep, 1), n_em:, :] = r["pack_v"][...].astype(bf16)[None]

    @pl.when(core == 1)
    def _():
        exchange("em", lambda j: em_all.at[rep], lambda j: em_all.at[rep], far, rep_id)

    def pass_to_core():
        arrive(em_all.at[pl.ds(0, 3)], r["em_recv"])
        for j in far:
            at = em_all.at[rep_peer(j)]
            send(at, at, r["rs_send"], r["em_recv"], dp_id(1))

    to_next_plane("c")
    share_total("a")
    share_total("b")
    to_far_plane("c")
    chip_total()
    pl.when(core == 1)(pass_to_core)
    collect_whole("c")

    @pl.when(core == 0)
    def _():
        arrive(em_all.at[pl.ds(0, 3)], r["em_recv"])

    grad_time = jnp.zeros((rows_time, width), f32)
    for j in range(n_rep):
        samples = unpacked(em_all[j, :n_em, :].astype(f32), 8 * n_sam, width).astype(bf16)
        grad_time = grad_time + contract_first(ft_all[j], samples)
    sums = jnp.zeros((2, width), f32)
    for j in range(n_rep):
        part = unpacked(em_all[j, n_em:, :].astype(f32), 4, width)
        sums = sums + part[:2] + part[2:]
    finish(rows_in + rows_out, grad_time)
    gg, gb = sums[0, :], sums[1, :]
    r["gg_o"][...], r["gb_o_"][...] = gg, gb
    r["eg_o"][...] = average(tg[...], sg[...], gg)
    r["eb_o"][...] = average(tb[...], sb[...], gb)
    collect("a", *pieces["a"])
    collect("b", *pieces["b"])
    collect("o", rows_in, rows_out)
    for key, ref in (("tf", tf_all), ("e", e_in), ("sm", small)):
        sent.append((ref.at[pl.ds(0, 7)], r[key + "_send"]))
    sent += [(r1_o, r["c0_send"]), (r1_i.at[pl.ds(0, 2)], r["c1_send"]), (r1_i.at[pl.ds(0, 2)], r["c2_send"])]
    for key in "abc":
        sent.append((r["r2_" + key].at[pl.ds(0, 3)], r["r2s_" + key]))
        sent.append((r["r3_" + key].at[0] if key == "c" else r["r3_" + key].at[pl.ds(0, 3)], r["r3s_" + key]))
    sent.append((r["r4_c"].at[0], r["r4s_c"]))
    sent += [(rz_v.at[pl.ds(0, 3)], r["rz_send"]), (r["r2z_v"].at[pl.ds(0, 3)], r["r2z_send"])]
    for key in "oab":
        sent.append((r["fin_" + key].at[pl.ds(0, 3)], r["r4s_" + key]))
    for ref, sem in sent:
        bytes_of(ref, sem).wait_send()
    features_sent()

    @pl.when(core == 1)
    def _():
        for key in ("em_send", "rs_send"):
            bytes_of(em_all.at[pl.ds(0, 3)], r[key]).wait_send()


LOADED = ("ts", "sw", "so", "to", "tw", "st", "tt", "x_s", "sg", "sb", "x_t", "tg", "tb")


def average(target_p, student_p, grad_p):
    return ema_decay * target_p + (1.0 - ema_decay) * (student_p - learn_rate * grad_p)


def output_kernel(grads, means, gg, gb, eg, eb, gw_o, go_o, gt_o, gg_o, gb_o, ew_o, eo_o, et_o, eg_o, eb_o, sem):
    copies = []
    for src, outs in ((grads, (gw_o, go_o, gt_o)), (means, (ew_o, eo_o, et_o))):
        start = 0
        for dst in outs:
            copies.append((src.at[pl.ds(start, dst.shape[0])], dst))
            start += dst.shape[0]
    copies += [(gg, gg_o), (gb, gb_o), (eg, eg_o), (eb, eb_o)]
    copies = [pltpu.make_async_copy(src, dst, sem.at[i]) for i, (src, dst) in enumerate(copies)]
    for copy in copies:
        copy.start()
    for copy in copies:
        copy.wait()


def fused_device(n_dp, n_rep, *args):
    (student_in, target_in, timesteps, sw, so, st, sg, sb, tw, to, tt, tg, tb) = args
    f32, bf16 = jnp.float32, jnp.bfloat16
    tokens, width = student_in.shape
    n_sam = timesteps.shape[0]
    rows_in, rows_out, rows_time = sw.shape[0], so.shape[0], st.shape[0]
    ff = rows_out * n_dp
    rows_all = rows_in + rows_out + rows_time
    vm = pltpu.VMEM
    dma = pltpu.SemaphoreType.DMA
    full = width // 128
    rows_emb = -(-(2 * n_sam * full + n_sam) // SUB) * SUB
    rows_small = -(-((n_sam + 4) * full + (n_sam + 4) // 2) // 16) * 16
    packed_in, packed_out = rows_in * full + rows_in // 2, rows_out * full + rows_out // 2
    scratch = dict(
        ts=pltpu.SMEM((n_sam,), jnp.int32),
        sw=vm(sw.shape, f32), so=vm(so.shape, f32), st=vm(st.shape, f32),
        tw=vm(tw.shape, f32), to=vm(to.shape, f32), tt=vm(tt.shape, f32),
        sg=vm(sg.shape, f32), sb=vm(sb.shape, f32), tg=vm(tg.shape, f32), tb=vm(tb.shape, f32),
        x_s=vm((width, tokens), bf16), x_t=vm((width, tokens), bf16),
        p_sin=vm((n_dp, packed_in, 128), bf16), p_out=vm((n_dp, rows_out * (full + 1), 128), bf16),
        p_tin=vm((n_dp, packed_in, 128), bf16), p_tout=vm((n_dp, rows_out * full, 128), bf16),
        ws_all=vm((n_dp * rows_in, width), bf16), os_all=vm((ff, width), bf16),
        wt_all=vm((n_dp * rows_in, width), bf16), ot_all=vm((ff, width), bf16),
        tf_own=vm((n_dp, SUB, rows_time), f32), tf_all=vm((n_dp, SUB, rows_time), f32),
        e_part=vm((n_dp, rows_emb, 128), f32), e_in=vm((n_dp, rows_emb, 128), f32),
        small=vm((n_dp, rows_small, 128), bf16), pack_v=vm((rows_small, 128), f32),
        ft_all=vm((n_rep, n_dp * n_sam, rows_time), bf16), em_all=vm((n_rep, n_dp * n_sam * full + n_dp * n_sam // 2 + rows_small, 128), bf16),
        normed_v=vm((tokens, width), f32), inv_v=vm((tokens, 1), f32), nb_v=vm((tokens, width), bf16),
        hid_v=vm((tokens, ff), bf16), hidt_v=vm((tokens, ff), bf16), a_v=vm((tokens, ff), f32), b_v=vm((tokens, ff), f32),
        y_v=vm((tokens, width), f32), xt_v=vm((tokens, width), f32), nbt_v=vm((tokens, width), bf16), gyb_v=vm((tokens, width), bf16),
        gm_v=vm((2, tokens, ff), bf16),
        gs_i=vm((n_dp * rows_in, width), f32), gs_o=vm((ff, width), f32),
        gb_i=vm((n_dp * rows_in, width), bf16), gb_o=vm((ff, width), bf16),
        r1_i=vm((4, rows_in, width), bf16), r1_o=vm((4, rows_out, width), bf16),
        rs_send=dma, ft_send=dma((2,)), ft_recv=dma((n_rep,)), ld_sem=dma((len(LOADED),)), g_send=dma((4,)), g_recv=dma((20,)),
    )
    for key, (_, count) in in_pieces(rows_in).items():
        packed = count * full + count // 2
        scratch["p_" + key] = vm((packed, 128), f32)
        for name in ("s2_", "r2_"):
            scratch[name + key] = vm((4, packed, 128), bf16)
        if key == "c":
            for name in ("r3_", "r4_"):
                scratch[name + key] = vm((2, packed, 128), bf16)
            scratch["r4s_" + key], scratch["r4r_" + key] = dma, dma
        else:
            scratch["r3_" + key] = vm((n_rep, packed // n_rep, 128), bf16)
            scratch["pb_" + key] = vm((n_rep, packed // n_rep, 128), bf16)
        for name in ("r2", "r3"):
            scratch[name + "s_" + key], scratch[name + "r_" + key] = dma, dma
    for key, packed in (("a", scratch["p_a"].shape[0]), ("b", scratch["p_b"].shape[0]), ("o", packed_out)):
        scratch["fin_" + key] = vm((n_rep, packed // n_rep, 128), bf16)
        scratch["r4s_" + key], scratch["r4r_" + key] = dma, dma
    scratch["pk_v"] = vm((packed_out, 128), f32)
    scratch["z_v"] = vm((n_rep, packed_out, 128), f32)
    for name in ("zb_v", "rz_v"):
        scratch[name] = vm((n_rep, packed_out, 128), bf16)
    scratch["tz_v"] = vm((4, packed_out // n_rep, 128), f32)
    for name in ("tzb_v", "r2z_v"):
        scratch[name] = vm((4, packed_out // n_rep, 128), bf16)
    for key in ("tf", "e", "sm", "em", "c0", "c1", "c2", "rz", "r2z"):
        scratch[key + "_send"], scratch[key + "_recv"] = dma, dma
    shape = jax.ShapeDtypeStruct
    results = dict(
        g_o=shape((rows_all, width), f32), e_o=shape((rows_all, width), f32), gg_o=shape((width,), f32),
        gb_o_=shape((width,), f32), eg_o=shape((width,), f32), eb_o=shape((width,), f32),
    )
    operands = dict(
        ts=timesteps, sw=sw, so=so, to=to, tw=tw, st=st, tt=tt, x_s=student_in.T, sg=sg, sb=sb,
        x_t=target_in.T, tg=tg, tb=tb,
    )
    names = tuple(key + "_h" for key in operands) + tuple(results) + tuple(scratch)
    values = pl.pallas_call(
        functools.partial(fused_kernel, n_rep, n_sam, names),
        out_shape=tuple(results.values()),
        in_specs=[pl.BlockSpec(memory_space=pltpu.HBM)] * len(operands),
        out_specs=[pl.BlockSpec(memory_space=vm)] * len(results),
        scratch_shapes=list(scratch.values()),
        compiler_params=pltpu.CompilerParams(
            collective_id=0, has_side_effects=True, vmem_limit_bytes=40 * 1024 * 1024
        ),
        name="distill_step",
    )(*(pltpu.with_memory_space_constraint(value, pltpu.HBM) for value in operands.values()))
    big = [shape(w.shape, f32) for w in (sw, so, st)]
    flat = [shape((width,), f32)] * 2
    return tuple(
        pl.pallas_call(
            output_kernel,
            out_shape=(*big, *flat, *big, *flat),
            in_specs=[pl.BlockSpec(memory_space=vm)] * len(results),
            out_specs=[pl.BlockSpec(memory_space=pltpu.HBM)] * 10,
            scratch_shapes=[dma((10,))],
            compiler_params=pltpu.CompilerParams(vmem_limit_bytes=8 * 1024 * 1024),
            name="output_step",
        )(*values)
    )


def fits_fused(n_dp, n_rep, args):
    tokens, samples = args[0].shape[0], args[2].shape[0]
    n_dev = n_dp * n_rep
    rows = [args[i].shape[0] for i in (3, 4, 5)]
    return (
        n_dp == 8
        and n_rep == 4
        and samples % n_dev == 0
        and 2 * (samples // n_dev) + 0 <= SUB
        and (samples // n_dev) % 2 == 0
        and tokens % samples == 0
        and (tokens // samples) % 128 == 0
        and all(r % (16 * n_dp) == 0 for r in rows)
        and all(r % (32 * n_dp) == 0 for r in rows[:1])
        and in_pieces(rows[0] // n_dp)["a"][1] % 64 == 0
        and in_pieces(rows[0] // n_dp)["a"][1] > 0
        and rows[0] == 2 * rows[1]
        and rows[2] == rows[1]
        and args[0].shape[1] % 128 == 64
    )


def solution(mesh):
    in_specs = (
        P(("dp", "rep"), None),
        P(("dp", "rep"), None),
        P(("dp", "rep")),
        P("dp", None),
        P("dp", None),
        P("dp", None),
        P(),
        P(),
        P("dp", None),
        P("dp", None),
        P("dp", None),
        P(),
        P(),
    )
    out_specs = (
        P("dp", None),
        P("dp", None),
        P("dp", None),
        P(),
        P(),
        P("dp", None),
        P("dp", None),
        P("dp", None),
        P(),
        P(),
    )
    n_dp, n_rep = mesh.shape["dp"], mesh.shape["rep"]

    def step(*args):
        fused = fits_fused(n_dp, n_rep, args)
        body = functools.partial(fused_device, n_dp, n_rep) if fused else per_device
        return jax.shard_map(
            body, mesh=mesh, in_specs=in_specs, out_specs=out_specs, check_vma=False
        )(*args)

    return step
```

```python
import functools
import math

import jax
import jax.numpy as jnp
from jax import lax
from jax.experimental import pallas as pl
from jax.experimental.pallas import tpu as pltpu
from jax.sharding import PartitionSpec as P

MESH = pl.DeviceIdType.MESH
SUB = 8

SKIP = 20


ema_decay = 0.95
learn_rate = 0.05


def sinusoid(step_ids, width):
    half_width = width // 2
    frequency = jnp.exp(-math.log(10000.0) * jnp.arange(half_width, dtype=jnp.float32) / half_width)
    angles = step_ids.astype(jnp.float32)[:, None] * frequency[None, :]
    return jnp.concatenate([jnp.cos(angles), jnp.sin(angles)], axis=1)


def gelu_tanh(value):
    inner = 0.7978845608 * (value + 0.044715 * value * value * value)
    return 0.5 * value * (1.0 + jnp.tanh(inner))


def gelu_slope(value):
    tangent = jnp.tanh(0.7978845608 * (value + 0.044715 * value * value * value))
    return 0.5 * (1.0 + tangent) + 0.5 * value * (1.0 - tangent * tangent) * 0.7978845608 * (
        1.0 + 0.134145 * value * value
    )


def contract_last(left, right):
    return lax.dot_general(
        left, right, (((1,), (1,)), ((), ())), preferred_element_type=jnp.float32
    )


def contract_first(left, right):
    return lax.dot_general(
        left, right, (((0,), (0,)), ((), ())), preferred_element_type=jnp.float32
    )


def forward(tok_rows, step_ids, w_in, w_out, w_time, gain, bias):
    time_feat = jax.nn.silu(sinusoid(step_ids, w_time.shape[0])).astype(jnp.bfloat16)
    embedding = jnp.dot(time_feat, w_time, preferred_element_type=jnp.float32)
    samples = step_ids.shape[0]
    width = tok_rows.shape[1]
    summed = tok_rows.astype(jnp.float32).reshape(samples, -1, width) + embedding[:, None, :]
    summed = summed.reshape(-1, width)
    center = summed - jnp.mean(summed, axis=1, keepdims=True)
    inv_std = lax.rsqrt(jnp.mean(center * center, axis=1, keepdims=True) + 1e-05)
    normed = center * inv_std
    normed_b = (normed * gain + bias).astype(jnp.bfloat16)
    mixed = contract_last(normed_b, w_in)
    hidden_count = w_out.shape[0]
    gate_part = mixed[:, :hidden_count]
    up_part = mixed[:, hidden_count:]
    gelu_gate = gelu_tanh(gate_part)
    hidden = (gelu_gate * up_part).astype(jnp.bfloat16)
    output = summed + jnp.dot(hidden, w_out, preferred_element_type=jnp.float32)
    return (output, (time_feat, normed, inv_std, normed_b, gate_part, up_part, gelu_gate, hidden))


def backward(grad_y, saved, w_in, w_out, gain):
    time_feat, normed, inv_std, normed_b, gate_part, up_part, gelu_gate, hidden = saved
    grad_yb = grad_y.astype(jnp.bfloat16)
    grad_h = contract_last(grad_yb, w_out)
    grad_mix = jnp.concatenate(
        [grad_h * up_part * gelu_slope(gate_part), grad_h * gelu_gate], axis=1
    ).astype(jnp.bfloat16)
    grad_z = jnp.dot(grad_mix, w_in, preferred_element_type=jnp.float32)
    grad_gain = jnp.sum(grad_z * normed, axis=0)
    grad_bias = jnp.sum(grad_z, axis=0)
    grad_n = grad_z * gain
    grad_s = grad_y + inv_std * (
        grad_n
        - jnp.mean(grad_n, axis=1, keepdims=True)
        - normed * jnp.mean(grad_n * normed, axis=1, keepdims=True)
    )
    samples = time_feat.shape[0]
    grad_emb = jnp.sum(grad_s.reshape(samples, -1, grad_s.shape[1]), axis=1)
    grad_time = lax.dot_general(
        time_feat.astype(jnp.float32),
        grad_emb,
        (((0,), (0,)), ((), ())),
        precision=lax.Precision.HIGHEST,
        preferred_element_type=jnp.float32,
    )
    return (grad_yb, grad_mix, grad_gain, grad_bias, grad_time)


def fetch(piece_in, piece_out, piece_time):
    return (
        lax.all_gather(piece_in, "dp", axis=0, tiled=True),
        lax.all_gather(piece_out, "dp", axis=0, tiled=True),
        lax.all_gather(piece_time, "dp", axis=0, tiled=True),
    )


def per_device(
    student_in,
    target_in,
    timesteps,
    student_win,
    student_wout,
    student_wtime,
    student_gain,
    student_bias,
    target_win,
    target_wout,
    target_wtime,
    target_gain,
    target_bias,
):
    s_in, s_out, s_time = fetch(
        student_win.astype(jnp.bfloat16),
        student_wout.astype(jnp.bfloat16),
        student_wtime.astype(jnp.bfloat16),
    )
    student_out, saved = forward(
        student_in, timesteps, s_in, s_out, s_time, student_gain, student_bias
    )
    t_in, t_out, t_time = fetch(
        target_win.astype(jnp.bfloat16),
        target_wout.astype(jnp.bfloat16),
        target_wtime.astype(jnp.bfloat16),
    )
    target_out, unused = forward(
        target_in, timesteps - SKIP, t_in, t_out, t_time, target_gain, target_bias
    )
    grad_y = (student_out - target_out) / student_in.shape[0]
    back_in, back_out = (
        lax.all_gather(student_win.astype(jnp.bfloat16), "dp", axis=0, tiled=True),
        lax.all_gather(student_wout.astype(jnp.bfloat16), "dp", axis=0, tiled=True),
    )
    grad_yb, grad_mix, grad_gain, grad_bias, grad_time = backward(
        grad_y, saved, back_in, back_out, student_gain
    )
    normed_b = saved[3]
    hidden = saved[7]
    part = grad_mix
    shard_in = lax.psum_scatter(
        contract_first(part, normed_b), "dp", scatter_dimension=0, tiled=True
    )
    part = hidden
    shard_out = lax.psum_scatter(
        contract_first(part, grad_yb), "dp", scatter_dimension=0, tiled=True
    )
    shard_time = lax.psum_scatter(grad_time, "dp", scatter_dimension=0, tiled=True)
    shard_in, shard_out, shard_time = lax.psum((shard_in, shard_out, shard_time), "rep")
    total_gain, total_bias = lax.psum((grad_gain, grad_bias), ("dp", "rep"))

    def average(target_p, student_p, grad_p):
        return ema_decay * target_p + (1.0 - ema_decay) * (student_p - learn_rate * grad_p)

    return (
        shard_in,
        shard_out,
        shard_time,
        total_gain,
        total_bias,
        average(target_win, student_win, shard_in),
        average(target_wout, student_wout, shard_out),
        average(target_wtime, student_wtime, shard_time),
        average(target_gain, student_gain, total_gain),
        average(target_bias, student_bias, total_bias),
    )


GATE_C = 0.7978845608


def put_packed(ref, value):
    rows, lo = value.shape[0], value.shape[1] // 128 * 128
    for i in range(lo // 128):
        ref[i * rows : (i + 1) * rows, :] = value[:, i * 128 : (i + 1) * 128].astype(ref.dtype)
    at, half = lo // 128 * rows, rows // 2
    rest = jnp.concatenate([value[:half, lo:], value[half:, lo:]], axis=1)
    ref[at : at + half, :] = rest.astype(ref.dtype)


def unpacked(value, rows, width):
    lo = width // 128 * 128
    at, half, rest = lo // 128 * rows, rows // 2, width - lo
    parts = [value[i * rows : (i + 1) * rows] for i in range(lo // 128)]
    tail = value[at : at + half]
    parts.append(jnp.concatenate([tail[:, :rest], tail[:, rest:]], axis=0))
    return jnp.concatenate(parts, axis=1)


def in_pieces(rows):
    big = rows * 2 // 5 // 16 * 16
    return {"a": (0, big), "b": (big, big), "c": (2 * big, rows - 2 * big)}


def out_pieces(rows):
    big = rows * 3 // 5 // 16 * 16
    return {"o": (0, big), "d": (big, rows - big)}


def fused_kernel(n_rep, n_sam, names, *refs):
    r = dict(zip(names, refs))
    f32, bf16 = jnp.float32, jnp.bfloat16
    me, rep = lax.axis_index("dp"), lax.axis_index("rep")
    core, col, row = lax.rem(me, 2), lax.rem(lax.div(me, 2), 2), lax.div(me, 4)
    sw, so, st, tw, to, tt = (r[k] for k in ("sw", "so", "st", "tw", "to", "tt"))
    sg, sb, tg, tb, x_s, x_t = (r[k] for k in ("sg", "sb", "tg", "tb", "x_s", "x_t"))
    rows_in, rows_out, rows_time = sw.shape[0], so.shape[0], st.shape[0]
    pieces = {**in_pieces(rows_in), **out_pieces(rows_out)}
    first_rows = pieces["o"][1]
    width, tokens = x_s.shape
    per = tokens // n_sam
    lo = width // 128 * 128
    rest = width - lo
    ws_all, os_all, wt_all, ot_all = (r[k] for k in ("ws_all", "os_all", "wt_all", "ot_all"))
    ff = os_all.shape[0]
    tf_own, tf_all, e_part, e_in = (r[k] for k in ("tf_own", "tf_all", "e_part", "e_in"))
    g_all, e_all = r["g_o"], r["e_o"]

    flip = lambda b, on: 1 - b if on else b

    def peer(t):
        return flip(row, t & 4) * 4 + flip(col, t & 2) * 2 + flip(core, t & 1)

    def dp_id(t):
        return {"dp": peer(t)}

    def rep_peer(j):
        return flip(lax.div(rep, 2), j & 2) * 2 + flip(lax.rem(rep, 2), j & 1)

    def rep_id(j):
        return {"rep": rep_peer(j)}

    barrier = pltpu.get_barrier_semaphore()
    for t in range(1, 8):
        pl.semaphore_signal(barrier, inc=1, device_id=dp_id(t), device_id_type=MESH)
    for valid, step in ((rep > 0, -1), (rep < n_rep - 1, 1)):

        @pl.when(valid)
        def _(step=step):
            pl.semaphore_signal(barrier, inc=1, device_id={"rep": rep + step}, device_id_type=MESH)


    loads = []
    for i, name in enumerate(LOADED):
        copy = pltpu.make_async_copy(r[name + "_h"], r[name], r["ld_sem"].at[i])
        copy.start()
        loads.append(copy)

    def loaded(*keys):
        for key in keys:
            loads[LOADED.index(key)].wait()

    def send(src, dst, s_sem, r_sem, where):
        pltpu.make_async_remote_copy(
            src_ref=src, dst_ref=dst, send_sem=s_sem, recv_sem=r_sem,
            device_id=where, device_id_type=MESH,
        ).start()

    def bytes_of(ref, sem):
        return pltpu.make_async_remote_copy(
            src_ref=ref, dst_ref=ref, send_sem=sem, recv_sem=sem,
            device_id=dp_id(1), device_id_type=MESH,
        )

    def arrive(ref, sem):
        bytes_of(ref, sem).wait_recv()

    sent = []

    def exchange(key, source, slots, peers, where):
        for j in peers:
            src, dst = source(j), slots(j)
            send(src, dst, r[key + "_send"], r[key + "_recv"], where(j))

    bufs = (r["p_sin"], r["p_out"], r["p_tin"], r["p_tout"])
    s_in, out, t_in, t_out = range(4)
    g_send, g_recv = r["g_send"], r["g_recv"]
    loaded("ts")
    line = lax.broadcasted_iota(jnp.int32, (SUB, rows_time), 0)
    lane = lax.broadcasted_iota(jnp.int32, (SUB, rows_time), 1)
    steps = jnp.zeros((SUB, rows_time), f32)
    for k in range(n_sam):
        value = r["ts"][k]
        steps = jnp.where(line == k, value.astype(f32), steps)
        steps = jnp.where(line == n_sam + k, (value - SKIP).astype(f32), steps)
    half_width = 4 * rows_time
    for d in range(8):
        place = (lane + (d % 4) * rows_time).astype(f32)
        angle = steps * jnp.exp(-math.log(10000.0) * place / half_width)
        wave = jax.nn.silu(jnp.cos(angle) if d < 4 else jnp.sin(angle))
        tf_own[d] = jnp.where(line < 2 * n_sam, wave.astype(bf16).astype(f32), 0.0)
    tf_all[pl.ds(me, 1)] = tf_own[pl.ds(me, 1)]
    loaded("sw")
    put_packed(bufs[s_in].at[me], sw[...])
    pl.semaphore_wait(barrier, 7 + jnp.minimum(rep, 1) + jnp.minimum(n_rep - 1 - rep, 1))

    def cut(seg):
        return bufs[seg].shape[1] // 32 * 16

    def push(seg, orel, t, r_at, start=0, count=None):
        count = bufs[seg].shape[1] if count is None else count
        part = bufs[seg].at[peer(orel), pl.ds(start, count)]
        send(part, part, g_send.at[seg], g_recv.at[seg * 5 + r_at], dp_id(t))

    def landed(seg, r_at, count=1):
        arrive(bufs[seg].at[pl.ds(0, count)], g_recv.at[seg * 5 + r_at])

    def landed_rows(seg, r_at, count):
        arrive(bufs[seg].at[0, pl.ds(0, count)], g_recv.at[seg * 5 + r_at])

    def open_gather(seg):
        c = cut(seg)
        d = bufs[seg].shape[1] - c
        push(seg, 0, 2, 0, 0, c)
        push(seg, 0, 4, 1, c, d)
        push(seg, 0, 2, 4, c, d)
        push(seg, 0, 4, 4, 0, c)
        push(seg, 0, 1, 3)
        sent.append((bufs[seg].at[pl.ds(0, 7)], g_send.at[seg]))

    def relay(seg):
        c = cut(seg)
        d = bufs[seg].shape[1] - c
        landed_rows(seg, 0, c)
        push(seg, 2, 4, 2, 0, c)
        landed_rows(seg, 1, d)
        push(seg, 4, 2, 2, c, d)

    def relay_near(seg):
        landed(seg, 4)
        push(seg, 2, 1, 3)
        push(seg, 4, 1, 3)

    def relay_far(seg):
        landed(seg, 2)
        push(seg, 6, 1, 3)

    def close_gather(seg):
        landed(seg, 3, 4)

    here, there = (0, 2, 4, 6), (1, 3, 5, 7)

    def place_in(seg, dst, rels):
        half = rows_in // 2
        at = lo // 128 * rows_in
        for o in map(peer, rels):
            first = pl.multiple_of(o * rows_in, 16)
            second = pl.multiple_of(o * rows_in + half, 16)
            for i in range(lo // 128):
                dst[pl.ds(first, rows_in), i * 128 : (i + 1) * 128] = bufs[seg][o, i * rows_in : (i + 1) * rows_in, :]
            tail = bufs[seg][o, at : at + half, :]
            dst[pl.ds(first, half), lo:] = tail[:, :rest]
            dst[pl.ds(second, half), lo:] = tail[:, rest:]

    def place_out(seg, dst, lanes, rels):
        at = lo // 128 * rows_out
        for o in map(peer, rels):
            first = pl.multiple_of(o * rows_out, 16)
            for i in range(lo // 128):
                dst[pl.ds(first, rows_out), i * 128 : (i + 1) * 128] = bufs[seg][o, i * rows_out : (i + 1) * rows_out, :]
            dst[pl.ds(first, rows_out), lo:] = bufs[out][o, at : at + rows_out, :][:, lanes : lanes + rest]

    near = (1, 2, 4, 3, 5, 6, 7)
    exchange("tf", lambda t: tf_own.at[peer(t)], lambda t: tf_all.at[me], near, dp_id)
    open_gather(s_in)
    loaded("tw")
    put_packed(bufs[t_in].at[me], tw[...])
    open_gather(t_in)
    loaded("so", "to")
    for i in range(lo // 128):
        at, lanes = slice(i * rows_out, (i + 1) * rows_out), slice(i * 128, (i + 1) * 128)
        bufs[out][me, at, :] = so[:, lanes].astype(bf16)
        bufs[t_out][me, at, :] = to[:, lanes].astype(bf16)
    at = slice(lo // 128 * rows_out, (lo // 128 + 1) * rows_out)
    bufs[out][me, at, :] = jnp.concatenate([so[:, lo:], to[:, lo:]], axis=1).astype(bf16)
    loaded("st", "tt")
    st_b, tt_b = st[...].astype(bf16), tt[...].astype(bf16)
    arrive(tf_all.at[pl.ds(0, 7)], r["tf_recv"])
    feats = tf_all[...].reshape(8 * SUB, rows_time).astype(bf16)
    part_s = jnp.dot(feats, st_b, preferred_element_type=f32)
    part_t = jnp.dot(feats, tt_b, preferred_element_type=f32)
    which = lax.rem(lax.broadcasted_iota(jnp.int32, part_s.shape, 0), SUB)
    part = jnp.where(which < n_sam, part_s, part_t)
    for d in range(8):
        put_packed(e_part.at[d], part[d * SUB : d * SUB + 2 * n_sam])
    e_in[pl.ds(me, 1)] = e_part[pl.ds(me, 1)]
    exchange("e", lambda t: e_part.at[peer(t)], lambda t: e_in.at[me], near, dp_id)
    relay(s_in)
    open_gather(out)
    open_gather(t_out)

    ft_all, em_all = r["ft_all"], r["em_all"]
    ft_all[pl.ds(rep, 1)] = jnp.concatenate([tf_all[d, :n_sam, :] for d in range(8)], axis=0).astype(bf16)[None]
    far = (3, 2, 1)

    def pass_features(hops):
        for back, valid, onward in ((-1, rep >= hops, rep < n_rep - 1), (1, rep + hops < n_rep, rep > 0)):

            @pl.when(valid)
            def _(back=back, onward=onward):
                b = rep + back * hops
                at = ft_all.at[b]
                if hops:
                    arrive(at, r["ft_recv"].at[b])

                @pl.when(onward)
                def _():
                    send(at, at, r["ft_send"].at[(1 + back) // 2], r["ft_recv"].at[b], {"rep": rep - back})

    def features_sent():
        for k in range(n_rep):

            @pl.when(rep == k)
            def _(k=k):
                if k < n_rep - 1:
                    bytes_of(ft_all.at[pl.ds(0, k + 1)], r["ft_send"].at[0]).wait_send()
                if k > 0:
                    bytes_of(ft_all.at[pl.ds(0, n_rep - k)], r["ft_send"].at[1]).wait_send()

    pass_features(0)
    start = 0
    for student, target in ((sw, tw), (so, to), (st, tt)):
        count = student.shape[0]
        e_all[start : start + count, :] = ema_decay * target[...] + (1.0 - ema_decay) * student[...]
        start += count
    y_v, normed_v, inv_v, nb_v, nbt_v = (r[k] for k in ("y_v", "normed_v", "inv_v", "nb_v", "nbt_v"))
    xt_v = r["xt_v"]
    loaded("x_s", "sg", "sb")
    for k in range(n_sam):
        y_v[pl.ds(k * per, per), :] = x_s[:, pl.ds(k * per, per)].astype(f32).T
    relay(t_in)
    relay_near(s_in)
    loaded("x_t", "tg", "tb")
    for k in range(n_sam):
        xt_v[pl.ds(k * per, per), :] = x_t[:, pl.ds(k * per, per)].astype(f32).T

    arrive(e_in.at[pl.ds(0, 7)], r["e_recv"])
    emb = e_in[0]
    for k in range(1, 8):
        emb = emb + e_in[k]
    emb = unpacked(emb, 2 * n_sam, width)

    hid_v, hidt_v, a_v, b_v, gyb_v, gm_v = (r[k] for k in ("hid_v", "hidt_v", "a_v", "b_v", "gyb_v", "gm_v"))

    def normalise(x_rows, k, shift, gain, bias):
        summed = x_rows[pl.ds(k * per, per), :] + shift
        center = summed - jnp.mean(summed, axis=1, keepdims=True)
        inv = lax.rsqrt(jnp.mean(center * center, axis=1, keepdims=True) + 1e-05)
        normed = center * inv
        return summed, inv, normed, (normed * gain + bias).astype(bf16)

    for k in range(n_sam):
        at = pl.ds(k * per, per)
        summed, inv, normed, nb = normalise(y_v, k, emb[k : k + 1], sg[...][None], sb[...][None])
        y_v[at, :], normed_v[at, :], nb_v[at, :] = summed, normed, nb
        inv_v[at, :] = inv
    relay_far(s_in)
    relay(out)
    relay_near(t_in)
    for k in range(n_sam):
        at = pl.ds(k * per, per)
        summed, inv, normed, nb = normalise(
            xt_v, k, emb[n_sam + k : n_sam + k + 1], tg[...][None], tb[...][None]
        )
        y_v[at, :], nbt_v[at, :] = y_v[at, :] - summed, nb
    pass_features(1)
    relay_near(out)
    place_in(s_in, ws_all, here)
    close_gather(s_in)
    place_in(s_in, ws_all, there)
    relay(t_out)

    for k in range(n_sam):
        at = pl.ds(k * per, per)
        gate = contract_last(nb_v[at, :], ws_all[:ff, :])
        up = contract_last(nb_v[at, :], ws_all[ff:, :])
        square = gate * gate
        half = 0.5 + 0.5 * jnp.tanh(gate * (GATE_C + GATE_C * 0.044715 * square))
        act = gate * half
        slope = half + act * (1.0 - half) * (2.0 * GATE_C + 2.0 * GATE_C * 0.134145 * square)
        a_v[at, :], b_v[at, :] = up * slope, act
        hid_v[at, :] = (act * up).astype(bf16)
        if k == 0:
            relay_far(t_in)
            relay_near(t_out)
    relay_far(out)
    pass_features(2)
    place_in(t_in, wt_all, here)
    close_gather(t_in)
    place_in(t_in, wt_all, there)
    for k in range(n_sam):
        at = pl.ds(k * per, per)
        gate = contract_last(nbt_v[at, :], wt_all[:ff, :])
        up = contract_last(nbt_v[at, :], wt_all[ff:, :])
        half = 0.5 + 0.5 * jnp.tanh(gate * (GATE_C + GATE_C * 0.044715 * (gate * gate)))
        hidt_v[at, :] = (gate * half * up).astype(bf16)
        if k == 0:
            relay_far(t_out)
    place_out(out, os_all, 0, here)
    close_gather(out)
    place_out(out, os_all, 0, there)
    for k in range(n_sam):
        at = pl.ds(k * per, per)
        y_v[at, :] = y_v[at, :] + jnp.dot(hid_v[at, :], os_all[...], preferred_element_type=f32)
    place_out(t_out, ot_all, rest, here)
    close_gather(t_out)
    place_out(t_out, ot_all, rest, there)
    for k in range(n_sam):
        at = pl.ds(k * per, per)
        gy = (y_v[at, :] - jnp.dot(hidt_v[at, :], ot_all[...], preferred_element_type=f32)) * (1.0 / tokens)
        y_v[at, :], gyb_v[at, :] = gy, gy.astype(bf16)

    pass_features(3)
    r1_o, r1_i = r["r1_o"], r["r1_i"]

    def to_core(src, dst, count, q, key):
        part = src.at[pl.ds(pl.multiple_of((2 * q + 1 - core) * count, 16), count)]
        send(part, dst.at[q], r[key + "_send"], r[key + "_recv"], dp_id(1))

    def pair(key, rel):
        first, count = pieces[key]
        owner = peer(rel)
        g, r1, stride = (r["gs_o"], r1_o, rows_out) if key == "d" else (r["gs_i"], r1_i, rows_in)
        own = g[pl.ds(pl.multiple_of(owner * stride + first, 16), count), :]
        return own + r1[lax.div(owner, 2), first : first + count, :].astype(f32)

    def to_chip(key, k):
        s2, r2 = r["s2_" + key], r["r2_" + key]
        put_packed(s2.at[k], pair(key, 2 * k))
        send(s2.at[k], r2.at[k], r["r2s_" + key], r["r2r_" + key], dp_id(2 * k))

    total_out = contract_first(hid_v[...], gyb_v[...])
    r["gs_o"][...] = total_out
    r["gb_o"][...] = total_out.astype(bf16)
    for q in range(4):
        to_core(r["gb_o"], r1_o, rows_out, q, "c0")
    for k in range(n_sam):
        at = pl.ds(k * per, per)
        gh = contract_last(gyb_v[at, :], os_all[...])
        gm_v[0, at, :], gm_v[1, at, :] = (gh * a_v[at, :]).astype(bf16), (gh * b_v[at, :]).astype(bf16)

    def weight_grad(turn):
        h = 1 - row if turn == 0 else row
        total = contract_first(gm_v[h], nb_v[...])
        at = pl.ds(pl.multiple_of(h * ff, 16), ff)
        r["gs_i"][at, :], r["gb_i"][at, :] = total, total.astype(bf16)
        for q in range(2):
            to_core(r["gb_i"], r1_i, rows_in, 2 * h + q, "c" + str(1 + turn))

    grad_gain = jnp.zeros((1, width), f32)
    grad_bias = grad_gain
    embs = []
    small = r["small"]

    def input_grad(k):
        at = pl.ds(k * per, per)
        gz = jnp.dot(gm_v[0, at, :], ws_all[:ff, :], preferred_element_type=f32) + jnp.dot(
            gm_v[1, at, :], ws_all[ff:, :], preferred_element_type=f32
        )
        normed = normed_v[at, :]
        gn = gz * sg[...][None]
        gs = y_v[at, :] + inv_v[at, :] * (
            gn
            - jnp.mean(gn, axis=1, keepdims=True)
            - normed * jnp.mean(gn * normed, axis=1, keepdims=True)
        )
        embs.append(jnp.sum(gs, axis=0, keepdims=True))
        return jnp.sum(gz * normed, axis=0, keepdims=True), jnp.sum(gz, axis=0, keepdims=True)

    weight_grad(0)
    arrive(r1_o, r["c0_recv"])
    pk_v, z_v, zb_v, rz_v = r["pk_v"], r["z_v"], r["zb_v"], r["rz_v"]
    share = pk_v.shape[0] // n_rep
    for q in range(4):
        own = r["gs_o"][pl.ds(pl.multiple_of((2 * q + core) * rows_out, 16), first_rows), :]
        put_packed(pk_v, own + r1_o[q, :first_rows, :].astype(f32))
        for j in range(n_rep):
            z_v[j, q * share : (q + 1) * share, :] = pk_v[j * share : (j + 1) * share, :]
    for j in range(n_rep):
        zb_v[j] = z_v[j].astype(bf16)
    exchange("rz", lambda j: zb_v.at[rep_peer(j)], lambda j: rz_v.at[j], far, rep_id)
    for k in (3, 2, 1):
        to_chip("d", k)
    weight_grad(1)
    arrive(r1_i.at[pl.ds(0, 2)], r["c1_recv"])
    to_chip("a", 3)
    to_chip("a", 2)
    for k in range(n_sam):
        more_gain, more_bias = input_grad(k)
        grad_gain, grad_bias = grad_gain + more_gain, grad_bias + more_bias
        if k == 0:
            arrive(r1_i.at[pl.ds(0, 2)], r["c2_recv"])
            to_chip("a", 1)
            for q in (3, 2, 1):
                to_chip("b", q)
    high = [v.astype(bf16).astype(f32) for v in (grad_gain, grad_bias)]
    low = [v - h for v, h in zip((grad_gain, grad_bias), high)]
    n_small = n_sam + 4
    r["pack_v"][...] = jnp.zeros(r["pack_v"].shape, f32)
    put_packed(r["pack_v"], jnp.concatenate(embs + high + low, axis=0))
    small[pl.ds(me, 1)] = r["pack_v"][...].astype(bf16)[None]
    exchange("sm", lambda t: small.at[me], lambda t: small.at[me], near, dp_id)
    for k in (3, 2, 1):
        to_chip("c", k)
    for key in "dabc":
        put_packed(r["p_" + key], pair(key, 0))

    def chips_total(key):
        p, r2 = r["p_" + key], r["r2_" + key]
        arrive(r2.at[pl.ds(1, 3)], r["r2r_" + key])
        p[...] = p[...] + r2[1].astype(f32) + r2[2].astype(f32) + r2[3].astype(f32)
        return p

    def to_planes(key):
        p, pb, r3 = chips_total(key), r["pb_" + key], r["r3_" + key]
        part = pb.shape[1]
        for q in range(n_rep):
            pb[q] = p[q * part : (q + 1) * part, :].astype(bf16)
        for j in far:
            send(pb.at[rep_peer(j)], r3.at[j], r["r3s_" + key], r["r3r_" + key], rep_id(j))

    def to_planes_whole(key):
        r3 = r["r3_" + key]
        r3[pl.ds(rep, 1)] = chips_total(key)[...].astype(bf16)[None]
        for j in far:
            send(r3.at[rep], r3.at[rep], r["r3s_" + key], r["r3r_" + key], rep_id(j))

    def to_next_plane(key):
        r3 = r["r3_" + key]
        slot = lax.rem(rep, 2)
        r3[pl.ds(slot, 1)] = chips_total(key)[...].astype(bf16)[None]
        send(r3.at[slot], r3.at[slot], r["r3s_" + key], r["r3r_" + key], rep_id(1))

    def to_far_plane(key):
        r3, r4 = r["r3_" + key], r["r4_" + key]
        slot = lax.div(rep, 2)
        arrive(r3.at[0], r["r3r_" + key])
        r4[pl.ds(slot, 1)] = (r3[0].astype(f32) + r3[1].astype(f32)).astype(bf16)[None]
        send(r4.at[slot], r4.at[slot], r["r4s_" + key], r["r4r_" + key], rep_id(2))

    def plane_total():
        arrive(rz_v.at[pl.ds(1, 3)], r["rz_recv"])
        tz_v, tzb_v = r["tz_v"], r["tzb_v"]
        total = z_v[rep]
        for j in range(1, n_rep):
            total = total + rz_v[j].astype(f32)
        pk_v[...] = total
        for q in range(4):
            part = pk_v[q * share : (q + 1) * share, :]
            tz_v[q], tzb_v[q] = part, part.astype(bf16)
        exchange(
            "r2z", lambda k: tzb_v.at[lax.div(peer(2 * k), 2)], lambda k: r["r2z_v"].at[k], (3, 1, 2),
            lambda k: dp_id(2 * k),
        )

    def chip_total():
        arrive(r["r2z_v"].at[pl.ds(1, 3)], r["r2z_recv"])
        total = r["tz_v"][lax.div(me, 2)]
        for k in (1, 2, 3):
            total = total + r["r2z_v"][k].astype(f32)
        spread("o", total)

    def spread(key, total):
        fin = r["fin_" + key]
        fin[pl.ds(rep, 1)] = total.astype(bf16)[None]
        for j in far:
            send(fin.at[rep], fin.at[rep], r["r4s_" + key], r["r4r_" + key], rep_id(j))

    def share_total(key):
        p, r3 = r["p_" + key], r["r3_" + key]
        part = r3.shape[1]
        total = p[pl.ds(pl.multiple_of(rep * part, 8), part), :]
        arrive(r3.at[pl.ds(1, 3)], r["r3r_" + key])
        for j in range(1, n_rep):
            total = total + r3[j].astype(f32)
        spread(key, total)

    def finish(start, grad):
        at = slice(start, start + grad.shape[0])
        g_all[at, :] = grad
        e_all[at, :] = e_all[at, :] - (1.0 - ema_decay) * learn_rate * grad

    def collect(key, start, count):
        p, fin = (pk_v if key == "o" else r["p_" + key]), r["fin_" + key]
        part = fin.shape[1]
        arrive(fin.at[pl.ds(0, 3)], r["r4r_" + key])
        for q in range(n_rep):
            p[q * part : (q + 1) * part, :] = fin[q].astype(f32)
        finish(start, unpacked(p[...], count, width))

    def collect_direct(key, start):
        r3 = r["r3_" + key]
        arrive(r3.at[pl.ds(0, 3)], r["r3r_" + key])
        total = r3[0].astype(f32)
        for j in range(1, n_rep):
            total = total + r3[j].astype(f32)
        first, count = pieces[key]
        finish(start + first, unpacked(total, count, width))

    def collect_whole(key):
        r4 = r["r4_" + key]
        arrive(r4.at[0], r["r4r_" + key])
        first, count = pieces[key]
        finish(first, unpacked(r4[0].astype(f32) + r4[1].astype(f32), count, width))

    to_planes_whole("d")
    to_planes("a")
    plane_total()
    to_planes("b")
    arrive(small.at[pl.ds(0, 7)], r["sm_recv"])
    part = [small[d].astype(f32) for d in range(8)]
    sums = part[0]
    for k in range(1, 8):
        sums = sums + part[k]
    sums = unpacked(sums, n_small, width)
    sums = sums[n_sam : n_sam + 2] + sums[n_sam + 2 : n_sam + 4]
    high = sums.astype(bf16).astype(f32)
    put_packed(r["pack_v"], jnp.concatenate([high, sums - high], axis=0))
    n_em = em_all.shape[1] - small.shape[1]
    put_packed(em_all.at[rep], jnp.concatenate([unpacked(p, n_small, width)[:n_sam] for p in part], axis=0))
    em_all[pl.ds(rep, 1), n_em:, :] = r["pack_v"][...].astype(bf16)[None]

    @pl.when(core == 1)
    def _():
        exchange("em", lambda j: em_all.at[rep], lambda j: em_all.at[rep], far, rep_id)

    def pass_to_core():
        arrive(em_all.at[pl.ds(0, 3)], r["em_recv"])
        for j in far:
            at = em_all.at[rep_peer(j)]
            send(at, at, r["rs_send"], r["em_recv"], dp_id(1))

    to_next_plane("c")
    share_total("a")
    chip_total()
    collect_direct("d", rows_in)
    share_total("b")
    to_far_plane("c")
    pl.when(core == 1)(pass_to_core)
    collect("a", *pieces["a"])

    @pl.when(core == 0)
    def _():
        arrive(em_all.at[pl.ds(0, 3)], r["em_recv"])

    grad_time = jnp.zeros((rows_time, width), f32)
    for j in range(n_rep):
        samples = unpacked(em_all[j, :n_em, :].astype(f32), 8 * n_sam, width).astype(bf16)
        grad_time = grad_time + contract_first(ft_all[j], samples)
    sums = jnp.zeros((2, width), f32)
    for j in range(n_rep):
        part = unpacked(em_all[j, n_em:, :].astype(f32), 4, width)
        sums = sums + part[:2] + part[2:]
    finish(rows_in + rows_out, grad_time)
    gg, gb = sums[0, :], sums[1, :]
    r["gg_o"][...], r["gb_o_"][...] = gg, gb
    r["eg_o"][...] = average(tg[...], sg[...], gg)
    r["eb_o"][...] = average(tb[...], sb[...], gb)
    collect("o", rows_in, first_rows)
    collect("b", *pieces["b"])
    collect_whole("c")
    for key, ref in (("tf", tf_all), ("e", e_in), ("sm", small)):
        sent.append((ref.at[pl.ds(0, 7)], r[key + "_send"]))
    sent += [(r1_o, r["c0_send"]), (r1_i.at[pl.ds(0, 2)], r["c1_send"]), (r1_i.at[pl.ds(0, 2)], r["c2_send"])]
    for key in "abcd":
        sent.append((r["r2_" + key].at[pl.ds(0, 3)], r["r2s_" + key]))
        sent.append((r["r3_" + key].at[0] if key == "c" else r["r3_" + key].at[pl.ds(0, 3)], r["r3s_" + key]))
    sent.append((r["r4_c"].at[0], r["r4s_c"]))
    sent += [(rz_v.at[pl.ds(0, 3)], r["rz_send"]), (r["r2z_v"].at[pl.ds(0, 3)], r["r2z_send"])]
    for key in "oab":
        sent.append((r["fin_" + key].at[pl.ds(0, 3)], r["r4s_" + key]))
    for ref, sem in sent:
        bytes_of(ref, sem).wait_send()
    features_sent()

    @pl.when(core == 1)
    def _():
        for key in ("em_send", "rs_send"):
            bytes_of(em_all.at[pl.ds(0, 3)], r[key]).wait_send()


LOADED = ("ts", "sw", "so", "to", "tw", "st", "tt", "x_s", "sg", "sb", "x_t", "tg", "tb")


def average(target_p, student_p, grad_p):
    return ema_decay * target_p + (1.0 - ema_decay) * (student_p - learn_rate * grad_p)


def output_kernel(grads, means, gg, gb, eg, eb, gw_o, go_o, gt_o, gg_o, gb_o, ew_o, eo_o, et_o, eg_o, eb_o, sem):
    copies = []
    for src, outs in ((grads, (gw_o, go_o, gt_o)), (means, (ew_o, eo_o, et_o))):
        start = 0
        for dst in outs:
            copies.append((src.at[pl.ds(start, dst.shape[0])], dst))
            start += dst.shape[0]
    copies += [(gg, gg_o), (gb, gb_o), (eg, eg_o), (eb, eb_o)]
    copies = [pltpu.make_async_copy(src, dst, sem.at[i]) for i, (src, dst) in enumerate(copies)]
    for copy in copies:
        copy.start()
    for copy in copies:
        copy.wait()


def fused_device(n_dp, n_rep, *args):
    (student_in, target_in, timesteps, sw, so, st, sg, sb, tw, to, tt, tg, tb) = args
    f32, bf16 = jnp.float32, jnp.bfloat16
    tokens, width = student_in.shape
    n_sam = timesteps.shape[0]
    rows_in, rows_out, rows_time = sw.shape[0], so.shape[0], st.shape[0]
    ff = rows_out * n_dp
    rows_all = rows_in + rows_out + rows_time
    vm = pltpu.VMEM
    dma = pltpu.SemaphoreType.DMA
    full = width // 128
    rows_emb = -(-(2 * n_sam * full + n_sam) // SUB) * SUB
    rows_small = -(-((n_sam + 4) * full + (n_sam + 4) // 2) // 16) * 16
    packed_in = rows_in * full + rows_in // 2
    first_rows = out_pieces(rows_out)["o"][1]
    packed_out = first_rows * full + first_rows // 2
    scratch = dict(
        ts=pltpu.SMEM((n_sam,), jnp.int32),
        sw=vm(sw.shape, f32), so=vm(so.shape, f32), st=vm(st.shape, f32),
        tw=vm(tw.shape, f32), to=vm(to.shape, f32), tt=vm(tt.shape, f32),
        sg=vm(sg.shape, f32), sb=vm(sb.shape, f32), tg=vm(tg.shape, f32), tb=vm(tb.shape, f32),
        x_s=vm((width, tokens), bf16), x_t=vm((width, tokens), bf16),
        p_sin=vm((n_dp, packed_in, 128), bf16), p_out=vm((n_dp, rows_out * (full + 1), 128), bf16),
        p_tin=vm((n_dp, packed_in, 128), bf16), p_tout=vm((n_dp, rows_out * full, 128), bf16),
        ws_all=vm((n_dp * rows_in, width), bf16), os_all=vm((ff, width), bf16),
        wt_all=vm((n_dp * rows_in, width), bf16), ot_all=vm((ff, width), bf16),
        tf_own=vm((n_dp, SUB, rows_time), f32), tf_all=vm((n_dp, SUB, rows_time), f32),
        e_part=vm((n_dp, rows_emb, 128), f32), e_in=vm((n_dp, rows_emb, 128), f32),
        small=vm((n_dp, rows_small, 128), bf16), pack_v=vm((rows_small, 128), f32),
        ft_all=vm((n_rep, n_dp * n_sam, rows_time), bf16), em_all=vm((n_rep, n_dp * n_sam * full + n_dp * n_sam // 2 + rows_small, 128), bf16),
        normed_v=vm((tokens, width), f32), inv_v=vm((tokens, 1), f32), nb_v=vm((tokens, width), bf16),
        hid_v=vm((tokens, ff), bf16), hidt_v=vm((tokens, ff), bf16), a_v=vm((tokens, ff), f32), b_v=vm((tokens, ff), f32),
        y_v=vm((tokens, width), f32), xt_v=vm((tokens, width), f32), nbt_v=vm((tokens, width), bf16), gyb_v=vm((tokens, width), bf16),
        gm_v=vm((2, tokens, ff), bf16),
        gs_i=vm((n_dp * rows_in, width), f32), gs_o=vm((ff, width), f32),
        gb_i=vm((n_dp * rows_in, width), bf16), gb_o=vm((ff, width), bf16),
        r1_i=vm((4, rows_in, width), bf16), r1_o=vm((4, rows_out, width), bf16),
        rs_send=dma, ft_send=dma((2,)), ft_recv=dma((n_rep,)), ld_sem=dma((len(LOADED),)), g_send=dma((4,)), g_recv=dma((20,)),
    )
    for key, (_, count) in (*in_pieces(rows_in).items(), ("d", out_pieces(rows_out)["d"])):
        packed = count * full + count // 2
        scratch["p_" + key] = vm((packed, 128), f32)
        for name in ("s2_", "r2_"):
            scratch[name + key] = vm((4, packed, 128), bf16)
        if key == "c":
            for name in ("r3_", "r4_"):
                scratch[name + key] = vm((2, packed, 128), bf16)
            scratch["r4s_" + key], scratch["r4r_" + key] = dma, dma
        elif key == "d":
            scratch["r3_" + key] = vm((n_rep, packed, 128), bf16)
        else:
            scratch["r3_" + key] = vm((n_rep, packed // n_rep, 128), bf16)
            scratch["pb_" + key] = vm((n_rep, packed // n_rep, 128), bf16)
        for name in ("r2", "r3"):
            scratch[name + "s_" + key], scratch[name + "r_" + key] = dma, dma
    for key, packed in (("a", scratch["p_a"].shape[0]), ("b", scratch["p_b"].shape[0]), ("o", packed_out)):
        scratch["fin_" + key] = vm((n_rep, packed // n_rep, 128), bf16)
        scratch["r4s_" + key], scratch["r4r_" + key] = dma, dma
    scratch["pk_v"] = vm((packed_out, 128), f32)
    scratch["z_v"] = vm((n_rep, packed_out, 128), f32)
    for name in ("zb_v", "rz_v"):
        scratch[name] = vm((n_rep, packed_out, 128), bf16)
    scratch["tz_v"] = vm((4, packed_out // n_rep, 128), f32)
    for name in ("tzb_v", "r2z_v"):
        scratch[name] = vm((4, packed_out // n_rep, 128), bf16)
    for key in ("tf", "e", "sm", "em", "c0", "c1", "c2", "rz", "r2z"):
        scratch[key + "_send"], scratch[key + "_recv"] = dma, dma
    shape = jax.ShapeDtypeStruct
    results = dict(
        g_o=shape((rows_all, width), f32), e_o=shape((rows_all, width), f32), gg_o=shape((width,), f32),
        gb_o_=shape((width,), f32), eg_o=shape((width,), f32), eb_o=shape((width,), f32),
    )
    operands = dict(
        ts=timesteps, sw=sw, so=so, to=to, tw=tw, st=st, tt=tt, x_s=student_in.T, sg=sg, sb=sb,
        x_t=target_in.T, tg=tg, tb=tb,
    )
    names = tuple(key + "_h" for key in operands) + tuple(results) + tuple(scratch)
    values = pl.pallas_call(
        functools.partial(fused_kernel, n_rep, n_sam, names),
        out_shape=tuple(results.values()),
        in_specs=[pl.BlockSpec(memory_space=pltpu.HBM)] * len(operands),
        out_specs=[pl.BlockSpec(memory_space=vm)] * len(results),
        scratch_shapes=list(scratch.values()),
        compiler_params=pltpu.CompilerParams(
            collective_id=0, has_side_effects=True, vmem_limit_bytes=40 * 1024 * 1024
        ),
        name="distill_step",
    )(*(pltpu.with_memory_space_constraint(value, pltpu.HBM) for value in operands.values()))
    big = [shape(w.shape, f32) for w in (sw, so, st)]
    flat = [shape((width,), f32)] * 2
    return tuple(
        pl.pallas_call(
            output_kernel,
            out_shape=(*big, *flat, *big, *flat),
            in_specs=[pl.BlockSpec(memory_space=vm)] * len(results),
            out_specs=[pl.BlockSpec(memory_space=pltpu.HBM)] * 10,
            scratch_shapes=[dma((10,))],
            compiler_params=pltpu.CompilerParams(vmem_limit_bytes=8 * 1024 * 1024),
            name="output_step",
        )(*values)
    )


def fits_fused(n_dp, n_rep, args):
    tokens, samples = args[0].shape[0], args[2].shape[0]
    n_dev = n_dp * n_rep
    rows = [args[i].shape[0] for i in (3, 4, 5)]
    return (
        n_dp == 8
        and n_rep == 4
        and samples % n_dev == 0
        and 2 * (samples // n_dev) + 0 <= SUB
        and (samples // n_dev) % 2 == 0
        and tokens % samples == 0
        and (tokens // samples) % 128 == 0
        and all(r % (16 * n_dp) == 0 for r in rows)
        and all(r % (32 * n_dp) == 0 for r in rows[:1])
        and in_pieces(rows[0] // n_dp)["a"][1] % 64 == 0
        and in_pieces(rows[0] // n_dp)["a"][1] > 0
        and out_pieces(rows[1] // n_dp)["o"][1] > 0
        and rows[0] == 2 * rows[1]
        and rows[2] == rows[1]
        and args[0].shape[1] % 128 == 64
    )


def solution(mesh):
    in_specs = (
        P(("dp", "rep"), None),
        P(("dp", "rep"), None),
        P(("dp", "rep")),
        P("dp", None),
        P("dp", None),
        P("dp", None),
        P(),
        P(),
        P("dp", None),
        P("dp", None),
        P("dp", None),
        P(),
        P(),
    )
    out_specs = (
        P("dp", None),
        P("dp", None),
        P("dp", None),
        P(),
        P(),
        P("dp", None),
        P("dp", None),
        P("dp", None),
        P(),
        P(),
    )
    n_dp, n_rep = mesh.shape["dp"], mesh.shape["rep"]

    def step(*args):
        fused = fits_fused(n_dp, n_rep, args)
        body = functools.partial(fused_device, n_dp, n_rep) if fused else per_device
        return jax.shard_map(
            body, mesh=mesh, in_specs=in_specs, out_specs=out_specs, check_vma=False
        )(*args)

    return step
```

```python
import functools
import math

import jax
import jax.numpy as jnp
from jax import lax
from jax.experimental import pallas as pl
from jax.experimental.pallas import tpu as pltpu
from jax.sharding import PartitionSpec as P

MESH = pl.DeviceIdType.MESH
SUB = 8

SKIP = 20


ema_decay = 0.95
learn_rate = 0.05


def sinusoid(step_ids, width):
    half_width = width // 2
    frequency = jnp.exp(-math.log(10000.0) * jnp.arange(half_width, dtype=jnp.float32) / half_width)
    angles = step_ids.astype(jnp.float32)[:, None] * frequency[None, :]
    return jnp.concatenate([jnp.cos(angles), jnp.sin(angles)], axis=1)


def gelu_tanh(value):
    inner = 0.7978845608 * (value + 0.044715 * value * value * value)
    return 0.5 * value * (1.0 + jnp.tanh(inner))


def gelu_slope(value):
    tangent = jnp.tanh(0.7978845608 * (value + 0.044715 * value * value * value))
    return 0.5 * (1.0 + tangent) + 0.5 * value * (1.0 - tangent * tangent) * 0.7978845608 * (
        1.0 + 0.134145 * value * value
    )


def contract_last(left, right):
    return lax.dot_general(
        left, right, (((1,), (1,)), ((), ())), preferred_element_type=jnp.float32
    )


def contract_first(left, right):
    return lax.dot_general(
        left, right, (((0,), (0,)), ((), ())), preferred_element_type=jnp.float32
    )


def forward(tok_rows, step_ids, w_in, w_out, w_time, gain, bias):
    time_feat = jax.nn.silu(sinusoid(step_ids, w_time.shape[0])).astype(jnp.bfloat16)
    embedding = jnp.dot(time_feat, w_time, preferred_element_type=jnp.float32)
    samples = step_ids.shape[0]
    width = tok_rows.shape[1]
    summed = tok_rows.astype(jnp.float32).reshape(samples, -1, width) + embedding[:, None, :]
    summed = summed.reshape(-1, width)
    center = summed - jnp.mean(summed, axis=1, keepdims=True)
    inv_std = lax.rsqrt(jnp.mean(center * center, axis=1, keepdims=True) + 1e-05)
    normed = center * inv_std
    normed_b = (normed * gain + bias).astype(jnp.bfloat16)
    mixed = contract_last(normed_b, w_in)
    hidden_count = w_out.shape[0]
    gate_part = mixed[:, :hidden_count]
    up_part = mixed[:, hidden_count:]
    gelu_gate = gelu_tanh(gate_part)
    hidden = (gelu_gate * up_part).astype(jnp.bfloat16)
    output = summed + jnp.dot(hidden, w_out, preferred_element_type=jnp.float32)
    return (output, (time_feat, normed, inv_std, normed_b, gate_part, up_part, gelu_gate, hidden))


def backward(grad_y, saved, w_in, w_out, gain):
    time_feat, normed, inv_std, normed_b, gate_part, up_part, gelu_gate, hidden = saved
    grad_yb = grad_y.astype(jnp.bfloat16)
    grad_h = contract_last(grad_yb, w_out)
    grad_mix = jnp.concatenate(
        [grad_h * up_part * gelu_slope(gate_part), grad_h * gelu_gate], axis=1
    ).astype(jnp.bfloat16)
    grad_z = jnp.dot(grad_mix, w_in, preferred_element_type=jnp.float32)
    grad_gain = jnp.sum(grad_z * normed, axis=0)
    grad_bias = jnp.sum(grad_z, axis=0)
    grad_n = grad_z * gain
    grad_s = grad_y + inv_std * (
        grad_n
        - jnp.mean(grad_n, axis=1, keepdims=True)
        - normed * jnp.mean(grad_n * normed, axis=1, keepdims=True)
    )
    samples = time_feat.shape[0]
    grad_emb = jnp.sum(grad_s.reshape(samples, -1, grad_s.shape[1]), axis=1)
    grad_time = lax.dot_general(
        time_feat.astype(jnp.float32),
        grad_emb,
        (((0,), (0,)), ((), ())),
        precision=lax.Precision.HIGHEST,
        preferred_element_type=jnp.float32,
    )
    return (grad_yb, grad_mix, grad_gain, grad_bias, grad_time)


def fetch(piece_in, piece_out, piece_time):
    return (
        lax.all_gather(piece_in, "dp", axis=0, tiled=True),
        lax.all_gather(piece_out, "dp", axis=0, tiled=True),
        lax.all_gather(piece_time, "dp", axis=0, tiled=True),
    )


def per_device(
    student_in,
    target_in,
    timesteps,
    student_win,
    student_wout,
    student_wtime,
    student_gain,
    student_bias,
    target_win,
    target_wout,
    target_wtime,
    target_gain,
    target_bias,
):
    s_in, s_out, s_time = fetch(
        student_win.astype(jnp.bfloat16),
        student_wout.astype(jnp.bfloat16),
        student_wtime.astype(jnp.bfloat16),
    )
    student_out, saved = forward(
        student_in, timesteps, s_in, s_out, s_time, student_gain, student_bias
    )
    t_in, t_out, t_time = fetch(
        target_win.astype(jnp.bfloat16),
        target_wout.astype(jnp.bfloat16),
        target_wtime.astype(jnp.bfloat16),
    )
    target_out, unused = forward(
        target_in, timesteps - SKIP, t_in, t_out, t_time, target_gain, target_bias
    )
    grad_y = (student_out - target_out) / student_in.shape[0]
    back_in, back_out = (
        lax.all_gather(student_win.astype(jnp.bfloat16), "dp", axis=0, tiled=True),
        lax.all_gather(student_wout.astype(jnp.bfloat16), "dp", axis=0, tiled=True),
    )
    grad_yb, grad_mix, grad_gain, grad_bias, grad_time = backward(
        grad_y, saved, back_in, back_out, student_gain
    )
    normed_b = saved[3]
    hidden = saved[7]
    part = grad_mix
    shard_in = lax.psum_scatter(
        contract_first(part, normed_b), "dp", scatter_dimension=0, tiled=True
    )
    part = hidden
    shard_out = lax.psum_scatter(
        contract_first(part, grad_yb), "dp", scatter_dimension=0, tiled=True
    )
    shard_time = lax.psum_scatter(grad_time, "dp", scatter_dimension=0, tiled=True)
    shard_in, shard_out, shard_time = lax.psum((shard_in, shard_out, shard_time), "rep")
    total_gain, total_bias = lax.psum((grad_gain, grad_bias), ("dp", "rep"))

    def average(target_p, student_p, grad_p):
        return ema_decay * target_p + (1.0 - ema_decay) * (student_p - learn_rate * grad_p)

    return (
        shard_in,
        shard_out,
        shard_time,
        total_gain,
        total_bias,
        average(target_win, student_win, shard_in),
        average(target_wout, student_wout, shard_out),
        average(target_wtime, student_wtime, shard_time),
        average(target_gain, student_gain, total_gain),
        average(target_bias, student_bias, total_bias),
    )


GATE_C = 0.7978845608


def put_packed(ref, value):
    rows, lo = value.shape[0], value.shape[1] // 128 * 128
    for i in range(lo // 128):
        ref[i * rows : (i + 1) * rows, :] = value[:, i * 128 : (i + 1) * 128].astype(ref.dtype)
    at, half = lo // 128 * rows, rows // 2
    rest = jnp.concatenate([value[:half, lo:], value[half:, lo:]], axis=1)
    ref[at : at + half, :] = rest.astype(ref.dtype)


def unpacked(value, rows, width):
    lo = width // 128 * 128
    at, half, rest = lo // 128 * rows, rows // 2, width - lo
    parts = [value[i * rows : (i + 1) * rows] for i in range(lo // 128)]
    tail = value[at : at + half]
    parts.append(jnp.concatenate([tail[:, :rest], tail[:, rest:]], axis=0))
    return jnp.concatenate(parts, axis=1)


def in_pieces(rows):
    big = rows * 2 // 5 // 16 * 16
    return {"a": (0, big), "b": (big, big), "c": (2 * big, rows - 2 * big)}


def out_pieces(rows):
    big = rows * 3 // 5 // 16 * 16
    return {"o": (0, big), "d": (big, rows - big)}


def fused_kernel(n_rep, n_sam, names, *refs):
    r = dict(zip(names, refs))
    f32, bf16 = jnp.float32, jnp.bfloat16
    me, rep = lax.axis_index("dp"), lax.axis_index("rep")
    core, col, row = lax.rem(me, 2), lax.rem(lax.div(me, 2), 2), lax.div(me, 4)
    sw, so, st, tw, to, tt = (r[k] for k in ("sw", "so", "st", "tw", "to", "tt"))
    sg, sb, tg, tb, x_s, x_t = (r[k] for k in ("sg", "sb", "tg", "tb", "x_s", "x_t"))
    rows_in, rows_out, rows_time = sw.shape[0], so.shape[0], st.shape[0]
    pieces = {**in_pieces(rows_in), **out_pieces(rows_out)}
    first_rows = pieces["o"][1]
    width, tokens = x_s.shape
    per = tokens // n_sam
    lo = width // 128 * 128
    rest = width - lo
    ws_all, os_all, wt_all, ot_all = (r[k] for k in ("ws_all", "os_all", "wt_all", "ot_all"))
    ff = os_all.shape[0]
    tf_own, tf_all, e_part, e_in = (r[k] for k in ("tf_own", "tf_all", "e_part", "e_in"))
    g_all, e_all = r["g_o"], r["e_o"]

    flip = lambda b, on: 1 - b if on else b

    def peer(t):
        return flip(row, t & 4) * 4 + flip(col, t & 2) * 2 + flip(core, t & 1)

    def dp_id(t):
        return {"dp": peer(t)}

    def rep_peer(j):
        return flip(lax.div(rep, 2), j & 2) * 2 + flip(lax.rem(rep, 2), j & 1)

    def rep_id(j):
        return {"rep": rep_peer(j)}

    barrier = pltpu.get_barrier_semaphore()
    for t in range(1, 8):
        pl.semaphore_signal(barrier, inc=1, device_id=dp_id(t), device_id_type=MESH)
    for valid, step in ((rep > 0, -1), (rep < n_rep - 1, 1)):

        @pl.when(valid)
        def _(step=step):
            pl.semaphore_signal(barrier, inc=1, device_id={"rep": rep + step}, device_id_type=MESH)


    loads = []
    for i, name in enumerate(LOADED):
        copy = pltpu.make_async_copy(r[name + "_h"], r[name], r["ld_sem"].at[i])
        copy.start()
        loads.append(copy)

    def loaded(*keys):
        for key in keys:
            loads[LOADED.index(key)].wait()

    def send(src, dst, s_sem, r_sem, where):
        pltpu.make_async_remote_copy(
            src_ref=src, dst_ref=dst, send_sem=s_sem, recv_sem=r_sem,
            device_id=where, device_id_type=MESH,
        ).start()

    def bytes_of(ref, sem):
        return pltpu.make_async_remote_copy(
            src_ref=ref, dst_ref=ref, send_sem=sem, recv_sem=sem,
            device_id=dp_id(1), device_id_type=MESH,
        )

    def arrive(ref, sem):
        bytes_of(ref, sem).wait_recv()

    for name in PACKED_SENDS:
        r[name] = r["g_s"]
    sent = []

    def exchange(key, source, slots, peers, where):
        for j in peers:
            src, dst = source(j), slots(j)
            send(src, dst, r[key + "_s"], r[key + "_r"], where(j))

    bufs = (r["p_sin"], r["p_out"], r["p_tin"], r["p_tout"])
    s_in, out, t_in, t_out = range(4)
    g_s, g_r = r["g_s"], r["g_r"]
    loaded("ts")
    line = lax.broadcasted_iota(jnp.int32, (SUB, rows_time), 0)
    lane = lax.broadcasted_iota(jnp.int32, (SUB, rows_time), 1)
    steps = jnp.zeros((SUB, rows_time), f32)
    for k in range(n_sam):
        value = r["ts"][k]
        steps = jnp.where(line == k, value.astype(f32), steps)
        steps = jnp.where(line == n_sam + k, (value - SKIP).astype(f32), steps)
    half_width = 4 * rows_time
    for d in range(8):
        place = (lane + (d % 4) * rows_time).astype(f32)
        angle = steps * jnp.exp(-math.log(10000.0) * place / half_width)
        wave = jax.nn.silu(jnp.cos(angle) if d < 4 else jnp.sin(angle))
        tf_own[d] = jnp.where(line < 2 * n_sam, wave.astype(bf16).astype(f32), 0.0)
    tf_all[pl.ds(me, 1)] = tf_own[pl.ds(me, 1)]
    loaded("sw")
    put_packed(bufs[s_in].at[me], sw[...])
    pl.semaphore_wait(barrier, 7 + jnp.minimum(rep, 1) + jnp.minimum(n_rep - 1 - rep, 1))

    def cut(seg):
        return bufs[seg].shape[1] // 32 * 16

    def push(seg, orel, t, r_at, start=0, count=None):
        count = bufs[seg].shape[1] if count is None else count
        part = bufs[seg].at[peer(orel), pl.ds(start, count)]
        send(part, part, g_s, g_r.at[seg * 5 + r_at], dp_id(t))

    def landed(seg, r_at, count=1):
        arrive(bufs[seg].at[pl.ds(0, count)], g_r.at[seg * 5 + r_at])

    def landed_rows(seg, r_at, count):
        arrive(bufs[seg].at[0, pl.ds(0, count)], g_r.at[seg * 5 + r_at])

    def open_gather(seg):
        c = cut(seg)
        d = bufs[seg].shape[1] - c
        push(seg, 0, 2, 0, 0, c)
        push(seg, 0, 4, 1, c, d)
        if seg != t_in:
            open_rest(seg)
        push(seg, 0, 1, 3)

    def open_rest(seg):
        c = cut(seg)
        push(seg, 0, 2, 4, c, bufs[seg].shape[1] - c)
        push(seg, 0, 4, 4, 0, c)

    def relay(seg):
        c = cut(seg)
        d = bufs[seg].shape[1] - c
        landed_rows(seg, 0, c)
        push(seg, 2, 4, 2, 0, c)
        landed_rows(seg, 1, d)
        push(seg, 4, 2, 2, c, d)

    def relay_near(seg):
        landed(seg, 4)
        push(seg, 2, 1, 3)
        push(seg, 4, 1, 3)

    def relay_far(seg):
        landed(seg, 2)
        push(seg, 6, 1, 3)

    def close_gather(seg):
        landed(seg, 3, 4)

    here, there = (0, 2, 4, 6), (1, 3, 5, 7)

    def place_in(seg, dst, rels):
        half = rows_in // 2
        at = lo // 128 * rows_in
        for o in map(peer, rels):
            first = pl.multiple_of(o * rows_in, 16)
            second = pl.multiple_of(o * rows_in + half, 16)
            for i in range(lo // 128):
                dst[pl.ds(first, rows_in), i * 128 : (i + 1) * 128] = bufs[seg][o, i * rows_in : (i + 1) * rows_in, :]
            tail = bufs[seg][o, at : at + half, :]
            dst[pl.ds(first, half), lo:] = tail[:, :rest]
            dst[pl.ds(second, half), lo:] = tail[:, rest:]

    def place_out(seg, dst, lanes, rels):
        at = lo // 128 * rows_out
        for o in map(peer, rels):
            first = pl.multiple_of(o * rows_out, 16)
            for i in range(lo // 128):
                dst[pl.ds(first, rows_out), i * 128 : (i + 1) * 128] = bufs[seg][o, i * rows_out : (i + 1) * rows_out, :]
            dst[pl.ds(first, rows_out), lo:] = bufs[out][o, at : at + rows_out, :][:, lanes : lanes + rest]

    near = (1, 2, 4, 3, 5, 6, 7)
    exchange("tf", lambda t: tf_own.at[peer(t)], lambda t: tf_all.at[me], near, dp_id)
    open_gather(s_in)
    loaded("tw")
    put_packed(bufs[t_in].at[me], tw[...])
    open_gather(t_in)
    loaded("so", "to")
    for i in range(lo // 128):
        at, lanes = slice(i * rows_out, (i + 1) * rows_out), slice(i * 128, (i + 1) * 128)
        bufs[out][me, at, :] = so[:, lanes].astype(bf16)
        bufs[t_out][me, at, :] = to[:, lanes].astype(bf16)
    at = slice(lo // 128 * rows_out, (lo // 128 + 1) * rows_out)
    bufs[out][me, at, :] = jnp.concatenate([so[:, lo:], to[:, lo:]], axis=1).astype(bf16)
    loaded("st", "tt")
    st_b, tt_b = st[...].astype(bf16), tt[...].astype(bf16)
    arrive(tf_all.at[pl.ds(0, 7)], r["tf_r"])
    feats = tf_all[...].reshape(8 * SUB, rows_time).astype(bf16)
    part_s = jnp.dot(feats, st_b, preferred_element_type=f32)
    part_t = jnp.dot(feats, tt_b, preferred_element_type=f32)
    which = lax.rem(lax.broadcasted_iota(jnp.int32, part_s.shape, 0), SUB)
    part = jnp.where(which < n_sam, part_s, part_t)
    for d in range(8):
        put_packed(e_part.at[d], part[d * SUB : d * SUB + 2 * n_sam])
    e_in[pl.ds(me, 1)] = e_part[pl.ds(me, 1)]
    exchange("e", lambda t: e_part.at[peer(t)], lambda t: e_in.at[me], near, dp_id)
    relay(s_in)
    open_rest(t_in)
    open_gather(out)
    open_gather(t_out)

    ft_all, em_all = r["ft_all"], r["em_all"]
    ft_all[pl.ds(rep, 1)] = jnp.concatenate([tf_all[d, :n_sam, :] for d in range(8)], axis=0).astype(bf16)[None]
    far = (3, 2, 1)

    def pass_features(hops):
        for back, valid, onward in ((-1, rep >= hops, rep < n_rep - 1), (1, rep + hops < n_rep, rep > 0)):

            @pl.when(valid)
            def _(back=back, onward=onward):
                b = rep + back * hops
                at = ft_all.at[b]
                if hops:
                    arrive(at, r["ft_r"].at[b])

                @pl.when(onward)
                def _():
                    send(at, at, r["ft_s"].at[(1 + back) // 2], r["ft_r"].at[b], {"rep": rep - back})

    def features_sent():
        for k in range(n_rep):

            @pl.when(rep == k)
            def _(k=k):
                if k < n_rep - 1:
                    bytes_of(ft_all.at[pl.ds(0, k + 1)], r["ft_s"].at[0]).wait_send()
                if k > 0:
                    bytes_of(ft_all.at[pl.ds(0, n_rep - k)], r["ft_s"].at[1]).wait_send()

    pass_features(0)
    start = 0
    for student, target in ((sw, tw), (so, to), (st, tt)):
        count = student.shape[0]
        e_all[start : start + count, :] = ema_decay * target[...] + (1.0 - ema_decay) * student[...]
        start += count
    y_v, normed_v, inv_v, nb_v, nbt_v = (r[k] for k in ("y_v", "normed_v", "inv_v", "nb_v", "nbt_v"))
    xt_v = r["xt_v"]
    loaded("x_s", "sg", "sb")
    for k in range(n_sam):
        y_v[pl.ds(k * per, per), :] = x_s[:, pl.ds(k * per, per)].astype(f32).T
    relay(t_in)
    relay_near(s_in)
    loaded("x_t", "tg", "tb")
    for k in range(n_sam):
        xt_v[pl.ds(k * per, per), :] = x_t[:, pl.ds(k * per, per)].astype(f32).T

    arrive(e_in.at[pl.ds(0, 7)], r["e_r"])
    emb = e_in[0]
    for k in range(1, 8):
        emb = emb + e_in[k]
    emb = unpacked(emb, 2 * n_sam, width)

    hid_v, hidt_v, a_v, b_v, gyb_v, gm_v = (r[k] for k in ("hid_v", "hidt_v", "a_v", "b_v", "gyb_v", "gm_v"))

    def normalise(x_rows, k, shift, gain, bias):
        summed = x_rows[pl.ds(k * per, per), :] + shift
        center = summed - jnp.mean(summed, axis=1, keepdims=True)
        inv = lax.rsqrt(jnp.mean(center * center, axis=1, keepdims=True) + 1e-05)
        normed = center * inv
        return summed, inv, normed, (normed * gain + bias).astype(bf16)

    for k in range(n_sam):
        at = pl.ds(k * per, per)
        summed, inv, normed, nb = normalise(y_v, k, emb[k : k + 1], sg[...][None], sb[...][None])
        y_v[at, :], normed_v[at, :], nb_v[at, :] = summed, normed, nb
        inv_v[at, :] = inv
    relay_far(s_in)
    relay(out)
    relay_near(t_in)
    for k in range(n_sam):
        at = pl.ds(k * per, per)
        summed, inv, normed, nb = normalise(
            xt_v, k, emb[n_sam + k : n_sam + k + 1], tg[...][None], tb[...][None]
        )
        y_v[at, :], nbt_v[at, :] = y_v[at, :] - summed, nb
    pass_features(1)
    relay_near(out)
    place_in(s_in, ws_all, here)
    close_gather(s_in)
    place_in(s_in, ws_all, there)
    relay(t_out)

    for k in range(n_sam):
        at = pl.ds(k * per, per)
        gate = contract_last(nb_v[at, :], ws_all[:ff, :])
        up = contract_last(nb_v[at, :], ws_all[ff:, :])
        square = gate * gate
        half = 0.5 + 0.5 * jnp.tanh(gate * (GATE_C + GATE_C * 0.044715 * square))
        act = gate * half
        slope = half + act * (1.0 - half) * (2.0 * GATE_C + 2.0 * GATE_C * 0.134145 * square)
        a_v[at, :], b_v[at, :] = up * slope, act
        hid_v[at, :] = (act * up).astype(bf16)
        if k == 0:
            relay_far(t_in)
            relay_near(t_out)
    relay_far(out)
    pass_features(2)
    place_in(t_in, wt_all, here)
    close_gather(t_in)
    place_in(t_in, wt_all, there)
    for k in range(n_sam):
        at = pl.ds(k * per, per)
        gate = contract_last(nbt_v[at, :], wt_all[:ff, :])
        up = contract_last(nbt_v[at, :], wt_all[ff:, :])
        half = 0.5 + 0.5 * jnp.tanh(gate * (GATE_C + GATE_C * 0.044715 * (gate * gate)))
        hidt_v[at, :] = (gate * half * up).astype(bf16)
        if k == 0:
            relay_far(t_out)
    place_out(out, os_all, 0, here)
    close_gather(out)
    place_out(out, os_all, 0, there)
    for k in range(n_sam):
        at = pl.ds(k * per, per)
        y_v[at, :] = y_v[at, :] + jnp.dot(hid_v[at, :], os_all[...], preferred_element_type=f32)
    place_out(t_out, ot_all, rest, here)
    close_gather(t_out)
    place_out(t_out, ot_all, rest, there)
    for k in range(n_sam):
        at = pl.ds(k * per, per)
        gy = (y_v[at, :] - jnp.dot(hidt_v[at, :], ot_all[...], preferred_element_type=f32)) * (1.0 / tokens)
        y_v[at, :], gyb_v[at, :] = gy, gy.astype(bf16)

    pass_features(3)
    r1_o, r1_i = r["r1_o"], r["r1_i"]

    def to_core(src, dst, count, q, key):
        part = src.at[pl.ds(pl.multiple_of((2 * q + 1 - core) * count, 16), count)]
        send(part, dst.at[q], r[key + "_s"], r[key + "_r"], dp_id(1))

    def pair(key, rel):
        first, count = pieces[key]
        owner = peer(rel)
        g, r1, stride = (r["gs_o"], r1_o, rows_out) if key == "d" else (r["gs_i"], r1_i, rows_in)
        own = g[pl.ds(pl.multiple_of(owner * stride + first, 16), count), :]
        return own + r1[lax.div(owner, 2), first : first + count, :].astype(f32)

    def to_chip(key, k):
        s2, r2 = r["s2_" + key], r["r2_" + key]
        put_packed(s2.at[k], pair(key, 2 * k))
        send(s2.at[k], r2.at[k], r["r2s_" + key], r["r2r_" + key], dp_id(2 * k))

    total_out = contract_first(hid_v[...], gyb_v[...])
    r["gs_o"][...] = total_out
    r["gb_o"][...] = total_out.astype(bf16)
    for q in range(4):
        to_core(r["gb_o"], r1_o, rows_out, q, "c0")
    for k in range(n_sam):
        at = pl.ds(k * per, per)
        gh = contract_last(gyb_v[at, :], os_all[...])
        gm_v[0, at, :], gm_v[1, at, :] = (gh * a_v[at, :]).astype(bf16), (gh * b_v[at, :]).astype(bf16)

    def weight_grad(turn):
        h = 1 - row if turn == 0 else row
        total = contract_first(gm_v[h], nb_v[...])
        at = pl.ds(pl.multiple_of(h * ff, 16), ff)
        r["gs_i"][at, :], r["gb_i"][at, :] = total, total.astype(bf16)
        for q in range(2):
            to_core(r["gb_i"], r1_i, rows_in, 2 * h + q, "c" + str(1 + turn))

    grad_gain = jnp.zeros((1, width), f32)
    grad_bias = grad_gain
    embs = []
    small = r["small"]

    def input_grad(k):
        at = pl.ds(k * per, per)
        gz = jnp.dot(gm_v[0, at, :], ws_all[:ff, :], preferred_element_type=f32) + jnp.dot(
            gm_v[1, at, :], ws_all[ff:, :], preferred_element_type=f32
        )
        normed = normed_v[at, :]
        gn = gz * sg[...][None]
        gs = y_v[at, :] + inv_v[at, :] * (
            gn
            - jnp.mean(gn, axis=1, keepdims=True)
            - normed * jnp.mean(gn * normed, axis=1, keepdims=True)
        )
        embs.append(jnp.sum(gs, axis=0, keepdims=True))
        return jnp.sum(gz * normed, axis=0, keepdims=True), jnp.sum(gz, axis=0, keepdims=True)

    weight_grad(0)
    arrive(r1_o, r["c0_r"])
    pk_v, z_v, zb_v, rz_v = r["pk_v"], r["z_v"], r["zb_v"], r["rz_v"]
    share = pk_v.shape[0] // n_rep
    for q in range(4):
        own = r["gs_o"][pl.ds(pl.multiple_of((2 * q + core) * rows_out, 16), first_rows), :]
        put_packed(pk_v, own + r1_o[q, :first_rows, :].astype(f32))
        for j in range(n_rep):
            z_v[j, q * share : (q + 1) * share, :] = pk_v[j * share : (j + 1) * share, :]
    for j in range(n_rep):
        zb_v[j] = z_v[j].astype(bf16)
    exchange("rz", lambda j: zb_v.at[rep_peer(j)], lambda j: rz_v.at[j], far, rep_id)
    for k in (3, 2, 1):
        to_chip("d", k)
    weight_grad(1)
    arrive(r1_i.at[pl.ds(0, 2)], r["c1_r"])
    to_chip("a", 3)
    to_chip("a", 2)
    for k in range(n_sam):
        more_gain, more_bias = input_grad(k)
        grad_gain, grad_bias = grad_gain + more_gain, grad_bias + more_bias
        if k == 0:
            arrive(r1_i.at[pl.ds(0, 2)], r["c2_r"])
            to_chip("a", 1)
            for q in (3, 2, 1):
                to_chip("b", q)
    high = [v.astype(bf16).astype(f32) for v in (grad_gain, grad_bias)]
    low = [v - h for v, h in zip((grad_gain, grad_bias), high)]
    n_small = n_sam + 4
    r["pack_v"][...] = jnp.zeros(r["pack_v"].shape, f32)
    put_packed(r["pack_v"], jnp.concatenate(embs + high + low, axis=0))
    small[pl.ds(me, 1)] = r["pack_v"][...].astype(bf16)[None]
    exchange("sm", lambda t: small.at[me], lambda t: small.at[me], near, dp_id)
    for k in (3, 2, 1):
        to_chip("c", k)
    for key in "dabc":
        put_packed(r["p_" + key], pair(key, 0))

    def chips_total(key):
        p, r2 = r["p_" + key], r["r2_" + key]
        arrive(r2.at[pl.ds(1, 3)], r["r2r_" + key])
        p[...] = p[...] + r2[1].astype(f32) + r2[2].astype(f32) + r2[3].astype(f32)
        return p

    def to_planes(key):
        p, pb, r3 = chips_total(key), r["pb_" + key], r["r3_" + key]
        part = pb.shape[1]
        for q in range(n_rep):
            pb[q] = p[q * part : (q + 1) * part, :].astype(bf16)
        for j in far:
            send(pb.at[rep_peer(j)], r3.at[j], r["r3s_" + key], r["r3r_" + key], rep_id(j))

    def to_planes_whole(key):
        r3 = r["r3_" + key]
        r3[pl.ds(rep, 1)] = chips_total(key)[...].astype(bf16)[None]
        for j in far:
            send(r3.at[rep], r3.at[rep], r["r3s_" + key], r["r3r_" + key], rep_id(j))

    def to_next_plane(key):
        r3 = r["r3_" + key]
        slot = lax.rem(rep, 2)
        r3[pl.ds(slot, 1)] = chips_total(key)[...].astype(bf16)[None]
        send(r3.at[slot], r3.at[slot], r["r3s_" + key], r["r3r_" + key], rep_id(1))

    def to_far_plane(key):
        r3, r4 = r["r3_" + key], r["r4_" + key]
        slot = lax.div(rep, 2)
        arrive(r3.at[0], r["r3r_" + key])
        r4[pl.ds(slot, 1)] = (r3[0].astype(f32) + r3[1].astype(f32)).astype(bf16)[None]
        send(r4.at[slot], r4.at[slot], r["r4s_" + key], r["r4r_" + key], rep_id(2))

    def plane_total():
        arrive(rz_v.at[pl.ds(1, 3)], r["rz_r"])
        tz_v, tzb_v = r["tz_v"], r["tzb_v"]
        total = z_v[rep]
        for j in range(1, n_rep):
            total = total + rz_v[j].astype(f32)
        pk_v[...] = total
        for q in range(4):
            part = pk_v[q * share : (q + 1) * share, :]
            tz_v[q], tzb_v[q] = part, part.astype(bf16)
        exchange(
            "r2z", lambda k: tzb_v.at[lax.div(peer(2 * k), 2)], lambda k: r["r2z_v"].at[k], (3, 1, 2),
            lambda k: dp_id(2 * k),
        )

    def chip_total():
        arrive(r["r2z_v"].at[pl.ds(1, 3)], r["r2z_r"])
        total = r["tz_v"][lax.div(me, 2)]
        for k in (1, 2, 3):
            total = total + r["r2z_v"][k].astype(f32)
        spread("o", total)

    def spread(key, total):
        fin = r["fin_" + key]
        fin[pl.ds(rep, 1)] = total.astype(bf16)[None]
        for j in far:
            send(fin.at[rep], fin.at[rep], r["r4s_" + key], r["r4r_" + key], rep_id(j))

    def share_total(key):
        p, r3 = r["p_" + key], r["r3_" + key]
        part = r3.shape[1]
        total = p[pl.ds(pl.multiple_of(rep * part, 8), part), :]
        arrive(r3.at[pl.ds(1, 3)], r["r3r_" + key])
        for j in range(1, n_rep):
            total = total + r3[j].astype(f32)
        spread(key, total)

    def finish(start, grad):
        at = slice(start, start + grad.shape[0])
        g_all[at, :] = grad
        e_all[at, :] = e_all[at, :] - (1.0 - ema_decay) * learn_rate * grad

    def collect(key, start, count):
        p, fin = (pk_v if key == "o" else r["p_" + key]), r["fin_" + key]
        part = fin.shape[1]
        arrive(fin.at[pl.ds(0, 3)], r["r4r_" + key])
        for q in range(n_rep):
            p[q * part : (q + 1) * part, :] = fin[q].astype(f32)
        finish(start, unpacked(p[...], count, width))

    def collect_direct(key, start):
        r3 = r["r3_" + key]
        arrive(r3.at[pl.ds(0, 3)], r["r3r_" + key])
        total = r3[0].astype(f32)
        for j in range(1, n_rep):
            total = total + r3[j].astype(f32)
        first, count = pieces[key]
        finish(start + first, unpacked(total, count, width))

    def collect_whole(key):
        r4 = r["r4_" + key]
        arrive(r4.at[0], r["r4r_" + key])
        first, count = pieces[key]
        finish(first, unpacked(r4[0].astype(f32) + r4[1].astype(f32), count, width))

    to_planes_whole("d")
    to_planes("a")
    plane_total()
    to_planes("b")
    arrive(small.at[pl.ds(0, 7)], r["sm_r"])
    part = [small[d].astype(f32) for d in range(8)]
    sums = part[0]
    for k in range(1, 8):
        sums = sums + part[k]
    sums = unpacked(sums, n_small, width)
    sums = sums[n_sam : n_sam + 2] + sums[n_sam + 2 : n_sam + 4]
    high = sums.astype(bf16).astype(f32)
    put_packed(r["pack_v"], jnp.concatenate([high, sums - high], axis=0))
    n_em = em_all.shape[1] - small.shape[1]
    put_packed(em_all.at[rep], jnp.concatenate([unpacked(p, n_small, width)[:n_sam] for p in part], axis=0))
    em_all[pl.ds(rep, 1), n_em:, :] = r["pack_v"][...].astype(bf16)[None]

    @pl.when(core == 1)
    def _():
        exchange("em", lambda j: em_all.at[rep], lambda j: em_all.at[rep], far, rep_id)

    def pass_to_core():
        arrive(em_all.at[pl.ds(0, 3)], r["em_r"])
        for j in far:
            at = em_all.at[rep_peer(j)]
            send(at, at, r["rs_s"], r["em_r"], dp_id(1))

    to_next_plane("c")
    share_total("a")
    chip_total()
    collect_direct("d", rows_in)
    share_total("b")
    to_far_plane("c")
    pl.when(core == 1)(pass_to_core)
    collect("a", *pieces["a"])

    @pl.when(core == 0)
    def _():
        arrive(em_all.at[pl.ds(0, 3)], r["em_r"])

    grad_time = jnp.zeros((rows_time, width), f32)
    for j in range(n_rep):
        samples = unpacked(em_all[j, :n_em, :].astype(f32), 8 * n_sam, width).astype(bf16)
        grad_time = grad_time + contract_first(ft_all[j], samples)
    sums = jnp.zeros((2, width), f32)
    for j in range(n_rep):
        part = unpacked(em_all[j, n_em:, :].astype(f32), 4, width)
        sums = sums + part[:2] + part[2:]
    finish(rows_in + rows_out, grad_time)
    gg, gb = sums[0, :], sums[1, :]
    r["gg_o"][...], r["gb_o_"][...] = gg, gb
    r["eg_o"][...] = average(tg[...], sg[...], gg)
    r["eb_o"][...] = average(tb[...], sb[...], gb)
    collect("o", rows_in, first_rows)
    collect("b", *pieces["b"])
    collect_whole("c")
    sent.append((r["all_v"], g_s))
    for key, ref in (("tf", tf_all), ("e", e_in)):
        sent.append((ref.at[pl.ds(0, 7)], r[key + "_s"]))
    sent += [(r1_o, r["c0_s"]), (r1_i.at[pl.ds(0, 2)], r["c1_s"]), (r1_i.at[pl.ds(0, 2)], r["c2_s"])]
    sent += [(r["r2z_v"].at[pl.ds(0, 3)], r["r2z_s"]), (r["fin_o"].at[pl.ds(0, 3)], r["r4s_o"])]
    for ref, sem in sent:
        bytes_of(ref, sem).wait_send()
    features_sent()

    @pl.when(core == 1)
    def _():
        for key in ("em_s", "rs_s"):
            bytes_of(em_all.at[pl.ds(0, 3)], r[key]).wait_send()


PACKED_SENDS = ("sm_s", "rz_s", "r4s_a", "r4s_b", "r4s_c") + tuple(n + k for n in ("r2s_", "r3s_") for k in "abcd")
LOADED = ("ts", "sw", "so", "to", "tw", "st", "tt", "x_s", "sg", "sb", "x_t", "tg", "tb")


def average(target_p, student_p, grad_p):
    return ema_decay * target_p + (1.0 - ema_decay) * (student_p - learn_rate * grad_p)


def output_kernel(grads, means, gg, gb, eg, eb, gw_o, go_o, gt_o, gg_o, gb_o, ew_o, eo_o, et_o, eg_o, eb_o, sem):
    copies = []
    for src, outs in ((grads, (gw_o, go_o, gt_o)), (means, (ew_o, eo_o, et_o))):
        start = 0
        for dst in outs:
            copies.append((src.at[pl.ds(start, dst.shape[0])], dst))
            start += dst.shape[0]
    copies += [(gg, gg_o), (gb, gb_o), (eg, eg_o), (eb, eb_o)]
    copies = [pltpu.make_async_copy(src, dst, sem.at[i]) for i, (src, dst) in enumerate(copies)]
    for copy in copies:
        copy.start()
    for copy in copies:
        copy.wait()


def fused_device(n_dp, n_rep, *args):
    (student_in, target_in, timesteps, sw, so, st, sg, sb, tw, to, tt, tg, tb) = args
    f32, bf16 = jnp.float32, jnp.bfloat16
    tokens, width = student_in.shape
    n_sam = timesteps.shape[0]
    rows_in, rows_out, rows_time = sw.shape[0], so.shape[0], st.shape[0]
    ff = rows_out * n_dp
    rows_all = rows_in + rows_out + rows_time
    vm = pltpu.VMEM
    dma = pltpu.SemaphoreType.DMA
    full = width // 128
    rows_emb = -(-(2 * n_sam * full + n_sam) // SUB) * SUB
    rows_small = -(-((n_sam + 4) * full + (n_sam + 4) // 2) // 16) * 16
    packed_in = rows_in * full + rows_in // 2
    first_rows = out_pieces(rows_out)["o"][1]
    packed_out = first_rows * full + first_rows // 2
    scratch = dict(
        ts=pltpu.SMEM((n_sam,), jnp.int32),
        sw=vm(sw.shape, f32), so=vm(so.shape, f32), st=vm(st.shape, f32),
        tw=vm(tw.shape, f32), to=vm(to.shape, f32), tt=vm(tt.shape, f32),
        sg=vm(sg.shape, f32), sb=vm(sb.shape, f32), tg=vm(tg.shape, f32), tb=vm(tb.shape, f32),
        x_s=vm((width, tokens), bf16), x_t=vm((width, tokens), bf16),
        p_sin=vm((n_dp, packed_in, 128), bf16), p_out=vm((n_dp, rows_out * (full + 1), 128), bf16),
        p_tin=vm((n_dp, packed_in, 128), bf16), p_tout=vm((n_dp, rows_out * full, 128), bf16),
        ws_all=vm((n_dp * rows_in, width), bf16), os_all=vm((ff, width), bf16),
        wt_all=vm((n_dp * rows_in, width), bf16), ot_all=vm((ff, width), bf16),
        tf_own=vm((n_dp, SUB, rows_time), f32), tf_all=vm((n_dp, SUB, rows_time), f32),
        e_part=vm((n_dp, rows_emb, 128), f32), e_in=vm((n_dp, rows_emb, 128), f32),
        small=vm((n_dp, rows_small, 128), bf16), pack_v=vm((rows_small, 128), f32),
        ft_all=vm((n_rep, n_dp * n_sam, rows_time), bf16), em_all=vm((n_rep, n_dp * n_sam * full + n_dp * n_sam // 2 + rows_small, 128), bf16),
        normed_v=vm((tokens, width), f32), inv_v=vm((tokens, 1), f32), nb_v=vm((tokens, width), bf16),
        hid_v=vm((tokens, ff), bf16), hidt_v=vm((tokens, ff), bf16), a_v=vm((tokens, ff), f32), b_v=vm((tokens, ff), f32),
        y_v=vm((tokens, width), f32), xt_v=vm((tokens, width), f32), nbt_v=vm((tokens, width), bf16), gyb_v=vm((tokens, width), bf16),
        gm_v=vm((2, tokens, ff), bf16),
        gs_i=vm((n_dp * rows_in, width), f32), gs_o=vm((ff, width), f32),
        gb_i=vm((n_dp * rows_in, width), bf16), gb_o=vm((ff, width), bf16),
        r1_i=vm((4, rows_in, width), bf16), r1_o=vm((4, rows_out, width), bf16),
        rs_s=dma, ft_s=dma((2,)), ft_r=dma((n_rep,)), ld_sem=dma((len(LOADED),)), g_s=dma, g_r=dma((20,)),
    )
    for key, (_, count) in (*in_pieces(rows_in).items(), ("d", out_pieces(rows_out)["d"])):
        packed = count * full + count // 2
        scratch["p_" + key] = vm((packed, 128), f32)
        for name in ("s2_", "r2_"):
            scratch[name + key] = vm((4, packed, 128), bf16)
        if key == "c":
            for name in ("r3_", "r4_"):
                scratch[name + key] = vm((2, packed, 128), bf16)
            scratch["r4s_" + key], scratch["r4r_" + key] = dma, dma
        elif key == "d":
            scratch["r3_" + key] = vm((n_rep, packed, 128), bf16)
        else:
            scratch["r3_" + key] = vm((n_rep, packed // n_rep, 128), bf16)
            scratch["pb_" + key] = vm((n_rep, packed // n_rep, 128), bf16)
        for name in ("r2", "r3"):
            scratch[name + "s_" + key], scratch[name + "r_" + key] = dma, dma
    for key, packed in (("a", scratch["p_a"].shape[0]), ("b", scratch["p_b"].shape[0]), ("o", packed_out)):
        scratch["fin_" + key] = vm((n_rep, packed // n_rep, 128), bf16)
        scratch["r4s_" + key], scratch["r4r_" + key] = dma, dma
    scratch["pk_v"] = vm((packed_out, 128), f32)
    scratch["z_v"] = vm((n_rep, packed_out, 128), f32)
    for name in ("zb_v", "rz_v"):
        scratch[name] = vm((n_rep, packed_out, 128), bf16)
    scratch["tz_v"] = vm((4, packed_out // n_rep, 128), f32)
    for name in ("tzb_v", "r2z_v"):
        scratch[name] = vm((4, packed_out // n_rep, 128), bf16)
    for key in ("tf", "e", "sm", "em", "c0", "c1", "c2", "rz", "r2z"):
        scratch[key + "_s"], scratch[key + "_r"] = dma, dma
    whole = packed_in * 2 + rows_out * (2 * full + 1)
    rows_sent = 7 * (whole + rows_small) + 3 * packed_out
    for key in "abcd":
        packed = scratch["p_" + key].shape[0]
        rows_sent += 3 * packed + {"a": 6 * packed // n_rep, "b": 6 * packed // n_rep, "c": 2 * packed, "d": 3 * packed}[key]
    scratch["all_v"] = vm((rows_sent, 128), bf16)
    for name in PACKED_SENDS:
        scratch.pop(name, None)
    shape = jax.ShapeDtypeStruct
    results = dict(
        g_o=shape((rows_all, width), f32), e_o=shape((rows_all, width), f32), gg_o=shape((width,), f32),
        gb_o_=shape((width,), f32), eg_o=shape((width,), f32), eb_o=shape((width,), f32),
    )
    operands = dict(
        ts=timesteps, sw=sw, so=so, to=to, tw=tw, st=st, tt=tt, x_s=student_in.T, sg=sg, sb=sb,
        x_t=target_in.T, tg=tg, tb=tb,
    )
    names = tuple(key + "_h" for key in operands) + tuple(results) + tuple(scratch)
    values = pl.pallas_call(
        functools.partial(fused_kernel, n_rep, n_sam, names),
        out_shape=tuple(results.values()),
        in_specs=[pl.BlockSpec(memory_space=pltpu.HBM)] * len(operands),
        out_specs=[pl.BlockSpec(memory_space=vm)] * len(results),
        scratch_shapes=list(scratch.values()),
        compiler_params=pltpu.CompilerParams(
            collective_id=0, has_side_effects=True, vmem_limit_bytes=40 * 1024 * 1024
        ),
        name="distill_step",
    )(*(pltpu.with_memory_space_constraint(value, pltpu.HBM) for value in operands.values()))
    big = [shape(w.shape, f32) for w in (sw, so, st)]
    flat = [shape((width,), f32)] * 2
    return tuple(
        pl.pallas_call(
            output_kernel,
            out_shape=(*big, *flat, *big, *flat),
            in_specs=[pl.BlockSpec(memory_space=vm)] * len(results),
            out_specs=[pl.BlockSpec(memory_space=pltpu.HBM)] * 10,
            scratch_shapes=[dma((10,))],
            compiler_params=pltpu.CompilerParams(vmem_limit_bytes=8 * 1024 * 1024),
            name="output_step",
        )(*values)
    )


def fits_fused(n_dp, n_rep, args):
    tokens, samples = args[0].shape[0], args[2].shape[0]
    n_dev = n_dp * n_rep
    rows = [args[i].shape[0] for i in (3, 4, 5)]
    return (
        n_dp == 8
        and n_rep == 4
        and samples % n_dev == 0
        and 2 * (samples // n_dev) + 0 <= SUB
        and (samples // n_dev) % 2 == 0
        and tokens % samples == 0
        and (tokens // samples) % 128 == 0
        and all(r % (16 * n_dp) == 0 for r in rows)
        and all(r % (32 * n_dp) == 0 for r in rows[:1])
        and in_pieces(rows[0] // n_dp)["a"][1] % 64 == 0
        and in_pieces(rows[0] // n_dp)["a"][1] > 0
        and out_pieces(rows[1] // n_dp)["o"][1] > 0
        and rows[0] == 2 * rows[1]
        and rows[2] == rows[1]
        and args[0].shape[1] % 128 == 64
    )


def solution(mesh):
    in_specs = (
        P(("dp", "rep"), None),
        P(("dp", "rep"), None),
        P(("dp", "rep")),
        P("dp", None),
        P("dp", None),
        P("dp", None),
        P(),
        P(),
        P("dp", None),
        P("dp", None),
        P("dp", None),
        P(),
        P(),
    )
    out_specs = (
        P("dp", None),
        P("dp", None),
        P("dp", None),
        P(),
        P(),
        P("dp", None),
        P("dp", None),
        P("dp", None),
        P(),
        P(),
    )
    n_dp, n_rep = mesh.shape["dp"], mesh.shape["rep"]

    def step(*args):
        fused = fits_fused(n_dp, n_rep, args)
        body = functools.partial(fused_device, n_dp, n_rep) if fused else per_device
        return jax.shard_map(
            body, mesh=mesh, in_specs=in_specs, out_specs=out_specs, check_vma=False
        )(*args)

    return step
```
